32 devices in a mesh: grp: 2 (over x), dom: 16 (over z, y, core).
Axes of the slice: x: 2, y: 2, z: 4, core: 2. Of those that a mesh axis runs over, the one named last changes fastest.
Arguments:
- positions: float32 [512, 3, 128], P(('grp', 'dom')), may hold values from 0 to 1
- smoothing: float32 [512, 128], P(('grp', 'dom')), may hold values from 0.35 to 0.55
- energy: float32 [512, 128], P(('grp', 'dom')), may hold values from 0.5 to 2
- mass: float32 [512, 128], P(('grp', 'dom')), may hold values from 0.00390625 to 0.015625
- old_density: float32 [512, 128], P(('grp', 'dom')), may hold values from 1 to 6
- active: int32 [512, 128], P(('grp', 'dom')), may hold values 0 or 1
- pair_list: int32 [512, 2], P(('grp', 'dom')), may hold values from 0 to 15
- export_leaves: int32 [768, 2], P(('grp', 'dom')), may hold values from 0 to 15
- export_route: int32 [768, 1], P(('grp', 'dom')), may hold values from 0 to 14; in each aligned block of 24 rows (0 to 23, 24 to 47, ...) at most 2 rows name the same one
Outputs:
- density: float32 [512, 128], P(('grp', 'dom'))
- acceleration: float32 [512, 3, 128], P(('grp', 'dom'))
- timestep: float32 [], replicated
The draws below stay inside these ranges and needn't reach their ends.
Inputs may be any that keep to these rules, and one draw needn't show every extreme that they name: `pair_list`: indices of leaf blocks of the domain that holds the row. `export_leaves`: column 0 is a leaf block of the domain that holds the row, column 1 a leaf block of the destination domain. `export_route`: among the rows of one domain no value occurs more than 2 times; in some domains one value occurs exactly 2 times. `active`: every domain holds some particles with value 1.
All inputs are finite; a program needn't handle non-finite values. No bound on the sum of `active` on one device may be relied on, other than what follows from the above.
Results may differ from the reference program's by a relative error of at most 0.0003.
Values sent between devices are 32-bit elements; how exact they have to be, the bound alone decides.
No kernel may reach another device: no remote copies, remote signals or barrier semaphores. Data moves between devices by JAX's collectives and lax.ppermute only.
A program may use at most 64 MiB of HBM per device.

```python
import math
import jax
import jax.numpy as jnp
import numpy as np
from jax import lax

LEAF = 128
LEAVES = 16
MOST = 2
EXPORTS = 24
LEAVES_ALL = 512
PAIRS_ALL = 512
EXPORTS_ALL = 768
N_GRP = 2
N_DOM = 16


def touch_ends(result, stream_key, smallest, high):
    longest = result.shape.index(max(result.shape))
    spots = []
    for shift in (0, 1):
        where = [jax.random.randint(jax.random.fold_in(stream_key, axis), (), 0, length) for axis, length in enumerate(result.shape)]
        where[longest] = (where[longest] + shift) % result.shape[longest]
        spots.append(tuple(where))
    return result.at[spots[0]].set(smallest).at[spots[1]].set(high)


def block_scale(rng, shape, split, low, largest):
    loudness = 1.0
    for dim, parts in split:
        steps = jax.random.uniform(jax.random.fold_in(jax.random.fold_in(rng, 6), dim), (parts,), jnp.float32, low / len(split), largest / len(split))
        loudness = loudness * jnp.repeat(jnp.exp(steps), shape[dim] // parts).reshape((-1,) + (1,) * (len(shape) - 1 - dim))
    return loudness


def deal_out(rng, own, number, rows, count, top, limit, skew):
    ranking = jax.random.permutation(rng, count)
    heavy_load, common = shares(count, rows * top, limit, skew, True), shares(count, rows * top, limit, skew, False)
    places = jnp.arange(count)

    def named(sizes, offset_by):
        used = int((sizes > 0).sum())
        fixed = max(1, used // 4)
        shifted = fixed + (places - fixed + offset_by * (used - fixed)) % max(1, count - fixed)
        return jnp.zeros((count,), jnp.int32).at[ranking[jnp.where(places < fixed, places, shifted)]].set(jnp.asarray(sizes, jnp.int32))

    sizes = jnp.where(number % 4 == 0, named(heavy_load, number // 4), named(common, number - number // 4 - 1))
    mixed = jax.random.permutation(jax.random.fold_in(own, 3), count)
    source_of, receiver = mixed[0:count // 2 * 2:2], mixed[1:count // 2 * 2:2]
    slack = jnp.minimum(sizes[source_of] - 1, limit - sizes[receiver]) // 2
    slack = jnp.where((source_of == ranking[0]) | (receiver == ranking[0]) | (sizes[receiver] == 0), 0, jnp.maximum(slack, 0))
    shifted = jax.random.randint(jax.random.fold_in(own, 4), (count // 2,), 0, 1 << 20) % (slack + 1)
    sizes = sizes.at[source_of].add(-shifted).at[receiver].add(shifted)
    items = jnp.searchsorted(jnp.cumsum(sizes), jnp.arange(rows * top), side="right").astype(jnp.int32)
    table = items.reshape(top, rows).T
    table = table[jax.random.permutation(jax.random.fold_in(own, 1), rows)]
    offset_by = jax.random.randint(jax.random.fold_in(own, 2), (rows, 1), 0, top)
    return jnp.take_along_axis(table, (jnp.arange(top)[None, :] + offset_by) % top, axis=1)


def shares(amount, total, most, lean, full):
    loads = [(1 << 20) // math.isqrt(grade ** lean) + 1 for grade in range(1, amount + 1)]
    largest = most if full else min(most, max(-(-total // amount), total * loads[0] // sum(loads)))
    least = 1 if total - largest >= amount - 1 else 0
    holding, surplus = [largest] + [least] * (amount - 1), total - largest - least * (amount - 1)
    while surplus > 0:
        candidates = [i for i in range(1, amount) if holding[i] < largest] or [i for i in range(1, amount) if holding[i] < most]
        whole, remaining = sum([loads[i] for i in candidates]), surplus
        for i in candidates:
            more = min(most - holding[i], max(1, remaining * loads[i] // whole), surplus)
            holding[i] = holding[i] + more
            surplus = surplus - more
    return np.array(holding)


def setup_inputs(seed: int = 0) -> dict:
    seeds = jax.random.split(jax.random.key(seed), 10)
    positions = jnp.clip(1.0 * jax.random.uniform(seeds[0], (LEAVES_ALL, 3, LEAF), jnp.float32) ** block_scale(seeds[0], (LEAVES_ALL, 3, LEAF), ((0, 32),), -0.2, 0.2), 0.0, 1.0)
    smoothing = jnp.clip(jnp.exp(math.log(0.55) - 0.45198516 * jax.random.uniform(seeds[1], (LEAVES_ALL, LEAF), jnp.float32) ** block_scale(seeds[1], (LEAVES_ALL, LEAF), ((0, 32),), -0.2, 0.2)), 0.35, 0.55)
    energy = jnp.clip(jnp.exp(math.log(2.0) - 1.3862944 * jax.random.uniform(seeds[2], (LEAVES_ALL, LEAF), jnp.float32) ** block_scale(seeds[2], (LEAVES_ALL, LEAF), ((0, 32),), -0.2, 0.2)), 0.5, 2.0)
    mass = jnp.clip(jnp.exp(math.log(0.015625) - 1.3862944 * jax.random.uniform(seeds[3], (LEAVES_ALL, LEAF), jnp.float32) ** block_scale(seeds[3], (LEAVES_ALL, LEAF), ((0, 32),), -0.2, 0.2)), 0.00390625, 0.015625)
    old_density = jnp.clip(jnp.exp(math.log(6.0) - 1.7917595 * jax.random.uniform(seeds[4], (LEAVES_ALL, LEAF), jnp.float32) ** block_scale(seeds[4], (LEAVES_ALL, LEAF), ((0, 32),), -0.2, 0.2)), 1.0, 6.0)
    active = touch_ends((jax.random.randint(seeds[5], (LEAVES_ALL, LEAF), 0, 4) < 3).astype(jnp.int32), jax.random.fold_in(seeds[5], 1), 0, 1)
    pair_list = touch_ends(jax.random.randint(seeds[6], (PAIRS_ALL, 2), 0, LEAVES), jax.random.fold_in(seeds[6], 1), 0, LEAVES - 1).astype(jnp.int32)
    export_leaves = touch_ends(jax.random.randint(seeds[7], (EXPORTS_ALL, 2), 0, LEAVES), jax.random.fold_in(seeds[7], 1), 0, LEAVES - 1).astype(jnp.int32)
    export_route_keys = jax.random.split(jax.random.fold_in(seeds[8], 1), EXPORTS_ALL // EXPORTS)
    export_route_turns = jax.random.permutation(jax.random.fold_in(seeds[8], 3), EXPORTS_ALL // EXPORTS)
    export_route = jax.vmap(lambda own, number: deal_out(jax.random.fold_in(seeds[8], 2), own, number, EXPORTS, N_DOM - 1, 1, MOST, 2))(export_route_keys, export_route_turns).reshape((EXPORTS_ALL, 1))
    return {"positions": positions, "smoothing": smoothing, "energy": energy, "mass": mass, "old_density": old_density, "active": active, "pair_list": pair_list, "export_leaves": export_leaves, "export_route": export_route}


ADIABATIC = 5.0 / 3.0
COURANT = 0.3

def kernel_value(dist, smooth):
    ratio = dist / smooth
    inner = 1.0 - 6.0 * ratio * ratio + 6.0 * ratio * ratio * ratio
    remain = jnp.maximum(1.0 - ratio, 0.0)
    outer = 2.0 * remain * remain * remain
    return jnp.where(ratio < 0.5, inner, outer) * (8.0 / math.pi) / (smooth * smooth * smooth)

def kernel_slope(dist, smooth):
    ratio = dist / smooth
    inner = -12.0 + 18.0 * ratio
    remain = jnp.maximum(1.0 - ratio, 0.0)
    outer = -6.0 * remain * remain / jnp.maximum(ratio, 0.5)
    square = smooth * smooth
    return jnp.where(ratio < 0.5, inner, outer) * (8.0 / math.pi) / (square * square * smooth)

def density_tile(own_pos, own_h, far_pos, far_mass):
    offset = own_pos[:, :, None] - far_pos[:, None, :]
    dist = jnp.sqrt(lax.optimization_barrier(jnp.sum(offset * offset, axis=0)))
    return lax.optimization_barrier(jnp.sum(kernel_value(dist, own_h[:, None]) * far_mass[None, :], axis=1))

def force_tile(own_pos, own_h, own_term, far_pos, far_h, far_mass, far_term):
    offset = own_pos[:, :, None] - far_pos[:, None, :]
    dist = jnp.sqrt(lax.optimization_barrier(jnp.sum(offset * offset, axis=0)))
    slope = 0.5 * (kernel_slope(dist, own_h[:, None]) + kernel_slope(dist, far_h[None, :]))
    weight = far_mass[None, :] * (own_term[:, None] + far_term[None, :]) * slope
    return -lax.optimization_barrier(jnp.sum(weight[None, :, :] * offset, axis=2))

def reference(positions, smoothing, energy, mass, old_density, active, pair_list, export_leaves, export_route):
    ranks = N_GRP * N_DOM
    device = jnp.arange(ranks, dtype=jnp.int32)
    pairs = pair_list.reshape(ranks, -1, 2)
    exports = export_leaves.reshape(ranks, -1, 2)
    routes = export_route.reshape(ranks, -1)
    within = device % N_DOM
    target_dev = (device - within)[:, None] + (within[:, None] + 1 + routes) % N_DOM
    base = (device * LEAVES)[:, None]
    own_leaf = jnp.concatenate([pairs[:, :, 0] + base, exports[:, :, 0] + base], axis=1).astype(jnp.int32)
    far_leaf = jnp.concatenate([pairs[:, :, 1] + base, exports[:, :, 1] + target_dev * LEAVES], axis=1).astype(jnp.int32)

    def density_rank(index):
        mine, theirs = index
        return jax.vmap(density_tile)(positions[mine], smoothing[mine], positions[theirs], mass[theirs])
    partial_value = lax.map(density_rank, (own_leaf, far_leaf))
    summed = jax.ops.segment_sum(partial_value.reshape(-1, LEAF), own_leaf.reshape(-1), num_segments=ranks * LEAVES)
    self_term = mass * kernel_value(jnp.zeros_like(smoothing), smoothing)
    density = jnp.where(active == 1, self_term + summed, old_density)
    term = (ADIABATIC - 1.0) * energy / density

    def force_rank(index):
        mine, theirs = index
        return jax.vmap(force_tile)(positions[mine], smoothing[mine], term[mine], positions[theirs], smoothing[theirs], mass[theirs], term[theirs])
    forces = lax.map(force_rank, (own_leaf, far_leaf))
    accel = jax.ops.segment_sum(forces.reshape(-1, 3, LEAF), own_leaf.reshape(-1), num_segments=ranks * LEAVES)
    acceleration = jnp.where((active == 1)[:, None, :], accel, 0.0)
    speed = jnp.sqrt(ADIABATIC * (ADIABATIC - 1.0) * energy)
    magnitude = jnp.sqrt(lax.optimization_barrier(jnp.sum(acceleration * acceleration, axis=1)))
    step_size = COURANT * smoothing / (speed + jnp.sqrt(smoothing * magnitude))
    timestep = jnp.min(jnp.where(active == 1, step_size, jnp.inf))
    return (density, acceleration, timestep)
```

```python
import math

import jax
import jax.numpy as jnp
from jax import lax
from jax.experimental import pallas as pl
from jax.experimental.pallas import tpu as pltpu
from jax.sharding import Mesh, PartitionSpec as P

ADIABATIC = 5.0 / 3.0
COURANT = 0.3
GROUP = 4
ROWS = 5
TINY = 1e-30
NORM = 8.0 / math.pi


def wide(ref, at, count):
    return ref[pl.ds(at, count), :]


def spread(out_ref, item, rows, leaves):
    width = rows.shape[1]
    turned = rows.T
    for leaf in range(leaves):
        out_ref[item, leaf] = jnp.broadcast_to(turned[:, leaf : leaf + 1], (width, width))


def separation(own_ref, own, far):
    dx = own_ref[0, own] - far[0]
    dy = own_ref[1, own] - far[1]
    dz = own_ref[2, own] - far[2]
    square = jnp.maximum(dx * dx + dy * dy + dz * dz, TINY)
    inverse = lax.rsqrt(square)
    return dx, dy, dz, square * inverse, inverse


def density_tile(own_ref, own, far):
    _, _, _, dist, _ = separation(own_ref, own, far)
    ratio = dist * own_ref[3, own]
    left = 1.0 - ratio
    inner = 1.0 - 6.0 * (ratio * ratio * left)
    remain = jnp.maximum(left, 0.0)
    outer = 2.0 * (remain * remain * remain)
    value = jnp.where(ratio < 0.5, inner, outer)
    return (jnp.sum(value * far[4], axis=1, keepdims=True),)


def slope(dist, inverse, smooth_inverse, smooth):
    ratio = dist * smooth_inverse
    remain = jnp.maximum(1.0 - ratio, 0.0)
    return jnp.where(ratio < 0.5, 3.0 * ratio - 2.0, -(remain * remain) * (smooth * inverse))


def force_tile(own_ref, own, far):
    dx, dy, dz, dist, inverse = separation(own_ref, own, far)
    mine = slope(dist, inverse, own_ref[3, own], own_ref[4, own]) * own_ref[5, own]
    theirs = slope(dist, inverse, far[5], far[3]) * far[6]
    weight = (mine + theirs) * (far[4] * (own_ref[6, own] + far[7]))
    return tuple(jnp.sum(weight * item, axis=1, keepdims=True) for item in (dx, dy, dz))


def tiles(count, entry, tile, acc_refs, own_ref, leaves):
    span = acc_refs[0].shape[1]
    for ref in acc_refs:
        ref[...] = jnp.zeros_like(ref)
    width = acc_refs[0].shape[0]
    lane = lax.broadcasted_iota(jnp.int32, (width, span), 1)
    short = lax.broadcasted_iota(jnp.int32, (1, span), 1)
    step = math.gcd(GROUP, count)

    def body(group, owners):
        for k in range(step):
            e = group * step + k
            own, far = entry(e)
            for ref, column in zip(acc_refs, tile(own_ref, own, far)):
                ref[...] = jnp.where(lane == e, column, ref[...])
            owners = jnp.where(short == e, own, owners)
        return owners

    owners = lax.fori_loop(0, count // step, body, jnp.full((1, span), -1, jnp.int32))
    leaf = lax.broadcasted_iota(jnp.int32, (leaves, span), 0)
    onehot = (leaf == owners).astype(jnp.float32)
    return [
        lax.dot_general(
            onehot,
            ref[...],
            (((1,), (1,)), ((), ())),
            precision=lax.Precision.HIGHEST,
            preferred_element_type=jnp.float32,
        )
        for ref in acc_refs
    ]


def local_entry(pair_ref, own_rows, leaves):
    def entry(e):
        own = pair_ref[e, 0]
        far = pair_ref[e, 1]
        return own, [wide(own_rows, c * leaves + far, 1) for c in range(own_rows.shape[0] // leaves)]

    return entry


def remote_entry(me_ref, leaf_ref, route_ref, near_ref, peer_ref, leaves, domains):
    me = me_ref[0]

    def entry(e):
        own = leaf_ref[e, 0]
        far = leaf_ref[e, 1]
        target = me + 1 + route_ref[e, 0]
        target = jnp.where(target >= domains, target - domains, target)
        chip = target // 2
        same = (target % 2) == (me % 2)
        rows = [
            jnp.where(
                same,
                near_ref[chip, pl.ds(c * leaves + far, 1), :],
                peer_ref[chip, pl.ds(c * leaves + far, 1), :],
            )
            for c in range(ROWS)
        ]
        return own, target, far, rows

    return entry


def slope_scale(h):
    square = h * h
    return (0.5 * NORM * 6.0) / (square * square * h)


def own_columns(out_ref, rows_ref, leaves, term=None):
    for c in range(3):
        spread(out_ref, c, rows_ref[pl.ds(c * leaves, leaves), :], leaves)
    h = rows_ref[pl.ds(3 * leaves, leaves), :]
    spread(out_ref, 3, 1.0 / h, leaves)
    if term is not None:
        spread(out_ref, 4, h, leaves)
        spread(out_ref, 5, slope_scale(h), leaves)
        spread(out_ref, 6, term, leaves)


def solution(mesh):
    groups, domains = mesh.shape["grp"], mesh.shape["dom"]
    chips = domains // 2
    fine = Mesh(mesh.devices.reshape(groups, chips, 2), ("grp", "chip", "core"))
    everyone = ("grp", "chip", "core")
    vmem = pl.BlockSpec(memory_space=pltpu.VMEM)
    smem = pl.BlockSpec(memory_space=pltpu.SMEM)

    def body(
        positions, smoothing, energy, mass, old_density, active, pair_list, export_leaves, export_route
    ):
        leaves, _, width = positions.shape
        pairs, exports = pair_list.shape[0], export_leaves.shape[0]
        local_span = -(-pairs // 128) * 128
        remote_span = -(-exports // 128) * 128
        f32 = jnp.float32
        sheet = jax.ShapeDtypeStruct((leaves, width), f32)
        me = (lax.axis_index("chip") * 2 + lax.axis_index("core")).astype(jnp.int32).reshape(1)
        own = jnp.concatenate(
            [positions.transpose(1, 0, 2).reshape(3 * leaves, width), smoothing, mass], axis=0
        )
        outgoing = jnp.broadcast_to(own[None], (chips,) + own.shape)
        near = lax.all_to_all(outgoing, "chip", split_axis=0, concat_axis=0, tiled=True)
        peer = lax.ppermute(near, "core", [(0, 1), (1, 0)])

        def local_density(pair_ref, own_ref, out_ref, cols, acc):
            own_columns(cols, own_ref, leaves)
            (total,) = tiles(
                pairs, local_entry(pair_ref, own_ref, leaves), density_tile, [acc], cols, leaves
            )
            out_ref[...] = total

        local_sum = pl.pallas_call(
            local_density,
            out_shape=sheet,
            in_specs=[smem, vmem],
            out_specs=vmem,
            scratch_shapes=[
                pltpu.VMEM((4, leaves, width, width), f32),
                pltpu.VMEM((width, local_span), f32),
            ],
            cost_estimate=pl.CostEstimate(
                flops=pairs * width * width * 30, bytes_accessed=65536, transcendentals=0
            ),
            name="local_density",
        )(pair_list, own)

        def remote_density(
            me_ref, leaf_ref, route_ref, own_ref, near_ref, peer_ref, local_ref, energy_ref,
            old_ref, active_ref, density_ref, term_ref, cols, acc
        ):
            own_columns(cols, own_ref, leaves)
            entry = remote_entry(me_ref, leaf_ref, route_ref, near_ref, peer_ref, leaves, domains)

            def pick(e):
                mine, _, _, rows = entry(e)
                return mine, rows

            (total,) = tiles(exports, pick, density_tile, [acc], cols, leaves)
            h = own_ref[pl.ds(3 * leaves, leaves), :]
            scale = NORM / (h * h * h)
            summed = (local_ref[...] + total + own_ref[pl.ds(4 * leaves, leaves), :]) * scale
            density = jnp.where(active_ref[...] == 1, summed, old_ref[...])
            density_ref[...] = density
            term_ref[...] = (ADIABATIC - 1.0) * energy_ref[...] / density

        density, term = pl.pallas_call(
            remote_density,
            out_shape=(sheet, sheet),
            in_specs=[smem, smem, smem] + [vmem] * 7,
            out_specs=(vmem, vmem),
            scratch_shapes=[
                pltpu.VMEM((4, leaves, width, width), f32),
                pltpu.VMEM((width, remote_span), f32),
            ],
            cost_estimate=pl.CostEstimate(
                flops=exports * width * width * 30, bytes_accessed=65536, transcendentals=0
            ),
            name="remote_density",
        )(me, export_leaves, export_route, own, near, peer, local_sum, energy, old_density, active)

        terms = lax.all_to_all(
            jnp.broadcast_to(term[None], (domains,) + term.shape),
            ("chip", "core"),
            split_axis=0,
            concat_axis=0,
            tiled=True,
        )

        def local_force(pair_ref, own_ref, term_ref, out_ref, cols, ax, ay, az):
            own_columns(cols, own_ref, leaves, term_ref[...])
            h = own_ref[pl.ds(3 * leaves, leaves), :]
            out_ref[0] = 1.0 / h
            out_ref[1] = slope_scale(h)

            def entry(e):
                mine = pair_ref[e, 0]
                far = pair_ref[e, 1]
                rows = [wide(own_ref, c * leaves + far, 1) for c in range(ROWS)]
                rows += [out_ref[c, pl.ds(far, 1), :] for c in range(2)]
                rows.append(wide(term_ref, far, 1))
                return mine, rows

            totals = tiles(pairs, entry, force_tile, [ax, ay, az], cols, leaves)
            for c in range(3):
                out_ref[c] = totals[c]

        local_accel = pl.pallas_call(
            local_force,
            out_shape=jax.ShapeDtypeStruct((3, leaves, width), f32),
            in_specs=[smem, vmem, vmem],
            out_specs=vmem,
            scratch_shapes=[pltpu.VMEM((7, leaves, width, width), f32)]
            + [pltpu.VMEM((width, local_span), f32)] * 3,
            cost_estimate=pl.CostEstimate(
                flops=pairs * width * width * 60, bytes_accessed=65536, transcendentals=0
            ),
            name="local_force",
        )(pair_list, own, term)

        members = groups * domains

        def remote_force(
            me_ref, leaf_ref, route_ref, own_ref, near_ref, peer_ref, term_ref, terms_ref,
            local_ref, energy_ref, active_ref, accel_ref, least_ref, cols, ax, ay, az
        ):
            own_columns(cols, own_ref, leaves, term_ref[...])
            entry = remote_entry(me_ref, leaf_ref, route_ref, near_ref, peer_ref, leaves, domains)

            def pick(e):
                mine, target, far, rows = entry(e)
                h = rows[3]
                rows = rows + [1.0 / h, slope_scale(h), terms_ref[target, pl.ds(far, 1), :]]
                return mine, rows

            totals = tiles(exports, pick, force_tile, [ax, ay, az], cols, leaves)
            awake = active_ref[...] == 1
            square = jnp.zeros((leaves, width), f32)
            for c in range(3):
                part = jnp.where(awake, -(local_ref[c] + totals[c]), 0.0)
                accel_ref[c] = part
                square = square + part * part
            h = own_ref[pl.ds(3 * leaves, leaves), :]
            speed = jnp.sqrt(ADIABATIC * (ADIABATIC - 1.0) * energy_ref[...])
            step = COURANT * h / (speed + jnp.sqrt(h * jnp.sqrt(square)))
            least_ref[...] = jnp.full(
                (members, width), jnp.min(jnp.where(awake, step, jnp.inf)), f32
            )

        accel, least = pl.pallas_call(
            remote_force,
            out_shape=(
                jax.ShapeDtypeStruct((3, leaves, width), f32),
                jax.ShapeDtypeStruct((members, width), f32),
            ),
            in_specs=[smem, smem, smem] + [vmem] * 8,
            out_specs=(vmem, vmem),
            scratch_shapes=[pltpu.VMEM((7, leaves, width, width), f32)]
            + [pltpu.VMEM((width, remote_span), f32)] * 3,
            cost_estimate=pl.CostEstimate(
                flops=exports * width * width * 60, bytes_accessed=65536, transcendentals=0
            ),
            name="remote_force",
        )(me, export_leaves, export_route, own, near, peer, term, terms, local_accel, energy, active)

        everywhere = lax.all_to_all(least, everyone, split_axis=0, concat_axis=0, tiled=True)
        return density, accel.transpose(1, 0, 2), jnp.min(everywhere)

    flat = P(everyone, None)
    deep = P(everyone, None, None)
    return jax.shard_map(
        body,
        mesh=fine,
        in_specs=(deep,) + (flat,) * 8,
        out_specs=(flat, deep, P()),
        check_vma=False,
    )
```

```python
import math

import jax
import jax.numpy as jnp
from jax import lax
from jax.experimental import pallas as pl
from jax.experimental.pallas import tpu as pltpu
from jax.sharding import Mesh, PartitionSpec as P

ADIABATIC = 5.0 / 3.0
COURANT = 0.3
GROUP = 4
TINY = 1e-30
NORM = 8.0 / math.pi
MIB = 1 << 20


def turn(rows):
    width = rows[0].shape[1]
    rows = list(rows) + [jnp.zeros_like(rows[0])] * (-len(rows) % 8)
    turned = jnp.concatenate(rows, axis=0).T
    return [jnp.broadcast_to(turned[:, k : k + 1], (width, width)) for k in range(len(rows))]


def separation(own, far):
    offset = [own[c] - far[c] for c in range(3)]
    square = offset[0] * offset[0] + offset[1] * offset[1] + offset[2] * offset[2]
    square = jnp.maximum(square, TINY)
    inverse = lax.rsqrt(square)
    return offset, square * inverse, inverse


def density_tile(own, far):
    far = turn(far)
    _, dist, _ = separation(own, far)
    ratio = dist * own[3]
    left = 1.0 - ratio
    inner = 1.0 - 6.0 * (ratio * ratio * left)
    remain = jnp.maximum(left, 0.0)
    outer = 2.0 * (remain * remain * remain)
    value = jnp.where(ratio < 0.5, inner, outer)
    return jnp.sum(value * far[3], axis=0, keepdims=True)


def slope(dist, smooth_inverse, scale):
    ratio = dist * smooth_inverse
    remain = jnp.maximum(1.0 - ratio, 0.0)
    return jnp.where(ratio < 0.5, ratio * (2.0 - 3.0 * ratio), remain * remain) * scale


def force_tile(own, far):
    offset, dist, inverse = separation(own, far)
    both = slope(dist, own[3], own[4]) + slope(dist, far[3], far[4])
    return offset, (inverse * far[5]) * both


def slope_scale(h):
    square = h * h
    return (3.0 * NORM) / (square * square)


def grouped(count, body):
    step = math.gcd(GROUP, count)

    def run(group, carry):
        for k in range(step):
            body(group * step + k)
        return carry

    lax.fori_loop(0, count // step, run, 0)


def row(ref, at):
    return ref[pl.ds(at, 1), :]


def add_row(ref, at, value):
    ref[pl.ds(at, 1), :] = ref[pl.ds(at, 1), :] + value


def solution(mesh):
    groups, domains = mesh.shape["grp"], mesh.shape["dom"]
    chips = domains // 2
    fine = Mesh(mesh.devices.reshape(groups, chips, 2), ("grp", "chip", "core"))
    everyone = ("grp", "chip", "core")
    members = groups * domains
    vmem = pl.BlockSpec(memory_space=pltpu.VMEM)
    smem = pl.BlockSpec(memory_space=pltpu.SMEM)

    def call(kernel, name, outs, ins, scratch, flops, mib):
        return pl.pallas_call(
            kernel,
            out_shape=outs,
            in_specs=ins,
            out_specs=jax.tree.map(lambda _: vmem, outs),
            scratch_shapes=scratch,
            cost_estimate=pl.CostEstimate(flops=flops, bytes_accessed=1 << 16, transcendentals=0),
            compiler_params=pltpu.CompilerParams(vmem_limit_bytes=mib * MIB),
            name=name,
        )

    def body(
        positions, smoothing, energy, mass, old_density, active, pair_list, export_leaves, export_route
    ):
        leaves, _, width = positions.shape
        pairs, exports = pair_list.shape[0], export_leaves.shape[0]
        f32 = jnp.float32

        def shape(*sizes):
            return jax.ShapeDtypeStruct(sizes, f32)

        place = positions.transpose(1, 0, 2)
        pair_list, export_leaves, export_route = pair_list.T, export_leaves.T, export_route.T
        own = jnp.concatenate([place.reshape(3 * leaves, width), smoothing, mass], axis=0)
        outgoing = jnp.broadcast_to(own[None], (chips,) + own.shape)
        near = lax.all_to_all(outgoing, "chip", split_axis=0, concat_axis=0, tiled=True)

        def local_density(pair_ref, place_ref, h_ref, mass_ref, out_ref, inverse):
            inverse[...] = 1.0 / h_ref[...]
            out_ref[...] = jnp.zeros_like(out_ref)

            def tile(e):
                mine, other = pair_ref[0, e], pair_ref[1, e]
                own_rows = [row(place_ref.at[c], mine) for c in range(3)] + [row(inverse, mine)]
                far_rows = [row(place_ref.at[c], other) for c in range(3)] + [row(mass_ref, other)]
                add_row(out_ref, mine, density_tile(own_rows, far_rows))

            grouped(pairs, tile)

        local_sum = call(
            local_density, "local_density", shape(leaves, width), [smem] + [vmem] * 3,
            [pltpu.VMEM((leaves, width), f32)], pairs * width * width * 30, 4,
        )(pair_list, place, smoothing, mass)
        near, local_sum = lax.optimization_barrier((near, local_sum))
        peer = lax.ppermute(near, "core", [(0, 1), (1, 0)])

        def export(leaf_ref, route_ref, near_ref, peer_ref, e, items):
            core = lax.axis_index("core")
            me = lax.axis_index("chip") * 2 + core
            other = leaf_ref[1, e]
            target = me + 1 + route_ref[0, e]
            target = jnp.where(target >= domains, target - domains, target)
            chip = target // 2
            same = (target - chip * 2) == core
            rows = [
                jnp.where(
                    same,
                    near_ref[chip, pl.ds(c * leaves + other, 1), :],
                    peer_ref[chip, pl.ds(c * leaves + other, 1), :],
                )
                for c in items
            ]
            return leaf_ref[0, e], target, other, rows

        def remote_density(
            leaf_ref, route_ref, place_ref, h_ref, mass_ref, near_ref, peer_ref, local_ref,
            energy_ref, old_ref, active_ref, density_ref, term_ref, spread_ref, inverse, total
        ):
            inverse[...] = 1.0 / h_ref[...]
            total[...] = local_ref[...]

            def tile(e):
                mine, _, _, far = export(leaf_ref, route_ref, near_ref, peer_ref, e, (0, 1, 2, 4))
                own_rows = [row(place_ref.at[c], mine) for c in range(3)] + [row(inverse, mine)]
                add_row(total, mine, density_tile(own_rows, far))

            grouped(exports, tile)
            h = h_ref[...]
            summed = (total[...] + mass_ref[...]) * (NORM / (h * h * h))
            density = jnp.where(active_ref[...] == 1, summed, old_ref[...])
            term = (ADIABATIC - 1.0) * energy_ref[...] / density
            density_ref[...] = density
            term_ref[...] = term
            for d in range(domains):
                spread_ref[d] = term

        density, term, outgoing = call(
            remote_density,
            "remote_density",
            (shape(leaves, width), shape(leaves, width), shape(domains, leaves, width)),
            [smem, smem] + [vmem] * 9,
            [pltpu.VMEM((leaves, width), f32)] * 2,
            exports * width * width * 30,
            4 + 2 * domains * leaves * width * 32 // MIB,
        )(
            export_leaves, export_route, place, smoothing, mass, near, peer, local_sum, energy,
            old_density, active,
        )
        terms = lax.all_to_all(
            outgoing, ("chip", "core"), split_axis=0, concat_axis=0, tiled=True
        )

        def prepare(
            pair_ref, leaf_ref, route_ref, place_ref, h_ref, mass_ref, near_ref, peer_ref,
            term_ref, sum_ref, weight_ref, inverse, scale, still
        ):
            inverse[...] = 1.0 / h_ref[...]
            scale[...] = slope_scale(h_ref[...])
            sum_ref[...] = jnp.zeros_like(sum_ref)
            still[...] = jnp.zeros_like(still)

            def mine_rows(mine):
                return [row(place_ref.at[c], mine) for c in range(3)] + [
                    row(inverse, mine),
                    row(scale, mine),
                ]

            def local_tile(e):
                mine, other = pair_ref[0, e], pair_ref[1, e]
                far = mine_rows(other) + [row(mass_ref, other), row(term_ref, other)]
                far = turn(far)
                offset, weight = force_tile(mine_rows(mine), far)
                weight = weight * (row(term_ref, mine) + far[6])
                for c in range(3):
                    part = jnp.sum(weight * offset[c], axis=0, keepdims=True)
                    add_row(sum_ref.at[c], mine, part)

            def remote_tile(e):
                mine, _, _, far = export(leaf_ref, route_ref, near_ref, peer_ref, e, (0, 1, 2, 3, 4))
                h = far[3]
                far = turn(far[:3] + [1.0 / h, slope_scale(h), far[4]])
                offset, weight = force_tile(mine_rows(mine), far)
                for c in range(3):
                    part = weight * offset[c]
                    weight_ref[e, c] = part
                    add_row(still.at[c], mine, jnp.sum(part, axis=0, keepdims=True))

            grouped(pairs, local_tile)
            grouped(exports, remote_tile)
            for c in range(3):
                sum_ref[c] = sum_ref[c] + term_ref[...] * still[c]

        stash = shape(exports, 3, width, width)
        stash_mib = exports * 3 * width * width * 4 // MIB + 1
        partial, weights = call(
            prepare,
            "prepare_force",
            (shape(3, leaves, width), stash),
            [smem] * 3 + [vmem] * 6,
            [pltpu.VMEM((leaves, width), f32)] * 2 + [pltpu.VMEM((3, leaves, width), f32)],
            (pairs + exports) * width * width * 60,
            6 + stash_mib + 2 * domains * leaves * width * 32 // MIB,
        )(
            pair_list, export_leaves, export_route, place, smoothing, mass, near, peer, term
        )

        def finish(
            leaf_ref, route_ref, h_ref, terms_ref, partial_ref, weight_ref, energy_ref, active_ref,
            accel_ref, least_ref, total
        ):
            total[...] = partial_ref[...]
            me = lax.axis_index("chip") * 2 + lax.axis_index("core")
            for first in range(0, exports, 8):
                many = min(8, exports - first)
                rows = []
                for e in range(first, first + many):
                    target = me + 1 + route_ref[0, e]
                    target = jnp.where(target >= domains, target - domains, target)
                    rows.append(terms_ref[target, pl.ds(leaf_ref[1, e], 1), :])
                columns = turn(rows)
                for k in range(many):
                    mine = leaf_ref[0, first + k]
                    for c in range(3):
                        part = weight_ref[first + k, c] * columns[k]
                        add_row(total.at[c], mine, jnp.sum(part, axis=0, keepdims=True))
            awake = active_ref[...] == 1
            square = jnp.zeros((leaves, width), f32)
            for c in range(3):
                part = jnp.where(awake, total[c], 0.0)
                accel_ref[c] = part
                square = square + part * part
            h = h_ref[...]
            speed = jnp.sqrt(ADIABATIC * (ADIABATIC - 1.0) * energy_ref[...])
            step = COURANT * h / (speed + jnp.sqrt(h * jnp.sqrt(square)))
            least_ref[...] = jnp.full(
                (members, width), jnp.min(jnp.where(awake, step, jnp.inf)), f32
            )

        accel, least = call(
            finish,
            "finish_force",
            (shape(3, leaves, width), shape(members, width)),
            [smem, smem] + [vmem] * 6,
            [pltpu.VMEM((3, leaves, width), f32)],
            exports * width * width * 6,
            4 + stash_mib + 2 * domains * leaves * width * 4 // MIB,
        )(export_leaves, export_route, smoothing, terms, partial, weights, energy, active)

        everywhere = lax.all_to_all(least, everyone, split_axis=0, concat_axis=0, tiled=True)
        return density, accel.transpose(1, 0, 2), jnp.min(everywhere)

    flat = P(everyone, None)
    deep = P(everyone, None, None)
    return jax.shard_map(
        body,
        mesh=fine,
        in_specs=(deep,) + (flat,) * 8,
        out_specs=(flat, deep, P()),
        check_vma=False,
    )
```

```python
import math

import jax
import jax.numpy as jnp
from jax import lax
from jax.experimental import pallas as pl
from jax.experimental.pallas import tpu as pltpu
from jax.sharding import Mesh, PartitionSpec as P

ADIABATIC = 5.0 / 3.0
COURANT = 0.3
GROUP = 4
TINY = 1e-30
NORM = 8.0 / math.pi
MIB = 1 << 20
X, MASS, H, INVERSE, SCALE, ORIGIN, ENERGY, OLD, ACTIVE, SUM, TABLE = 0, 3, 4, 5, 6, 7, 10, 11, 12, 13, 14


def product(a, b, dims):
    return lax.dot_general(
        a, b, (dims, ((), ())), precision=lax.Precision.HIGHEST, preferred_element_type=jnp.float32
    )


def turn(rows):
    width, count = rows[0].shape[1], len(rows)
    rows = list(rows) + [jnp.zeros_like(rows[0])] * (-count % 8)
    turned = jnp.concatenate(rows, axis=0).T
    return [jnp.broadcast_to(turned[:, k : k + 1], (width, width)) for k in range(count)]


def separation(right, place):
    norm = place[0] * place[0] + place[1] * place[1] + place[2] * place[2]
    zero = jnp.zeros_like(norm)
    left = jnp.concatenate(place + [norm, jnp.ones_like(norm), zero, zero, zero], axis=0)
    square = jnp.maximum(product(left, right, ((0,), (0,))), TINY)
    inverse = lax.rsqrt(square)
    return square * inverse, inverse


def density_tile(right, own_inverse, place, mass):
    (mass,) = turn([mass])
    dist, _ = separation(right, place)
    ratio = dist * own_inverse
    left = 1.0 - ratio
    inner = 1.0 - 6.0 * (ratio * ratio * left)
    remain = jnp.maximum(left, 0.0)
    outer = 2.0 * (remain * remain * remain)
    value = jnp.where(ratio < 0.5, inner, outer)
    return jnp.sum(value * mass, axis=0, keepdims=True)


def slope(dist, smooth_inverse, scale):
    ratio = dist * smooth_inverse
    remain = jnp.maximum(1.0 - ratio, 0.0)
    return jnp.where(ratio < 0.5, ratio * (2.0 - 3.0 * ratio), remain * remain) * scale


def weight_tile(right, own_inverse, own_scale, place, inverse, scale):
    inverse, scale = turn([inverse, scale])
    dist, over = separation(right, place)
    return over * (slope(dist, own_inverse, own_scale) + slope(dist, inverse, scale))


def moments(mass, place):
    half = [mass] + [mass * item for item in place]
    return jnp.concatenate(half + half, axis=0)


def force(weights, rows, far_term, own_term, own_place):
    item = lax.broadcasted_iota(jnp.int32, rows.shape, 0)
    rows = jnp.where(item < 4, rows, rows * far_term)
    sums = product(rows, weights, ((1,), (0,)))
    sums = own_term * sums[:4] + sums[4:]
    return own_place[:4] * sums[:1] - sums


def slope_scale(h):
    square = h * h
    return (3.0 * NORM) / (square * square)


def grouped(count, body):
    step = math.gcd(GROUP, count)

    def run(group, carry):
        for k in range(step):
            body(group * step + k)
        return carry

    lax.fori_loop(0, count // step, run, 0)


def fetch(sems, *pairs):
    copies = [pltpu.make_async_copy(a, b, sems.at[i]) for i, (a, b) in enumerate(pairs)]
    for copy in copies:
        copy.start()
    for copy in copies:
        copy.wait()


def solution(mesh):
    groups, domains = mesh.shape["grp"], mesh.shape["dom"]
    chips = domains // 2
    fine = Mesh(mesh.devices.reshape(groups, chips, 2), ("grp", "chip", "core"))
    everyone = ("grp", "chip", "core")
    members = groups * domains
    vmem = pl.BlockSpec(memory_space=pltpu.VMEM)
    hbm = pl.BlockSpec(memory_space=pltpu.HBM)

    def call(kernel, name, outs, ins, scratch, flops, mib):
        return pl.pallas_call(
            kernel,
            out_shape=outs,
            in_specs=ins,
            out_specs=jax.tree.map(lambda _: vmem, outs),
            scratch_shapes=scratch,
            cost_estimate=pl.CostEstimate(flops=flops, bytes_accessed=1 << 16, transcendentals=0),
            compiler_params=pltpu.CompilerParams(vmem_limit_bytes=mib * MIB),
            name=name,
        )

    def body(
        positions, smoothing, energy, mass, old_density, active, pair_list, export_leaves, export_route
    ):
        leaves, _, width = positions.shape
        pairs, exports = pair_list.shape[0], export_leaves.shape[0]
        f32, s32 = jnp.float32, jnp.int32
        tile_flops = width * width

        def shape(*sizes):
            return jax.ShapeDtypeStruct(sizes, f32)

        place = positions.transpose(1, 0, 2)
        pair_list, export_leaves, export_route = pair_list.T, export_leaves.T, export_route.T
        pair_table, leaf_table = pltpu.SMEM((2, pairs), s32), pltpu.SMEM((2, exports), s32)
        route_table = pltpu.SMEM((1, exports), s32)

        outgoing = jnp.concatenate(
            [
                jnp.broadcast_to(item[None], (chips,) + item.shape)
                for item in (place.reshape(3 * leaves, width), smoothing, mass)
            ],
            axis=1,
        )
        near = lax.all_to_all(outgoing, "chip", split_axis=0, concat_axis=0, tiled=True)

        def row(own_ref, item, leaf):
            return own_ref[item, pl.ds(leaf, 1), :]

        def local_place(own_ref, mine, other):
            return [row(own_ref, X + c, other) - row(own_ref, ORIGIN + c, mine) for c in range(3)]

        def local_density(
            pair_hbm, place_hbm, h_hbm, mass_hbm, energy_hbm, old_hbm, active_hbm, own_ref, right_ref,
            centred_ref, pair_ref, active_ref, sems
        ):
            fetch(
                sems,
                (pair_hbm, pair_ref),
                (place_hbm, own_ref.at[pl.ds(X, 3)]),
                (h_hbm, own_ref.at[H]),
                (mass_hbm, own_ref.at[MASS]),
                (energy_hbm, own_ref.at[ENERGY]),
                (old_hbm, own_ref.at[OLD]),
                (active_hbm, active_ref),
            )
            h = own_ref[H]
            own_ref[ACTIVE] = active_ref[...].astype(f32)
            own_ref[INVERSE] = 1.0 / h
            own_ref[SCALE] = slope_scale(h)
            own_ref[SUM] = jnp.zeros_like(h)
            norm = jnp.zeros_like(h)
            centred = []
            for c in range(3):
                mean = jnp.sum(own_ref[X + c], axis=1, keepdims=True) * (1.0 / width)
                mean = jnp.broadcast_to(mean, h.shape)
                own_ref[ORIGIN + c] = mean
                item = own_ref[X + c] - mean
                norm = norm + item * item
                centred.append(item)
            zero, one = jnp.zeros_like(h), jnp.ones_like(h)
            rights = [-2.0 * item for item in centred] + [one, norm, zero, zero, zero]
            places = [zero] + centred + [zero] * 4
            for k in range(8):
                for leaf in range(leaves):
                    right_ref[leaf, k : k + 1, :] = rights[k][leaf : leaf + 1]
                    centred_ref[leaf, k : k + 1, :] = places[k][leaf : leaf + 1]

            def tile(e):
                mine, other = pair_ref[0, e], pair_ref[1, e]
                own_ref[SUM, pl.ds(mine, 1), :] = row(own_ref, SUM, mine) + density_tile(
                    right_ref[mine],
                    row(own_ref, INVERSE, mine),
                    local_place(own_ref, mine, other),
                    row(own_ref, MASS, other),
                )

            grouped(pairs, tile)

        own, right, centred = call(
            local_density,
            "local_density",
            (shape(TABLE, leaves, width), shape(leaves, 8, width), shape(leaves, 8, width)),
            [hbm] * 7,
            [pair_table, pltpu.VMEM((leaves, width), s32), pltpu.SemaphoreType.DMA((7,))],
            pairs * tile_flops * 30,
            4,
        )(pair_list, place, smoothing, mass, energy, old_density, active)
        near, own = lax.optimization_barrier((near, own))
        peer = lax.ppermute(near, "core", [(0, 1), (1, 0)])

        def export(leaf_ref, route_ref, near_ref, peer_ref, own_ref, e, items):
            core = lax.axis_index("core")
            me = lax.axis_index("chip") * 2 + core
            mine, other = leaf_ref[0, e], leaf_ref[1, e]
            target = me + 1 + route_ref[0, e]
            target = jnp.where(target >= domains, target - domains, target)
            chip = target // 2
            same = (target - chip * 2) == core

            def get(c):
                at = pl.ds(c * leaves + other, 1)
                return jnp.where(same, near_ref[chip, at, :], peer_ref[chip, at, :])

            spot = [get(c) - row(own_ref, ORIGIN + c, mine) for c in range(3)]
            return mine, spot, [get(c) for c in items]

        def remote_density(
            leaf_hbm, route_hbm, own_ref, right_ref, near_ref, peer_ref, density_ref, term_ref,
            spread_ref, total, leaf_ref, route_ref, sems
        ):
            fetch(sems, (leaf_hbm, leaf_ref), (route_hbm, route_ref))
            total[...] = own_ref[SUM]

            def tile(e):
                mine, spot, (far_mass,) = export(
                    leaf_ref, route_ref, near_ref, peer_ref, own_ref, e, (4,)
                )
                at = pl.ds(mine, 1)
                total[at, :] = total[at, :] + density_tile(
                    right_ref[mine], row(own_ref, INVERSE, mine), spot, far_mass
                )

            grouped(exports, tile)
            inverse = own_ref[INVERSE]
            summed = (total[...] + own_ref[MASS]) * (NORM * (inverse * inverse * inverse))
            density = jnp.where(own_ref[ACTIVE] == 1.0, summed, own_ref[OLD])
            term = (ADIABATIC - 1.0) * own_ref[ENERGY] / density
            density_ref[...] = density
            term_ref[...] = term
            for d in range(domains):
                spread_ref[d] = term

        wire_mib = 2 * domains * leaves * width * 20 // MIB
        density, term, outgoing = call(
            remote_density,
            "remote_density",
            (shape(leaves, width), shape(leaves, width), shape(domains, leaves, width)),
            [hbm] * 2 + [vmem] * 4,
            [pltpu.VMEM((leaves, width), f32), leaf_table, route_table, pltpu.SemaphoreType.DMA((2,))],
            exports * tile_flops * 30,
            6 + wire_mib,
        )(export_leaves, export_route, own, right, near, peer)
        terms = lax.all_to_all(outgoing, ("chip", "core"), split_axis=0, concat_axis=0, tiled=True)

        def prepare(
            pair_hbm, leaf_hbm, route_hbm, own_ref, right_ref, centred_ref, near_ref, peer_ref,
            term_ref, sum_ref, weight_ref, moment_ref, pair_ref, leaf_ref, route_ref, sems
        ):
            fetch(sems, (pair_hbm, pair_ref), (leaf_hbm, leaf_ref), (route_hbm, route_ref))
            sum_ref[...] = jnp.zeros_like(sum_ref)

            def weigh(mine, spot, inverse, scale):
                return weight_tile(
                    right_ref[mine],
                    row(own_ref, INVERSE, mine),
                    row(own_ref, SCALE, mine),
                    spot,
                    inverse,
                    scale,
                )

            def local_tile(e):
                mine, other = pair_ref[0, e], pair_ref[1, e]
                spot = local_place(own_ref, mine, other)
                weights = weigh(mine, spot, row(own_ref, INVERSE, other), row(own_ref, SCALE, other))
                rows = moments(row(own_ref, MASS, other), spot)
                far_term, own_term = term_ref[pl.ds(other, 1), :], term_ref[pl.ds(mine, 1), :]
                sum_ref[mine] = sum_ref[mine] + force(
                    weights, rows, far_term, own_term, centred_ref[mine]
                )

            def remote_tile(e):
                mine, spot, (h, far_mass) = export(
                    leaf_ref, route_ref, near_ref, peer_ref, own_ref, e, (3, 4)
                )
                weight_ref[e] = weigh(mine, spot, 1.0 / h, slope_scale(h))
                moment_ref[e] = moments(far_mass, spot)

            grouped(pairs, local_tile)
            grouped(exports, remote_tile)

        stash_mib = 2 * exports * width * (width + 8) * 4 // MIB
        partial, weights, rows = call(
            prepare,
            "prepare_force",
            (shape(leaves, 4, width), shape(exports, width, width), shape(exports, 8, width)),
            [hbm] * 3 + [vmem] * 6,
            [pair_table, leaf_table, route_table, pltpu.SemaphoreType.DMA((3,))],
            (pairs + exports) * tile_flops * 60,
            6 + stash_mib + wire_mib,
        )(pair_list, export_leaves, export_route, own, right, centred, near, peer, term)

        def finish(
            leaf_hbm, route_hbm, own_ref, centred_ref, term_ref, terms_ref, partial_ref, weight_ref,
            moment_ref, accel_ref, least_ref, total, leaf_ref, route_ref, sems
        ):
            fetch(sems, (leaf_hbm, leaf_ref), (route_hbm, route_ref))
            total[...] = partial_ref[...]
            me = lax.axis_index("chip") * 2 + lax.axis_index("core")

            def tile(e):
                mine, other = leaf_ref[0, e], leaf_ref[1, e]
                target = me + 1 + route_ref[0, e]
                target = jnp.where(target >= domains, target - domains, target)
                far_term = terms_ref[target, pl.ds(other, 1), :]
                total[mine] = total[mine] + force(
                    weight_ref[e],
                    moment_ref[e],
                    far_term,
                    term_ref[pl.ds(mine, 1), :],
                    centred_ref[mine],
                )

            grouped(exports, tile)
            for c in range(3):
                for leaf in range(leaves):
                    accel_ref[c, leaf : leaf + 1, :] = total[leaf, c + 1 : c + 2, :]
            awake = own_ref[ACTIVE] == 1.0
            square = jnp.zeros((leaves, width), f32)
            for c in range(3):
                part = jnp.where(awake, accel_ref[c], 0.0)
                accel_ref[c] = part
                square = square + part * part
            h = own_ref[H]
            speed = jnp.sqrt(ADIABATIC * (ADIABATIC - 1.0) * own_ref[ENERGY])
            step = COURANT * h / (speed + jnp.sqrt(h * jnp.sqrt(square)))
            least_ref[...] = jnp.full(
                (members, width), jnp.min(jnp.where(awake, step, jnp.inf)), f32
            )

        accel, least = call(
            finish,
            "finish_force",
            (shape(3, leaves, width), shape(members, width)),
            [hbm] * 2 + [vmem] * 7,
            [pltpu.VMEM((leaves, 4, width), f32), leaf_table, route_table, pltpu.SemaphoreType.DMA((2,))],
            exports * tile_flops * 16,
            6 + stash_mib + wire_mib,
        )(export_leaves, export_route, own, centred, term, terms, partial, weights, rows)

        everywhere = lax.all_to_all(least, everyone, split_axis=0, concat_axis=0, tiled=True)
        return density, accel.transpose(1, 0, 2), jnp.min(everywhere)

    flat = P(everyone, None)
    deep = P(everyone, None, None)
    return jax.shard_map(
        body,
        mesh=fine,
        in_specs=(deep,) + (flat,) * 8,
        out_specs=(flat, deep, P()),
        check_vma=False,
    )
```

```python
import math

import jax
import jax.numpy as jnp
from jax import lax
from jax.experimental import pallas as pl
from jax.experimental.pallas import tpu as pltpu
from jax.sharding import Mesh, PartitionSpec as P

ADIABATIC = 5.0 / 3.0
COURANT = 0.3
GROUP = 4
TINY = 1e-30
NORM = 8.0 / math.pi
MIB = 1 << 20
X, MASS, H, INVERSE, SCALE, ORIGIN, ENERGY, OLD, ACTIVE, SUM, TABLE = 0, 3, 4, 5, 6, 7, 10, 11, 12, 13, 14


def split(item):
    first = item.astype(jnp.bfloat16).astype(jnp.float32)
    rest = item - first
    second = rest.astype(jnp.bfloat16).astype(jnp.float32)
    return first, second, rest - second


def product(a, b, dims):
    return lax.dot_general(a, b, (dims, ((), ())), preferred_element_type=jnp.float32)


def left_terms(item):
    first, second, third = split(item)
    return jnp.concatenate([first, first, second, first, third, second], axis=0).astype(jnp.bfloat16)


def right_terms(item):
    first, second, third = split(item)
    return jnp.concatenate([first, second, first, third, first, second], axis=0).astype(jnp.bfloat16)


def turn(rows):
    width, count = rows[0].shape[1], len(rows)
    rows = list(rows) + [jnp.zeros_like(rows[0])] * (-count % 8)
    turned = jnp.concatenate(rows, axis=0).T
    return [jnp.broadcast_to(turned[:, k : k + 1], (width, width)) for k in range(count)]


def separation(right, place):
    norm = place[0] * place[0] + place[1] * place[1] + place[2] * place[2]
    zero = jnp.zeros_like(norm)
    left = jnp.concatenate(place + [norm, jnp.ones_like(norm), zero, zero, zero], axis=0)
    square = jnp.maximum(product(left_terms(left), right, ((0,), (0,))), TINY)
    inverse = lax.rsqrt(square)
    return square * inverse, inverse


def density_tile(right, own_inverse, place, mass):
    (mass,) = turn([mass])
    dist, _ = separation(right, place)
    ratio = dist * own_inverse
    left = 1.0 - ratio
    inner = 1.0 - 6.0 * (ratio * ratio * left)
    remain = jnp.maximum(left, 0.0)
    outer = 2.0 * (remain * remain * remain)
    value = jnp.where(ratio < 0.5, inner, outer)
    return jnp.sum(value * mass, axis=0, keepdims=True)


def slope(dist, smooth_inverse, scale):
    ratio = dist * smooth_inverse
    remain = jnp.maximum(1.0 - ratio, 0.0)
    return jnp.where(ratio < 0.5, ratio * (2.0 - 3.0 * ratio), remain * remain) * scale


def weight_tile(right, own_inverse, own_scale, place, inverse, scale):
    inverse, scale = turn([inverse, scale])
    dist, over = separation(right, place)
    return over * (slope(dist, own_inverse, own_scale) + slope(dist, inverse, scale))


def moments(mass, place):
    half = [mass] + [mass * item for item in place]
    return jnp.concatenate(half + half, axis=0)


def force(weights, rows, far_term, own_term, own_place):
    item = lax.broadcasted_iota(jnp.int32, rows.shape, 0)
    rows = jnp.where(item < 4, rows, rows * far_term)
    rows = jnp.concatenate(split(rows), axis=0).astype(jnp.bfloat16)
    sums = product(jnp.concatenate([rows, rows, rows], axis=1), weights, ((1,), (0,)))
    sums = sums[:8] + sums[8:16] + sums[16:]
    sums = own_term * sums[:4] + sums[4:]
    return own_place[:4] * sums[:1] - sums


def stack(weights):
    return jnp.concatenate([part.astype(jnp.bfloat16) for part in split(weights)], axis=0)


def slope_scale(h):
    square = h * h
    return (3.0 * NORM) / (square * square)


def grouped(count, body, group=GROUP):
    step = math.gcd(group, count)

    def run(group, carry):
        for k in range(step):
            body(group * step + k)
        return carry

    lax.fori_loop(0, count // step, run, 0)


def fetch(sems, *pairs):
    copies = [pltpu.make_async_copy(a, b, sems.at[i]) for i, (a, b) in enumerate(pairs)]
    for copy in copies:
        copy.start()
    for copy in copies:
        copy.wait()


def solution(mesh):
    groups, domains = mesh.shape["grp"], mesh.shape["dom"]
    chips = domains // 2
    fine = Mesh(mesh.devices.reshape(groups, chips, 2), ("grp", "chip", "core"))
    everyone = ("grp", "chip", "core")
    members = groups * domains
    vmem = pl.BlockSpec(memory_space=pltpu.VMEM)
    hbm = pl.BlockSpec(memory_space=pltpu.HBM)

    def call(kernel, name, outs, ins, scratch, flops, mib):
        return pl.pallas_call(
            kernel,
            out_shape=outs,
            in_specs=ins,
            out_specs=jax.tree.map(lambda _: vmem, outs),
            scratch_shapes=scratch,
            cost_estimate=pl.CostEstimate(flops=flops, bytes_accessed=1 << 16, transcendentals=0),
            compiler_params=pltpu.CompilerParams(vmem_limit_bytes=mib * MIB),
            name=name,
        )

    def body(
        positions, smoothing, energy, mass, old_density, active, pair_list, export_leaves, export_route
    ):
        leaves, _, width = positions.shape
        pairs, exports = pair_list.shape[0], export_leaves.shape[0]
        f32, s32 = jnp.float32, jnp.int32
        tile_flops = width * width

        def shape(*sizes):
            return jax.ShapeDtypeStruct(sizes, f32)

        place = positions.transpose(1, 0, 2)
        pair_list, export_leaves, export_route = pair_list.T, export_leaves.T, export_route.T
        pair_table, leaf_table = pltpu.SMEM((2, pairs), s32), pltpu.SMEM((2, exports), s32)
        route_table = pltpu.SMEM((1, exports), s32)

        def copy_out(place_ref, h_ref, mass_ref, out_ref, sems):
            copies = []
            for k in range(chips):
                to = out_ref.at[k]
                copies += [(place_ref, to.at[pl.ds(0, 3)]), (h_ref, to.at[3]), (mass_ref, to.at[4])]
            fetch(sems, *copies)

        outgoing = pl.pallas_call(
            copy_out,
            out_shape=shape(chips, 5, leaves, width),
            in_specs=[hbm] * 3,
            out_specs=hbm,
            scratch_shapes=[pltpu.SemaphoreType.DMA((3 * chips,))],
            compiler_params=pltpu.CompilerParams(vmem_limit_bytes=MIB),
            name="copy_out",
        )(place, smoothing, mass).reshape(chips, 5 * leaves, width)
        near = lax.all_to_all(outgoing, "chip", split_axis=0, concat_axis=0, tiled=True)

        def row(own_ref, item, leaf):
            return own_ref[item, pl.ds(leaf, 1), :]

        def local_place(own_ref, mine, other):
            return [row(own_ref, X + c, other) - row(own_ref, ORIGIN + c, mine) for c in range(3)]

        def local_density(
            pair_hbm, place_hbm, h_hbm, mass_hbm, energy_hbm, old_hbm, active_hbm, own_ref, right_ref,
            centred_ref, pair_ref, active_ref, sems
        ):
            fetch(
                sems,
                (pair_hbm, pair_ref),
                (place_hbm, own_ref.at[pl.ds(X, 3)]),
                (h_hbm, own_ref.at[H]),
                (mass_hbm, own_ref.at[MASS]),
                (energy_hbm, own_ref.at[ENERGY]),
                (old_hbm, own_ref.at[OLD]),
                (active_hbm, active_ref),
            )
            h = own_ref[H]
            own_ref[ACTIVE] = active_ref[...].astype(f32)
            own_ref[INVERSE] = 1.0 / h
            own_ref[SCALE] = slope_scale(h)
            own_ref[SUM] = jnp.zeros_like(h)
            norm = jnp.zeros_like(h)
            centred = []
            for c in range(3):
                mean = jnp.sum(own_ref[X + c], axis=1, keepdims=True) * (1.0 / width)
                mean = jnp.broadcast_to(mean, h.shape)
                own_ref[ORIGIN + c] = mean
                item = own_ref[X + c] - mean
                norm = norm + item * item
                centred.append(item)
            zero, one = jnp.zeros_like(h), jnp.ones_like(h)
            rights = [-2.0 * item for item in centred] + [one, norm, zero, zero, zero]
            places = [zero] + centred + [zero] * 4
            for leaf in range(leaves):
                at = slice(leaf, leaf + 1)
                right_ref[leaf] = right_terms(jnp.concatenate([item[at] for item in rights], axis=0))
                centred_ref[leaf] = jnp.concatenate([item[at] for item in places], axis=0)

            def tile(e):
                mine, other = pair_ref[0, e], pair_ref[1, e]
                own_ref[SUM, pl.ds(mine, 1), :] = row(own_ref, SUM, mine) + density_tile(
                    right_ref[mine],
                    row(own_ref, INVERSE, mine),
                    local_place(own_ref, mine, other),
                    row(own_ref, MASS, other),
                )

            grouped(pairs, tile)

        own, right, centred = call(
            local_density,
            "local_density",
            (
                shape(TABLE, leaves, width),
                jax.ShapeDtypeStruct((leaves, 48, width), jnp.bfloat16),
                shape(leaves, 8, width),
            ),
            [hbm] * 7,
            [pair_table, pltpu.VMEM((leaves, width), s32), pltpu.SemaphoreType.DMA((7,))],
            pairs * tile_flops * 30,
            4,
        )(pair_list, place, smoothing, mass, energy, old_density, active)
        near, own = lax.optimization_barrier((near, own))
        peer = lax.ppermute(near, "core", [(0, 1), (1, 0)])

        def export(leaf_ref, route_ref, near_ref, peer_ref, own_ref, e, items):
            core = lax.axis_index("core")
            me = lax.axis_index("chip") * 2 + core
            mine, other = leaf_ref[0, e], leaf_ref[1, e]
            target = me + 1 + route_ref[0, e]
            target = jnp.where(target >= domains, target - domains, target)
            chip = target // 2
            same = (target - chip * 2) == core

            def get(c):
                at = pl.ds(c * leaves + other, 1)
                return jnp.where(same, near_ref[chip, at, :], peer_ref[chip, at, :])

            spot = [get(c) - row(own_ref, ORIGIN + c, mine) for c in range(3)]
            return mine, spot, [get(c) for c in items]

        def remote_density(
            leaf_hbm, route_hbm, own_ref, right_ref, near_ref, peer_ref, density_ref, term_ref,
            spread_ref, total, leaf_ref, route_ref, sems
        ):
            fetch(sems, (leaf_hbm, leaf_ref), (route_hbm, route_ref))
            total[...] = own_ref[SUM]

            def tile(e):
                mine, spot, (far_mass,) = export(
                    leaf_ref, route_ref, near_ref, peer_ref, own_ref, e, (4,)
                )
                at = pl.ds(mine, 1)
                total[at, :] = total[at, :] + density_tile(
                    right_ref[mine], row(own_ref, INVERSE, mine), spot, far_mass
                )

            grouped(exports, tile)
            inverse = own_ref[INVERSE]
            summed = (total[...] + own_ref[MASS]) * (NORM * (inverse * inverse * inverse))
            density = jnp.where(own_ref[ACTIVE] == 1.0, summed, own_ref[OLD])
            term = (ADIABATIC - 1.0) * own_ref[ENERGY] / density
            density_ref[...] = density
            term_ref[...] = term
            for d in range(domains):
                spread_ref[d] = term

        wire_mib = 2 * domains * leaves * width * 20 // MIB
        density, term, outgoing = call(
            remote_density,
            "remote_density",
            (shape(leaves, width), shape(leaves, width), shape(domains, leaves, width)),
            [hbm] * 2 + [vmem] * 4,
            [pltpu.VMEM((leaves, width), f32), leaf_table, route_table, pltpu.SemaphoreType.DMA((2,))],
            exports * tile_flops * 30,
            6 + wire_mib,
        )(export_leaves, export_route, own, right, near, peer)
        terms = lax.all_to_all(outgoing, ("chip", "core"), split_axis=0, concat_axis=0, tiled=True)

        def prepare(
            pair_hbm, leaf_hbm, route_hbm, own_ref, right_ref, centred_ref, near_ref, peer_ref,
            term_ref, sum_ref, weight_ref, moment_ref, pair_ref, leaf_ref, route_ref, sems
        ):
            fetch(sems, (pair_hbm, pair_ref), (leaf_hbm, leaf_ref), (route_hbm, route_ref))
            sum_ref[...] = jnp.zeros_like(sum_ref)

            def weigh(mine, spot, inverse, scale):
                return weight_tile(
                    right_ref[mine],
                    row(own_ref, INVERSE, mine),
                    row(own_ref, SCALE, mine),
                    spot,
                    inverse,
                    scale,
                )

            def local_tile(e):
                mine, other = pair_ref[0, e], pair_ref[1, e]
                spot = local_place(own_ref, mine, other)
                weights = stack(
                    weigh(mine, spot, row(own_ref, INVERSE, other), row(own_ref, SCALE, other))
                )
                rows = moments(row(own_ref, MASS, other), spot)
                far_term, own_term = term_ref[pl.ds(other, 1), :], term_ref[pl.ds(mine, 1), :]
                sum_ref[mine] = sum_ref[mine] + force(
                    weights, rows, far_term, own_term, centred_ref[mine]
                )

            def remote_tile(e):
                mine, spot, (h, far_mass) = export(
                    leaf_ref, route_ref, near_ref, peer_ref, own_ref, e, (3, 4)
                )
                weight_ref[e] = stack(weigh(mine, spot, 1.0 / h, slope_scale(h)))
                moment_ref[e] = moments(far_mass, spot)

            grouped(pairs, local_tile)
            grouped(exports, remote_tile)

        stash_mib = 2 * exports * width * (6 * width + 32) // MIB
        partial, weights, rows = call(
            prepare,
            "prepare_force",
            (
                shape(leaves, 4, width),
                jax.ShapeDtypeStruct((exports, 3 * width, width), jnp.bfloat16),
                shape(exports, 8, width),
            ),
            [hbm] * 3 + [vmem] * 6,
            [pair_table, leaf_table, route_table, pltpu.SemaphoreType.DMA((3,))],
            (pairs + exports) * tile_flops * 60,
            6 + stash_mib + wire_mib,
        )(pair_list, export_leaves, export_route, own, right, centred, near, peer, term)

        def finish(
            leaf_hbm, route_hbm, own_ref, centred_ref, term_ref, terms_ref, partial_ref, weight_ref,
            moment_ref, accel_ref, least_ref, total, leaf_ref, route_ref, sems
        ):
            fetch(sems, (leaf_hbm, leaf_ref), (route_hbm, route_ref))
            total[...] = partial_ref[...]
            me = lax.axis_index("chip") * 2 + lax.axis_index("core")

            def tile(e):
                mine, other = leaf_ref[0, e], leaf_ref[1, e]
                target = me + 1 + route_ref[0, e]
                target = jnp.where(target >= domains, target - domains, target)
                far_term = terms_ref[target, pl.ds(other, 1), :]
                total[mine] = total[mine] + force(
                    weight_ref[e],
                    moment_ref[e],
                    far_term,
                    term_ref[pl.ds(mine, 1), :],
                    centred_ref[mine],
                )

            grouped(exports, tile)
            for c in range(3):
                for leaf in range(leaves):
                    accel_ref[c, leaf : leaf + 1, :] = total[leaf, c + 1 : c + 2, :]
            awake = own_ref[ACTIVE] == 1.0
            square = jnp.zeros((leaves, width), f32)
            for c in range(3):
                part = jnp.where(awake, accel_ref[c], 0.0)
                accel_ref[c] = part
                square = square + part * part
            h = own_ref[H]
            speed = jnp.sqrt(ADIABATIC * (ADIABATIC - 1.0) * own_ref[ENERGY])
            step = COURANT * h / (speed + jnp.sqrt(h * jnp.sqrt(square)))
            least_ref[...] = jnp.full(
                (members, width), jnp.min(jnp.where(awake, step, jnp.inf)), f32
            )

        accel, least = call(
            finish,
            "finish_force",
            (shape(3, leaves, width), shape(members, width)),
            [hbm] * 2 + [vmem] * 7,
            [pltpu.VMEM((leaves, 4, width), f32), leaf_table, route_table, pltpu.SemaphoreType.DMA((2,))],
            exports * tile_flops * 16,
            6 + stash_mib + wire_mib,
        )(export_leaves, export_route, own, centred, term, terms, partial, weights, rows)

        everywhere = lax.all_to_all(least, everyone, split_axis=0, concat_axis=0, tiled=True)
        return density, accel.transpose(1, 0, 2), jnp.min(everywhere)

    flat = P(everyone, None)
    deep = P(everyone, None, None)
    return jax.shard_map(
        body,
        mesh=fine,
        in_specs=(deep,) + (flat,) * 8,
        out_specs=(flat, deep, P()),
        check_vma=False,
    )
```

```python
import math

import jax
import jax.numpy as jnp
from jax import lax
from jax.experimental import pallas as pl
from jax.experimental.pallas import tpu as pltpu
from jax.sharding import Mesh, PartitionSpec as P

ADIABATIC = 5.0 / 3.0
COURANT = 0.3
GROUP = 24
TINY = 1e-30
NORM = 8.0 / math.pi
MIB = 1 << 20
X, MASS, H, INVERSE, SCALE, ORIGIN, ENERGY, OLD, ACTIVE, SUM, TABLE = 0, 3, 4, 5, 6, 7, 10, 11, 12, 13, 14


def split(item):
    first = item.astype(jnp.bfloat16).astype(jnp.float32)
    rest = item - first
    second = rest.astype(jnp.bfloat16).astype(jnp.float32)
    return first, second, rest - second


def product(a, b, dims):
    return lax.dot_general(a, b, (dims, ((), ())), preferred_element_type=jnp.float32)


def left_terms(item):
    first, second, third = split(item)
    return jnp.concatenate([first, first, second, first, third, second], axis=0).astype(jnp.bfloat16)


def right_terms(item):
    first, second, third = split(item)
    return jnp.concatenate([first, second, first, third, first, second], axis=0).astype(jnp.bfloat16)


def turn(rows):
    width, count = rows[0].shape[1], len(rows)
    rows = list(rows) + [jnp.zeros_like(rows[0])] * (-count % 8)
    turned = jnp.concatenate(rows, axis=0).T
    return [jnp.broadcast_to(turned[:, k : k + 1], (width, width)) for k in range(count)]


def separation(right, place):
    norm = place[0] * place[0] + place[1] * place[1] + place[2] * place[2]
    zero = jnp.zeros_like(norm)
    left = jnp.concatenate(place + [norm, jnp.ones_like(norm), zero, zero, zero], axis=0)
    square = jnp.maximum(product(left_terms(left), right, ((0,), (0,))), TINY)
    inverse = lax.rsqrt(square)
    return square * inverse, inverse


def density_tile(right, own_inverse, place, mass):
    (mass,) = turn([mass])
    dist, _ = separation(right, place)
    ratio = dist * own_inverse
    left = 1.0 - ratio
    inner = 1.0 - 6.0 * (ratio * ratio * left)
    remain = jnp.maximum(left, 0.0)
    outer = 2.0 * (remain * remain * remain)
    value = jnp.where(ratio < 0.5, inner, outer)
    return jnp.sum(value * mass, axis=0, keepdims=True)


def slope(dist, smooth_inverse, scale):
    ratio = dist * smooth_inverse
    remain = jnp.maximum(1.0 - ratio, 0.0)
    return jnp.where(ratio < 0.5, ratio * (2.0 - 3.0 * ratio), remain * remain) * scale


def weight_tile(right, own_inverse, own_scale, place, inverse, scale):
    inverse, scale = turn([inverse, scale])
    dist, over = separation(right, place)
    return over * (slope(dist, own_inverse, own_scale) + slope(dist, inverse, scale))


def moments(mass, place):
    half = [mass] + [mass * item for item in place]
    return jnp.concatenate(half + half, axis=0)


def force(weights, rows, far_term, own_term, own_place):
    item = lax.broadcasted_iota(jnp.int32, rows.shape, 0)
    rows = jnp.where(item < 4, rows, rows * far_term)
    rows = jnp.concatenate(split(rows), axis=0).astype(jnp.bfloat16)
    sums = product(jnp.concatenate([rows, rows, rows], axis=1), weights, ((1,), (0,)))
    sums = sums[:8] + sums[8:16] + sums[16:]
    sums = own_term * sums[:4] + sums[4:]
    return own_place[:4] * sums[:1] - sums


def stack(weights):
    return jnp.concatenate([part.astype(jnp.bfloat16) for part in split(weights)], axis=0)


def slope_scale(h):
    square = h * h
    return (3.0 * NORM) / (square * square)


def grouped(count, body, group=GROUP):
    step = max(d for d in range(1, min(group, count) + 1) if count % d == 0)

    def run(group, carry):
        for k in range(step):
            body(group * step + k)
        return carry

    lax.fori_loop(0, count // step, run, 0)


def fetch(sems, *pairs):
    copies = [pltpu.make_async_copy(a, b, sems.at[i]) for i, (a, b) in enumerate(pairs)]
    for copy in copies:
        copy.start()
    for copy in copies:
        copy.wait()


def solution(mesh):
    groups, domains = mesh.shape["grp"], mesh.shape["dom"]
    chips = domains // 2
    fine = Mesh(mesh.devices.reshape(groups, chips, 2), ("grp", "chip", "core"))
    everyone = ("grp", "chip", "core")
    members = groups * domains
    vmem = pl.BlockSpec(memory_space=pltpu.VMEM)
    hbm = pl.BlockSpec(memory_space=pltpu.HBM)

    def call(kernel, name, outs, ins, scratch, flops, mib):
        return pl.pallas_call(
            kernel,
            out_shape=outs,
            in_specs=ins,
            out_specs=jax.tree.map(lambda _: vmem, outs),
            scratch_shapes=scratch,
            cost_estimate=pl.CostEstimate(flops=flops, bytes_accessed=1 << 16, transcendentals=0),
            compiler_params=pltpu.CompilerParams(vmem_limit_bytes=mib * MIB),
            name=name,
        )

    def body(
        positions, smoothing, energy, mass, old_density, active, pair_list, export_leaves, export_route
    ):
        leaves, _, width = positions.shape
        pairs, exports = pair_list.shape[0], export_leaves.shape[0]
        f32, s32 = jnp.float32, jnp.int32
        tile_flops = width * width

        def shape(*sizes):
            return jax.ShapeDtypeStruct(sizes, f32)

        def kept(item):
            return pltpu.with_memory_space_constraint(item, pltpu.HBM)

        place = kept(positions.transpose(1, 0, 2))
        smoothing, energy, mass = kept(smoothing), kept(energy), kept(mass)
        old_density, active = kept(old_density), kept(active)
        pair_list, export_leaves = kept(pair_list.T), kept(export_leaves.T)
        export_route = kept(export_route.T)
        pair_table, leaf_table = pltpu.SMEM((2, pairs), s32), pltpu.SMEM((2, exports), s32)
        route_table = pltpu.SMEM((1, exports), s32)
        sheet = pltpu.VMEM((leaves, width), f32)

        def copy_out(place_ref, h_ref, mass_ref, out_ref, sems):
            copies = []
            for k in range(chips):
                to = out_ref.at[k]
                copies += [(place_ref, to.at[pl.ds(0, 3)]), (h_ref, to.at[3]), (mass_ref, to.at[4])]
            fetch(sems, *copies)

        outgoing = pl.pallas_call(
            copy_out,
            out_shape=shape(chips, 5, leaves, width),
            in_specs=[hbm] * 3,
            out_specs=hbm,
            scratch_shapes=[pltpu.SemaphoreType.DMA((3 * chips,))],
            compiler_params=pltpu.CompilerParams(vmem_limit_bytes=MIB),
            name="copy_out",
        )(place, smoothing, mass).reshape(chips, 5 * leaves, width)
        near = lax.all_to_all(outgoing, "chip", split_axis=0, concat_axis=0, tiled=True)

        def row(own_ref, item, leaf):
            return own_ref[item, pl.ds(leaf, 1), :]

        def local_place(own_ref, mine, other):
            return [row(own_ref, X + c, other) - row(own_ref, ORIGIN + c, mine) for c in range(3)]

        def local_density(
            pair_hbm, place_hbm, h_hbm, mass_hbm, energy_hbm, old_hbm, active_hbm, own_ref, right_ref,
            centred_ref, pair_ref, active_ref, sems
        ):
            fetch(
                sems,
                (pair_hbm, pair_ref),
                (place_hbm, own_ref.at[pl.ds(X, 3)]),
                (h_hbm, own_ref.at[H]),
                (mass_hbm, own_ref.at[MASS]),
                (energy_hbm, own_ref.at[ENERGY]),
                (old_hbm, own_ref.at[OLD]),
                (active_hbm, active_ref),
            )
            h = own_ref[H]
            own_ref[ACTIVE] = active_ref[...].astype(f32)
            own_ref[INVERSE] = 1.0 / h
            own_ref[SCALE] = slope_scale(h)
            own_ref[SUM] = jnp.zeros_like(h)
            norm = jnp.zeros_like(h)
            centred = []
            for c in range(3):
                mean = jnp.sum(own_ref[X + c], axis=1, keepdims=True) * (1.0 / width)
                mean = jnp.broadcast_to(mean, h.shape)
                own_ref[ORIGIN + c] = mean
                item = own_ref[X + c] - mean
                norm = norm + item * item
                centred.append(item)
            zero, one = jnp.zeros_like(h), jnp.ones_like(h)
            rights = [-2.0 * item for item in centred] + [one, norm, zero, zero, zero]
            places = [zero] + centred + [zero] * 4
            for leaf in range(leaves):
                at = slice(leaf, leaf + 1)
                right_ref[leaf] = right_terms(jnp.concatenate([item[at] for item in rights], axis=0))
                centred_ref[leaf] = jnp.concatenate([item[at] for item in places], axis=0)

            def tile(e):
                mine, other = pair_ref[0, e], pair_ref[1, e]
                own_ref[SUM, pl.ds(mine, 1), :] = row(own_ref, SUM, mine) + density_tile(
                    right_ref[mine],
                    row(own_ref, INVERSE, mine),
                    local_place(own_ref, mine, other),
                    row(own_ref, MASS, other),
                )

            grouped(pairs, tile)

        own, right, centred = call(
            local_density,
            "local_density",
            (
                shape(TABLE, leaves, width),
                jax.ShapeDtypeStruct((leaves, 48, width), jnp.bfloat16),
                shape(leaves, 8, width),
            ),
            [hbm] * 7,
            [pair_table, pltpu.VMEM((leaves, width), s32), pltpu.SemaphoreType.DMA((7,))],
            pairs * tile_flops * 30,
            4,
        )(pair_list, place, smoothing, mass, energy, old_density, active)
        near, own = lax.optimization_barrier((near, own))
        peer = lax.ppermute(near, "core", [(0, 1), (1, 0)])

        def export(leaf_ref, route_ref, near_ref, peer_ref, own_ref, e, items):
            core = lax.axis_index("core")
            me = lax.axis_index("chip") * 2 + core
            mine, other = leaf_ref[0, e], leaf_ref[1, e]
            target = me + 1 + route_ref[0, e]
            target = jnp.where(target >= domains, target - domains, target)
            chip = target // 2
            same = (target - chip * 2) == core

            def get(c):
                at = pl.ds(c * leaves + other, 1)
                return jnp.where(same, near_ref[chip, at, :], peer_ref[chip, at, :])

            spot = [get(c) - row(own_ref, ORIGIN + c, mine) for c in range(3)]
            return mine, spot, [get(c) for c in items]

        def remote_density(
            leaf_hbm, route_hbm, own_ref, right_ref, near_ref, peer_ref, density_ref, term_ref,
            spread_ref, total, leaf_ref, route_ref, sems
        ):
            fetch(sems, (leaf_hbm, leaf_ref), (route_hbm, route_ref))
            total[...] = own_ref[SUM]

            def tile(e):
                mine, spot, (far_mass,) = export(
                    leaf_ref, route_ref, near_ref, peer_ref, own_ref, e, (4,)
                )
                at = pl.ds(mine, 1)
                total[at, :] = total[at, :] + density_tile(
                    right_ref[mine], row(own_ref, INVERSE, mine), spot, far_mass
                )

            grouped(exports, tile)
            inverse = own_ref[INVERSE]
            summed = (total[...] + own_ref[MASS]) * (NORM * (inverse * inverse * inverse))
            density = jnp.where(own_ref[ACTIVE] == 1.0, summed, own_ref[OLD])
            term = (ADIABATIC - 1.0) * own_ref[ENERGY] / density
            density_ref[...] = density
            term_ref[...] = term
            for d in range(domains):
                spread_ref[d] = term

        wire_mib = 2 * domains * leaves * width * 20 // MIB
        density, term, outgoing = call(
            remote_density,
            "remote_density",
            (shape(leaves, width), pltpu.HBM((leaves, width), f32), shape(domains, leaves, width)),
            [hbm] * 2 + [vmem] * 4,
            [sheet, leaf_table, route_table, pltpu.SemaphoreType.DMA((2,))],
            exports * tile_flops * 30,
            6 + wire_mib,
        )(export_leaves, export_route, own, right, near, peer)
        term = kept(term)
        terms = lax.all_to_all(outgoing, ("chip", "core"), split_axis=0, concat_axis=0, tiled=True)

        def prepare(
            pair_hbm, leaf_hbm, route_hbm, term_hbm, own_ref, right_ref, centred_ref, near_ref,
            peer_ref, sum_ref, weight_ref, moment_ref, pair_ref, leaf_ref, route_ref, term_ref, sems
        ):
            fetch(
                sems,
                (pair_hbm, pair_ref),
                (leaf_hbm, leaf_ref),
                (route_hbm, route_ref),
                (term_hbm, term_ref),
            )
            sum_ref[...] = jnp.zeros_like(sum_ref)

            def weigh(mine, spot, inverse, scale):
                return weight_tile(
                    right_ref[mine],
                    row(own_ref, INVERSE, mine),
                    row(own_ref, SCALE, mine),
                    spot,
                    inverse,
                    scale,
                )

            def local_tile(e):
                mine, other = pair_ref[0, e], pair_ref[1, e]
                spot = local_place(own_ref, mine, other)
                weights = stack(
                    weigh(mine, spot, row(own_ref, INVERSE, other), row(own_ref, SCALE, other))
                )
                rows = moments(row(own_ref, MASS, other), spot)
                far_term, own_term = term_ref[pl.ds(other, 1), :], term_ref[pl.ds(mine, 1), :]
                sum_ref[mine] = sum_ref[mine] + force(
                    weights, rows, far_term, own_term, centred_ref[mine]
                )

            def remote_tile(e):
                mine, spot, (h, far_mass) = export(
                    leaf_ref, route_ref, near_ref, peer_ref, own_ref, e, (3, 4)
                )
                weight_ref[e] = stack(weigh(mine, spot, 1.0 / h, slope_scale(h)))
                moment_ref[e] = moments(far_mass, spot)

            grouped(pairs, local_tile)
            grouped(exports, remote_tile)

        stash_mib = 2 * exports * width * (6 * width + 32) // MIB
        partial, weights, rows = call(
            prepare,
            "prepare_force",
            (
                shape(leaves, 4, width),
                jax.ShapeDtypeStruct((exports, 3 * width, width), jnp.bfloat16),
                pltpu.HBM((exports, 8, width), f32),
            ),
            [hbm] * 4 + [vmem] * 5,
            [pair_table, leaf_table, route_table, sheet, pltpu.SemaphoreType.DMA((4,))],
            (pairs + exports) * tile_flops * 60,
            6 + stash_mib + wire_mib,
        )(pair_list, export_leaves, export_route, term, own, right, centred, near, peer)

        def finish(
            leaf_hbm, route_hbm, term_hbm, moment_hbm, own_ref, centred_ref, terms_ref, partial_ref,
            weight_ref, accel_ref, least_ref, total, leaf_ref, route_ref, term_ref, moment_ref, sems
        ):
            fetch(
                sems,
                (leaf_hbm, leaf_ref),
                (route_hbm, route_ref),
                (term_hbm, term_ref),
                (moment_hbm, moment_ref),
            )
            total[...] = partial_ref[...]
            me = lax.axis_index("chip") * 2 + lax.axis_index("core")

            def tile(e):
                mine, other = leaf_ref[0, e], leaf_ref[1, e]
                target = me + 1 + route_ref[0, e]
                target = jnp.where(target >= domains, target - domains, target)
                far_term = terms_ref[target, pl.ds(other, 1), :]
                total[mine] = total[mine] + force(
                    weight_ref[e],
                    moment_ref[e],
                    far_term,
                    term_ref[pl.ds(mine, 1), :],
                    centred_ref[mine],
                )

            grouped(exports, tile)
            for c in range(3):
                for leaf in range(leaves):
                    accel_ref[c, leaf : leaf + 1, :] = total[leaf, c + 1 : c + 2, :]
            awake = own_ref[ACTIVE] == 1.0
            square = jnp.zeros((leaves, width), f32)
            for c in range(3):
                part = jnp.where(awake, accel_ref[c], 0.0)
                accel_ref[c] = part
                square = square + part * part
            h = own_ref[H]
            speed = jnp.sqrt(ADIABATIC * (ADIABATIC - 1.0) * own_ref[ENERGY])
            step = COURANT * h / (speed + jnp.sqrt(h * jnp.sqrt(square)))
            least_ref[...] = jnp.full(
                (members, width), jnp.min(jnp.where(awake, step, jnp.inf)), f32
            )

        accel, least = call(
            finish,
            "finish_force",
            (shape(3, leaves, width), shape(members, width)),
            [hbm] * 4 + [vmem] * 5,
            [
                pltpu.VMEM((leaves, 4, width), f32),
                leaf_table,
                route_table,
                sheet,
                pltpu.VMEM((exports, 8, width), f32),
                pltpu.SemaphoreType.DMA((4,)),
            ],
            exports * tile_flops * 16,
            6 + stash_mib + wire_mib,
        )(export_leaves, export_route, term, kept(rows), own, centred, terms, partial, weights)

        everywhere = lax.all_to_all(least, everyone, split_axis=0, concat_axis=0, tiled=True)
        return density, accel.transpose(1, 0, 2), jnp.min(everywhere)

    flat = P(everyone, None)
    deep = P(everyone, None, None)
    return jax.shard_map(
        body,
        mesh=fine,
        in_specs=(deep,) + (flat,) * 8,
        out_specs=(flat, deep, P()),
        check_vma=False,
    )
```

```python
import math

import jax
import jax.numpy as jnp
from jax import lax
from jax.experimental import pallas as pl
from jax.experimental.pallas import tpu as pltpu
from jax.sharding import Mesh, PartitionSpec as P

ADIABATIC = 5.0 / 3.0
COURANT = 0.3
GROUP = 24
TINY = 1e-30
NORM = 8.0 / math.pi
MIB = 1 << 20
X, MASS, H, INVERSE, SCALE, ORIGIN, ENERGY, OLD, ACTIVE, SUM, TABLE = 0, 3, 4, 5, 6, 7, 10, 11, 12, 13, 14


def split(item):
    first = item.astype(jnp.bfloat16).astype(jnp.float32)
    rest = item - first
    second = rest.astype(jnp.bfloat16).astype(jnp.float32)
    return first, second, rest - second


def product(a, b, dims):
    return lax.dot_general(a, b, (dims, ((), ())), preferred_element_type=jnp.float32)


def left_terms(item):
    first, second, third = split(item)
    return jnp.concatenate([first, first, second, first, third, second], axis=0).astype(jnp.bfloat16)


def right_terms(item):
    first, second, third = split(item)
    return jnp.concatenate([first, second, first, third, first, second], axis=0).astype(jnp.bfloat16)


def turn(rows):
    width, count = rows[0].shape[1], len(rows)
    rows = list(rows) + [jnp.zeros_like(rows[0])] * (-count % 8)
    turned = jnp.concatenate(rows, axis=0).T
    return [jnp.broadcast_to(turned[:, k : k + 1], (width, width)) for k in range(count)]


def separation(right, place):
    norm = place[0] * place[0] + place[1] * place[1] + place[2] * place[2]
    zero = jnp.zeros_like(norm)
    left = jnp.concatenate(place + [norm, jnp.ones_like(norm), zero, zero, zero], axis=0)
    square = jnp.maximum(product(left_terms(left), right, ((0,), (0,))), TINY)
    inverse = lax.rsqrt(square)
    return square * inverse, inverse


def density_tile(right, own_inverse, place, mass):
    (mass,) = turn([mass])
    dist, _ = separation(right, place)
    ratio = dist * own_inverse
    left = 1.0 - ratio
    inner = 1.0 - 6.0 * (ratio * ratio * left)
    remain = jnp.maximum(left, 0.0)
    outer = 2.0 * (remain * remain * remain)
    value = jnp.where(ratio < 0.5, inner, outer)
    return jnp.sum(value * mass, axis=0, keepdims=True)


def slope(dist, smooth_inverse, scale):
    ratio = dist * smooth_inverse
    remain = jnp.maximum(1.0 - ratio, 0.0)
    return jnp.where(ratio < 0.5, ratio * (2.0 - 3.0 * ratio), remain * remain) * scale


def weight_tile(right, own_inverse, own_scale, place, inverse, scale):
    inverse, scale = turn([inverse, scale])
    dist, over = separation(right, place)
    return over * (slope(dist, own_inverse, own_scale) + slope(dist, inverse, scale))


def moments(mass, place):
    half = [mass] + [mass * item for item in place]
    return jnp.concatenate(half + half, axis=0)


def force(weights, rows, far_term, own_term, own_place):
    item = lax.broadcasted_iota(jnp.int32, rows.shape, 0)
    rows = jnp.where(item < 4, rows, rows * far_term)
    rows = jnp.concatenate(split(rows), axis=0).astype(jnp.bfloat16)
    sums = product(jnp.concatenate([rows, rows, rows], axis=1), weights, ((1,), (0,)))
    sums = sums[:8] + sums[8:16] + sums[16:]
    sums = own_term * sums[:4] + sums[4:]
    return own_place[:4] * sums[:1] - sums


def stack(weights):
    return jnp.concatenate([part.astype(jnp.bfloat16) for part in split(weights)], axis=0)


def slope_scale(h):
    square = h * h
    return (3.0 * NORM) / (square * square)


def grouped(count, body, group=GROUP):
    step = max(d for d in range(1, min(group, count) + 1) if count % d == 0)

    def run(group, carry):
        for k in range(step):
            body(group * step + k)
        return carry

    lax.fori_loop(0, count // step, run, 0)


def fetch(sems, *pairs):
    copies = [pltpu.make_async_copy(a, b, sems.at[i]) for i, (a, b) in enumerate(pairs)]
    for copy in copies:
        copy.start()
    for copy in copies:
        copy.wait()


def solution(mesh):
    groups, domains = mesh.shape["grp"], mesh.shape["dom"]
    chips = domains // 2
    fine = Mesh(mesh.devices.reshape(groups, chips, 2), ("grp", "chip", "core"))
    everyone = ("grp", "chip", "core")
    members = groups * domains
    vmem = pl.BlockSpec(memory_space=pltpu.VMEM)
    hbm = pl.BlockSpec(memory_space=pltpu.HBM)

    def call(kernel, name, outs, ins, scratch, flops, mib):
        return pl.pallas_call(
            kernel,
            out_shape=outs,
            in_specs=ins,
            out_specs=jax.tree.map(lambda _: vmem, outs),
            scratch_shapes=scratch,
            cost_estimate=pl.CostEstimate(flops=flops, bytes_accessed=1 << 16, transcendentals=0),
            compiler_params=pltpu.CompilerParams(vmem_limit_bytes=mib * MIB),
            name=name,
        )

    def body(
        positions, smoothing, energy, mass, old_density, active, pair_list, export_leaves, export_route
    ):
        leaves, _, width = positions.shape
        pairs, exports = pair_list.shape[0], export_leaves.shape[0]
        f32, s32 = jnp.float32, jnp.int32
        tile_flops = width * width

        def shape(*sizes):
            return jax.ShapeDtypeStruct(sizes, f32)

        def near_core(*sizes):
            small = math.prod(sizes) * 4 <= MIB // 2
            return (pltpu.VMEM if small else pltpu.HBM)(sizes, f32)

        def kept(item):
            return pltpu.with_memory_space_constraint(item, pltpu.HBM)

        awake = active
        place = kept(positions.transpose(1, 0, 2))
        smoothing, energy, mass = kept(smoothing), kept(energy), kept(mass)
        old_density, active = kept(old_density), kept(active)
        pair_list, export_leaves = kept(pair_list.T), kept(export_leaves.T)
        export_route = kept(export_route.T)
        pair_table, leaf_table = pltpu.SMEM((2, pairs), s32), pltpu.SMEM((2, exports), s32)
        route_table = pltpu.SMEM((1, exports), s32)
        sheet = pltpu.VMEM((leaves, width), f32)

        def copy_out(place_ref, h_ref, mass_ref, out_ref, sems):
            copies = []
            for k in range(chips):
                to = out_ref.at[k]
                copies += [(place_ref, to.at[pl.ds(0, 3)]), (h_ref, to.at[3]), (mass_ref, to.at[4])]
            fetch(sems, *copies)

        outgoing = call(
            copy_out,
            "copy_out",
            near_core(chips, 5, leaves, width),
            [hbm] * 3,
            [pltpu.SemaphoreType.DMA((3 * chips,))],
            1,
            4 + 2 * chips * 5 * leaves * width * 4 // MIB,
        )(place, smoothing, mass).reshape(chips, 5 * leaves, width)
        near = lax.all_to_all(outgoing, "chip", split_axis=0, concat_axis=0, tiled=True)

        def row(own_ref, item, leaf):
            return own_ref[item, pl.ds(leaf, 1), :]

        def local_place(own_ref, mine, other):
            return [row(own_ref, X + c, other) - row(own_ref, ORIGIN + c, mine) for c in range(3)]

        def local_density(
            pair_hbm, place_hbm, h_hbm, mass_hbm, energy_hbm, old_hbm, active_hbm, own_ref, right_ref,
            centred_ref, pair_ref, active_ref, sems
        ):
            fetch(
                sems,
                (pair_hbm, pair_ref),
                (place_hbm, own_ref.at[pl.ds(X, 3)]),
                (h_hbm, own_ref.at[H]),
                (mass_hbm, own_ref.at[MASS]),
                (energy_hbm, own_ref.at[ENERGY]),
                (old_hbm, own_ref.at[OLD]),
                (active_hbm, active_ref),
            )
            h = own_ref[H]
            own_ref[ACTIVE] = active_ref[...].astype(f32)
            own_ref[INVERSE] = 1.0 / h
            own_ref[SCALE] = slope_scale(h)
            own_ref[SUM] = jnp.zeros_like(h)
            norm = jnp.zeros_like(h)
            centred = []
            for c in range(3):
                mean = jnp.sum(own_ref[X + c], axis=1, keepdims=True) * (1.0 / width)
                mean = jnp.broadcast_to(mean, h.shape)
                own_ref[ORIGIN + c] = mean
                item = own_ref[X + c] - mean
                norm = norm + item * item
                centred.append(item)
            zero, one = jnp.zeros_like(h), jnp.ones_like(h)
            rights = [-2.0 * item for item in centred] + [one, norm, zero, zero, zero]
            places = [zero] + centred + [zero] * 4
            for leaf in range(leaves):
                at = slice(leaf, leaf + 1)
                right_ref[leaf] = right_terms(jnp.concatenate([item[at] for item in rights], axis=0))
                centred_ref[leaf] = jnp.concatenate([item[at] for item in places], axis=0)

            def tile(e):
                mine, other = pair_ref[0, e], pair_ref[1, e]
                own_ref[SUM, pl.ds(mine, 1), :] = row(own_ref, SUM, mine) + density_tile(
                    right_ref[mine],
                    row(own_ref, INVERSE, mine),
                    local_place(own_ref, mine, other),
                    row(own_ref, MASS, other),
                )

            grouped(pairs, tile)

        own, right, centred = call(
            local_density,
            "local_density",
            (
                shape(TABLE, leaves, width),
                jax.ShapeDtypeStruct((leaves, 48, width), jnp.bfloat16),
                shape(leaves, 8, width),
            ),
            [hbm] * 7,
            [pair_table, pltpu.VMEM((leaves, width), s32), pltpu.SemaphoreType.DMA((7,))],
            pairs * tile_flops * 30,
            4,
        )(pair_list, place, smoothing, mass, energy, old_density, active)
        near, own = lax.optimization_barrier((near, own))
        peer = lax.ppermute(near, "core", [(0, 1), (1, 0)])

        def export(leaf_ref, route_ref, near_ref, peer_ref, own_ref, e, items):
            core = lax.axis_index("core")
            me = lax.axis_index("chip") * 2 + core
            mine, other = leaf_ref[0, e], leaf_ref[1, e]
            target = me + 1 + route_ref[0, e]
            target = jnp.where(target >= domains, target - domains, target)
            chip = target // 2
            same = (target - chip * 2) == core

            def get(c):
                at = pl.ds(c * leaves + other, 1)
                return jnp.where(same, near_ref[chip, at, :], peer_ref[chip, at, :])

            spot = [get(c) - row(own_ref, ORIGIN + c, mine) for c in range(3)]
            return mine, spot, [get(c) for c in items]

        def remote_density(
            leaf_hbm, route_hbm, own_ref, right_ref, near_ref, peer_ref, spread_ref, total, leaf_ref,
            route_ref, sems
        ):
            fetch(sems, (leaf_hbm, leaf_ref), (route_hbm, route_ref))
            total[...] = own_ref[SUM]

            def tile(e):
                mine, spot, (far_mass,) = export(
                    leaf_ref, route_ref, near_ref, peer_ref, own_ref, e, (4,)
                )
                at = pl.ds(mine, 1)
                total[at, :] = total[at, :] + density_tile(
                    right_ref[mine], row(own_ref, INVERSE, mine), spot, far_mass
                )

            grouped(exports, tile)
            inverse = own_ref[INVERSE]
            summed = (total[...] + own_ref[MASS]) * (NORM * (inverse * inverse * inverse))
            density = jnp.where(own_ref[ACTIVE] == 1.0, summed, own_ref[OLD])
            term = (ADIABATIC - 1.0) * own_ref[ENERGY] / density
            for d in range(domains):
                spread_ref[d] = term

        wire_mib = 2 * domains * leaves * width * 20 // MIB
        outgoing = call(
            remote_density,
            "remote_density",
            near_core(domains, leaves, width),
            [hbm] * 2 + [vmem] * 4,
            [sheet, leaf_table, route_table, pltpu.SemaphoreType.DMA((2,))],
            exports * tile_flops * 30,
            6 + wire_mib,
        )(export_leaves, export_route, own, right, near, peer)
        terms = lax.all_to_all(outgoing, ("chip", "core"), split_axis=0, concat_axis=0, tiled=True)

        def prepare(
            pair_hbm, leaf_hbm, route_hbm, spread_ref, own_ref, right_ref, centred_ref, near_ref,
            peer_ref, density_ref, sum_ref, weight_ref, moment_ref, pair_ref, leaf_ref, route_ref, sems
        ):
            fetch(
                sems,
                (pair_hbm, pair_ref),
                (leaf_hbm, leaf_ref),
                (route_hbm, route_ref),
            )
            term_ref = spread_ref.at[0]
            fresh = (ADIABATIC - 1.0) * own_ref[ENERGY] / term_ref[...]
            density_ref[...] = jnp.where(own_ref[ACTIVE] == 1.0, fresh, own_ref[OLD])
            sum_ref[...] = jnp.zeros_like(sum_ref)

            def weigh(mine, spot, inverse, scale):
                return weight_tile(
                    right_ref[mine],
                    row(own_ref, INVERSE, mine),
                    row(own_ref, SCALE, mine),
                    spot,
                    inverse,
                    scale,
                )

            def local_tile(e):
                mine, other = pair_ref[0, e], pair_ref[1, e]
                spot = local_place(own_ref, mine, other)
                weights = stack(
                    weigh(mine, spot, row(own_ref, INVERSE, other), row(own_ref, SCALE, other))
                )
                rows = moments(row(own_ref, MASS, other), spot)
                far_term, own_term = term_ref[pl.ds(other, 1), :], term_ref[pl.ds(mine, 1), :]
                sum_ref[mine] = sum_ref[mine] + force(
                    weights, rows, far_term, own_term, centred_ref[mine]
                )

            def remote_tile(e):
                mine, spot, (h, far_mass) = export(
                    leaf_ref, route_ref, near_ref, peer_ref, own_ref, e, (3, 4)
                )
                weight_ref[e] = stack(weigh(mine, spot, 1.0 / h, slope_scale(h)))
                moment_ref[e] = moments(far_mass, spot)

            grouped(pairs, local_tile)
            grouped(exports, remote_tile)

        stash_mib = 2 * exports * width * (6 * width + 32) // MIB
        density, partial, weights, rows = call(
            prepare,
            "prepare_force",
            (
                shape(leaves, width),
                shape(leaves, 4, width),
                jax.ShapeDtypeStruct((exports, 3 * width, width), jnp.bfloat16),
                pltpu.HBM((exports, 8, width), f32),
            ),
            [hbm] * 3 + [vmem] * 6,
            [pair_table, leaf_table, route_table, pltpu.SemaphoreType.DMA((3,))],
            (pairs + exports) * tile_flops * 60,
            6 + stash_mib + wire_mib,
        )(pair_list, export_leaves, export_route, outgoing, own, right, centred, near, peer)

        def finish(
            leaf_hbm, route_hbm, moment_hbm, own_ref, centred_ref, terms_ref, partial_ref, weight_ref,
            accel_ref, least_ref, total, leaf_ref, route_ref, moment_ref, sems
        ):
            fetch(
                sems,
                (leaf_hbm, leaf_ref),
                (route_hbm, route_ref),
                (moment_hbm, moment_ref),
            )
            total[...] = partial_ref[...]
            me = lax.axis_index("chip") * 2 + lax.axis_index("core")

            def tile(e):
                mine, other = leaf_ref[0, e], leaf_ref[1, e]
                target = me + 1 + route_ref[0, e]
                target = jnp.where(target >= domains, target - domains, target)
                far_term = terms_ref[target, pl.ds(other, 1), :]
                total[mine] = total[mine] + force(
                    weight_ref[e],
                    moment_ref[e],
                    far_term,
                    terms_ref[me, pl.ds(mine, 1), :],
                    centred_ref[mine],
                )

            grouped(exports, tile)
            for c in range(3):
                for leaf in range(leaves):
                    accel_ref[c, leaf : leaf + 1, :] = total[leaf, c + 1 : c + 2, :]
            awake = own_ref[ACTIVE] == 1.0
            square = accel_ref[0] * accel_ref[0] + accel_ref[1] * accel_ref[1]
            square = square + accel_ref[2] * accel_ref[2]
            h = own_ref[H]
            speed = jnp.sqrt(ADIABATIC * (ADIABATIC - 1.0) * own_ref[ENERGY])
            step = COURANT * h / (speed + jnp.sqrt(h * jnp.sqrt(square)))
            least_ref[...] = jnp.full(
                (members, width), jnp.min(jnp.where(awake, step, jnp.inf)), f32
            )

        accel, least = call(
            finish,
            "finish_force",
            (near_core(3, leaves, width), near_core(members, width)),
            [hbm] * 3 + [vmem] * 5,
            [
                pltpu.VMEM((leaves, 4, width), f32),
                leaf_table,
                route_table,
                pltpu.VMEM((exports, 8, width), f32),
                pltpu.SemaphoreType.DMA((3,)),
            ],
            exports * tile_flops * 16,
            6 + stash_mib + wire_mib,
        )(export_leaves, export_route, kept(rows), own, centred, terms, partial, weights)

        everywhere = lax.all_to_all(least, everyone, split_axis=0, concat_axis=0, tiled=True)
        accel = jnp.where((awake == 1)[:, None, :], accel.transpose(1, 0, 2), 0.0)
        return density, accel, jnp.min(everywhere)

    flat = P(everyone, None)
    deep = P(everyone, None, None)
    return jax.shard_map(
        body,
        mesh=fine,
        in_specs=(deep,) + (flat,) * 8,
        out_specs=(flat, deep, P()),
        check_vma=False,
    )
```

```python
import math

import jax
import jax.numpy as jnp
from jax import lax
from jax.experimental import pallas as pl
from jax.experimental.pallas import tpu as pltpu
from jax.sharding import Mesh, PartitionSpec as P

ADIABATIC = 5.0 / 3.0
COURANT = 0.3
GROUP = 24
TINY = 1e-30
NORM = 8.0 / math.pi
MIB = 1 << 20
X, MASS, H, INVERSE, SCALE, ORIGIN, ENERGY, OLD, ACTIVE, SUM, TABLE = 0, 3, 4, 5, 6, 7, 10, 11, 12, 13, 14


def split(item):
    first = item.astype(jnp.bfloat16).astype(jnp.float32)
    rest = item - first
    second = rest.astype(jnp.bfloat16).astype(jnp.float32)
    return first, second, rest - second


def product(a, b, dims):
    return lax.dot_general(a, b, (dims, ((), ())), preferred_element_type=jnp.float32)


def left_terms(item):
    first, second, third = split(item)
    return jnp.concatenate([first, first, second, first, third, second], axis=0).astype(jnp.bfloat16)


def right_terms(item):
    first, second, third = split(item)
    return jnp.concatenate([first, second, first, third, first, second], axis=0).astype(jnp.bfloat16)


def turn(rows):
    width, count = rows[0].shape[1], len(rows)
    rows = list(rows) + [jnp.zeros_like(rows[0])] * (-count % 8)
    turned = jnp.concatenate(rows, axis=0).T
    return [jnp.broadcast_to(turned[:, k : k + 1], (width, width)) for k in range(count)]


def separation(right, place):
    norm = place[0] * place[0] + place[1] * place[1] + place[2] * place[2]
    zero = jnp.zeros_like(norm)
    left = jnp.concatenate(place + [norm, jnp.ones_like(norm), zero, zero, zero], axis=0)
    square = jnp.maximum(product(left_terms(left), right, ((0,), (0,))), TINY)
    inverse = lax.rsqrt(square)
    return square * inverse, inverse


def density_tile(right, own_inverse, place, mass):
    (mass,) = turn([mass])
    dist, _ = separation(right, place)
    ratio = dist * own_inverse
    left = 1.0 - ratio
    inner = 1.0 - 6.0 * (ratio * ratio * left)
    remain = jnp.maximum(left, 0.0)
    outer = 2.0 * (remain * remain * remain)
    value = jnp.where(ratio < 0.5, inner, outer)
    return jnp.sum(value * mass, axis=0, keepdims=True)


def slope(dist, smooth_inverse, scale):
    ratio = dist * smooth_inverse
    remain = jnp.maximum(1.0 - ratio, 0.0)
    return jnp.where(ratio < 0.5, ratio * (2.0 - 3.0 * ratio), remain * remain) * scale


def weight_tile(right, own_inverse, own_scale, place, inverse, scale):
    inverse, scale = turn([inverse, scale])
    dist, over = separation(right, place)
    return over * (slope(dist, own_inverse, own_scale) + slope(dist, inverse, scale))


def moments(mass, place):
    half = [mass] + [mass * item for item in place]
    return jnp.concatenate(half + half, axis=0)


def force(weights, rows, far_term, own_term, own_place):
    item = lax.broadcasted_iota(jnp.int32, rows.shape, 0)
    rows = jnp.where(item < 4, rows, rows * far_term)
    rows = jnp.concatenate(split(rows), axis=0).astype(jnp.bfloat16)
    sums = product(jnp.concatenate([rows, rows, rows], axis=1), weights, ((1,), (0,)))
    sums = sums[:8] + sums[8:16] + sums[16:]
    sums = own_term * sums[:4] + sums[4:]
    return own_place[:4] * sums[:1] - sums


def stack(weights):
    return jnp.concatenate([part.astype(jnp.bfloat16) for part in split(weights)], axis=0)


def slope_scale(h):
    square = h * h
    return (3.0 * NORM) / (square * square)


def grouped(count, body, group=GROUP):
    step = max(d for d in range(1, min(group, count) + 1) if count % d == 0)

    def run(group, carry):
        for k in range(step):
            body(group * step + k)
        return carry

    lax.fori_loop(0, count // step, run, 0)


def fetch(sems, *pairs):
    copies = [pltpu.make_async_copy(a, b, sems.at[i]) for i, (a, b) in enumerate(pairs)]
    for copy in copies:
        copy.start()
    for copy in copies:
        copy.wait()


def solution(mesh):
    groups, domains = mesh.shape["grp"], mesh.shape["dom"]
    chips = domains // 2
    fine = Mesh(mesh.devices.reshape(groups, chips, 2), ("grp", "chip", "core"))
    everyone = ("grp", "chip", "core")
    members = groups * domains
    vmem = pl.BlockSpec(memory_space=pltpu.VMEM)
    hbm = pl.BlockSpec(memory_space=pltpu.HBM)

    def call(kernel, name, outs, ins, scratch, flops, mib):
        return pl.pallas_call(
            kernel,
            out_shape=outs,
            in_specs=ins,
            out_specs=jax.tree.map(lambda _: vmem, outs),
            scratch_shapes=scratch,
            cost_estimate=pl.CostEstimate(flops=flops, bytes_accessed=1 << 16, transcendentals=0),
            compiler_params=pltpu.CompilerParams(vmem_limit_bytes=mib * MIB),
            name=name,
        )

    def body(
        positions, smoothing, energy, mass, old_density, active, pair_list, export_leaves, export_route
    ):
        leaves, _, width = positions.shape
        pairs, exports = pair_list.shape[0], export_leaves.shape[0]
        f32, s32 = jnp.float32, jnp.int32
        tile_flops = width * width

        def shape(*sizes):
            return jax.ShapeDtypeStruct(sizes, f32)

        def kept(item):
            return pltpu.with_memory_space_constraint(item, pltpu.HBM)

        place = kept(positions.transpose(1, 0, 2))
        smoothing, energy, mass = kept(smoothing), kept(energy), kept(mass)
        old_density, active = kept(old_density), kept(active)
        pair_list, export_leaves = kept(pair_list.T), kept(export_leaves.T)
        export_route = kept(export_route.T)
        pair_table, leaf_table = pltpu.SMEM((2, pairs), s32), pltpu.SMEM((2, exports), s32)
        route_table = pltpu.SMEM((1, exports), s32)
        sheet = pltpu.VMEM((leaves, width), f32)

        def copy_out(place_ref, h_ref, mass_ref, out_ref, mine_ref, sems):
            fetch(
                sems,
                (place_ref, mine_ref.at[pl.ds(0, 3)]),
                (h_ref, mine_ref.at[3]),
                (mass_ref, mine_ref.at[4]),
            )
            fetch(sems, *[(mine_ref, out_ref.at[k]) for k in range(chips)])

        outgoing = pl.pallas_call(
            copy_out,
            out_shape=pltpu.HBM((chips, 5, leaves, width), f32),
            in_specs=[hbm] * 3,
            out_specs=hbm,
            scratch_shapes=[
                pltpu.VMEM((5, leaves, width), f32),
                pltpu.SemaphoreType.DMA((max(3, chips),)),
            ],
            compiler_params=pltpu.CompilerParams(vmem_limit_bytes=2 * MIB),
            name="copy_out",
        )(place, smoothing, mass).reshape(chips, 5 * leaves, width)
        near = lax.all_to_all(outgoing, "chip", split_axis=0, concat_axis=0, tiled=True)

        def row(own_ref, item, leaf):
            return own_ref[item, pl.ds(leaf, 1), :]

        def local_place(own_ref, mine, other):
            return [row(own_ref, X + c, other) - row(own_ref, ORIGIN + c, mine) for c in range(3)]

        def local_density(
            pair_hbm, place_hbm, h_hbm, mass_hbm, energy_hbm, old_hbm, active_hbm, own_ref, right_ref,
            centred_ref, pair_ref, active_ref, sems
        ):
            fetch(
                sems,
                (pair_hbm, pair_ref),
                (place_hbm, own_ref.at[pl.ds(X, 3)]),
                (h_hbm, own_ref.at[H]),
                (mass_hbm, own_ref.at[MASS]),
                (energy_hbm, own_ref.at[ENERGY]),
                (old_hbm, own_ref.at[OLD]),
                (active_hbm, active_ref),
            )
            h = own_ref[H]
            own_ref[ACTIVE] = active_ref[...].astype(f32)
            own_ref[INVERSE] = 1.0 / h
            own_ref[SCALE] = slope_scale(h)
            own_ref[SUM] = jnp.zeros_like(h)
            norm = jnp.zeros_like(h)
            centred = []
            for c in range(3):
                mean = jnp.sum(own_ref[X + c], axis=1, keepdims=True) * (1.0 / width)
                mean = jnp.broadcast_to(mean, h.shape)
                own_ref[ORIGIN + c] = mean
                item = own_ref[X + c] - mean
                norm = norm + item * item
                centred.append(item)
            zero, one = jnp.zeros_like(h), jnp.ones_like(h)
            rights = [-2.0 * item for item in centred] + [one, norm, zero, zero, zero]
            places = [zero] + centred + [zero] * 4
            for leaf in range(leaves):
                at = slice(leaf, leaf + 1)
                right_ref[leaf] = right_terms(jnp.concatenate([item[at] for item in rights], axis=0))
                centred_ref[leaf] = jnp.concatenate([item[at] for item in places], axis=0)

            def tile(e):
                mine, other = pair_ref[0, e], pair_ref[1, e]
                own_ref[SUM, pl.ds(mine, 1), :] = row(own_ref, SUM, mine) + density_tile(
                    right_ref[mine],
                    row(own_ref, INVERSE, mine),
                    local_place(own_ref, mine, other),
                    row(own_ref, MASS, other),
                )

            grouped(pairs, tile)

        own, right, centred = call(
            local_density,
            "local_density",
            (
                shape(TABLE, leaves, width),
                jax.ShapeDtypeStruct((leaves, 48, width), jnp.bfloat16),
                shape(leaves, 8, width),
            ),
            [hbm] * 7,
            [pair_table, pltpu.VMEM((leaves, width), s32), pltpu.SemaphoreType.DMA((7,))],
            pairs * tile_flops * 30,
            4,
        )(pair_list, place, smoothing, mass, energy, old_density, active)
        near, own = lax.optimization_barrier((near, own))
        peer = lax.ppermute(near, "core", [(0, 1), (1, 0)])

        def export(leaf_ref, route_ref, near_ref, peer_ref, own_ref, e, items):
            core = lax.axis_index("core")
            me = lax.axis_index("chip") * 2 + core
            mine, other = leaf_ref[0, e], leaf_ref[1, e]
            target = me + 1 + route_ref[0, e]
            target = jnp.where(target >= domains, target - domains, target)
            chip = target // 2
            same = (target - chip * 2) == core

            def get(c):
                at = pl.ds(c * leaves + other, 1)
                return jnp.where(same, near_ref[chip, at, :], peer_ref[chip, at, :])

            spot = [get(c) - row(own_ref, ORIGIN + c, mine) for c in range(3)]
            return mine, spot, [get(c) for c in items]

        def remote_density(
            leaf_hbm, route_hbm, own_ref, right_ref, near_ref, peer_ref, spread_ref, total, leaf_ref,
            route_ref, sems
        ):
            fetch(sems, (leaf_hbm, leaf_ref), (route_hbm, route_ref))
            total[...] = own_ref[SUM]

            def tile(e):
                mine, spot, (far_mass,) = export(
                    leaf_ref, route_ref, near_ref, peer_ref, own_ref, e, (4,)
                )
                at = pl.ds(mine, 1)
                total[at, :] = total[at, :] + density_tile(
                    right_ref[mine], row(own_ref, INVERSE, mine), spot, far_mass
                )

            grouped(exports, tile)
            inverse = own_ref[INVERSE]
            summed = (total[...] + own_ref[MASS]) * (NORM * (inverse * inverse * inverse))
            density = jnp.where(own_ref[ACTIVE] == 1.0, summed, own_ref[OLD])
            term = (ADIABATIC - 1.0) * own_ref[ENERGY] / density
            for d in range(domains):
                spread_ref[d] = term

        wire_mib = 2 * domains * leaves * width * 20 // MIB
        outgoing = call(
            remote_density,
            "remote_density",
            pltpu.HBM((domains, leaves, width), f32),
            [hbm] * 2 + [vmem] * 4,
            [sheet, leaf_table, route_table, pltpu.SemaphoreType.DMA((2,))],
            exports * tile_flops * 30,
            6 + wire_mib,
        )(export_leaves, export_route, own, right, near, peer)
        terms = lax.all_to_all(outgoing, ("chip", "core"), split_axis=0, concat_axis=0, tiled=True)

        def prepare(
            pair_hbm, leaf_hbm, route_hbm, spread_hbm, own_ref, right_ref, centred_ref, near_ref,
            peer_ref, density_ref, sum_ref, weight_ref, moment_ref, pair_ref, leaf_ref, route_ref,
            term_ref, sems
        ):
            fetch(
                sems,
                (pair_hbm, pair_ref),
                (leaf_hbm, leaf_ref),
                (route_hbm, route_ref),
                (spread_hbm.at[0], term_ref),
            )
            fresh = (ADIABATIC - 1.0) * own_ref[ENERGY] / term_ref[...]
            density_ref[...] = jnp.where(own_ref[ACTIVE] == 1.0, fresh, own_ref[OLD])
            sum_ref[...] = jnp.zeros_like(sum_ref)

            def weigh(mine, spot, inverse, scale):
                return weight_tile(
                    right_ref[mine],
                    row(own_ref, INVERSE, mine),
                    row(own_ref, SCALE, mine),
                    spot,
                    inverse,
                    scale,
                )

            def local_tile(e):
                mine, other = pair_ref[0, e], pair_ref[1, e]
                spot = local_place(own_ref, mine, other)
                weights = stack(
                    weigh(mine, spot, row(own_ref, INVERSE, other), row(own_ref, SCALE, other))
                )
                rows = moments(row(own_ref, MASS, other), spot)
                far_term, own_term = term_ref[pl.ds(other, 1), :], term_ref[pl.ds(mine, 1), :]
                sum_ref[mine] = sum_ref[mine] + force(
                    weights, rows, far_term, own_term, centred_ref[mine]
                )

            def remote_tile(e):
                mine, spot, (h, far_mass) = export(
                    leaf_ref, route_ref, near_ref, peer_ref, own_ref, e, (3, 4)
                )
                weight_ref[e] = stack(weigh(mine, spot, 1.0 / h, slope_scale(h)))
                moment_ref[e] = moments(far_mass, spot)

            grouped(pairs, local_tile)
            grouped(exports, remote_tile)

        stash_mib = 2 * exports * width * (6 * width + 32) // MIB
        density, partial, weights, rows = call(
            prepare,
            "prepare_force",
            (
                shape(leaves, width),
                shape(leaves, 4, width),
                jax.ShapeDtypeStruct((exports, 3 * width, width), jnp.bfloat16),
                pltpu.HBM((exports, 8, width), f32),
            ),
            [hbm] * 4 + [vmem] * 5,
            [pair_table, leaf_table, route_table, sheet, pltpu.SemaphoreType.DMA((4,))],
            (pairs + exports) * tile_flops * 60,
            6 + stash_mib + wire_mib,
        )(pair_list, export_leaves, export_route, kept(outgoing), own, right, centred, near, peer)

        def finish(
            leaf_hbm, route_hbm, moment_hbm, own_ref, centred_ref, terms_ref, partial_ref, weight_ref,
            accel_ref, least_ref, total, leaf_ref, route_ref, moment_ref, sems
        ):
            fetch(
                sems,
                (leaf_hbm, leaf_ref),
                (route_hbm, route_ref),
                (moment_hbm, moment_ref),
            )
            total[...] = partial_ref[...]
            me = lax.axis_index("chip") * 2 + lax.axis_index("core")

            def tile(e):
                mine, other = leaf_ref[0, e], leaf_ref[1, e]
                target = me + 1 + route_ref[0, e]
                target = jnp.where(target >= domains, target - domains, target)
                far_term = terms_ref[target, pl.ds(other, 1), :]
                total[mine] = total[mine] + force(
                    weight_ref[e],
                    moment_ref[e],
                    far_term,
                    terms_ref[me, pl.ds(mine, 1), :],
                    centred_ref[mine],
                )

            grouped(exports, tile)
            for c in range(3):
                for leaf in range(leaves):
                    accel_ref[c, leaf : leaf + 1, :] = total[leaf, c + 1 : c + 2, :]
            awake = own_ref[ACTIVE] == 1.0
            square = jnp.zeros((leaves, width), f32)
            for c in range(3):
                part = jnp.where(awake, accel_ref[c], 0.0)
                accel_ref[c] = part
                square = square + part * part
            h = own_ref[H]
            speed = jnp.sqrt(ADIABATIC * (ADIABATIC - 1.0) * own_ref[ENERGY])
            step = COURANT * h / (speed + jnp.sqrt(h * jnp.sqrt(square)))
            least_ref[...] = jnp.full(
                (members, width), jnp.min(jnp.where(awake, step, jnp.inf)), f32
            )

        accel, least = call(
            finish,
            "finish_force",
            (shape(3, leaves, width), shape(members, width)),
            [hbm] * 3 + [vmem] * 5,
            [
                pltpu.VMEM((leaves, 4, width), f32),
                leaf_table,
                route_table,
                pltpu.VMEM((exports, 8, width), f32),
                pltpu.SemaphoreType.DMA((3,)),
            ],
            exports * tile_flops * 16,
            6 + stash_mib + wire_mib,
        )(export_leaves, export_route, kept(rows), own, centred, terms, partial, weights)

        everywhere = lax.all_to_all(least, everyone, split_axis=0, concat_axis=0, tiled=True)
        return density, accel.transpose(1, 0, 2), jnp.min(everywhere)

    flat = P(everyone, None)
    deep = P(everyone, None, None)
    return jax.shard_map(
        body,
        mesh=fine,
        in_specs=(deep,) + (flat,) * 8,
        out_specs=(flat, deep, P()),
        check_vma=False,
    )
```

```python
import math

import jax
import jax.numpy as jnp
from jax import lax
from jax.experimental import pallas as pl
from jax.experimental.pallas import tpu as pltpu
from jax.sharding import Mesh, PartitionSpec as P

ADIABATIC = 5.0 / 3.0
COURANT = 0.3
GROUP = 24
TINY = 1e-30
NORM = 8.0 / math.pi
MIB = 1 << 20
X, MASS, H, INVERSE, SCALE, ORIGIN, ENERGY, OLD, ACTIVE, SUM, TABLE = 0, 3, 4, 5, 6, 7, 10, 11, 12, 13, 14


def split(item):
    first = item.astype(jnp.bfloat16).astype(jnp.float32)
    rest = item - first
    second = rest.astype(jnp.bfloat16).astype(jnp.float32)
    return first, second, rest - second


def product(a, b, dims):
    return lax.dot_general(a, b, (dims, ((), ())), preferred_element_type=jnp.float32)


def left_terms(item):
    first, second, third = split(item)
    return jnp.concatenate([first, first, second, first, third, second], axis=0).astype(jnp.bfloat16)


def right_terms(item):
    first, second, third = split(item)
    return jnp.concatenate([first, second, first, third, first, second], axis=0).astype(jnp.bfloat16)


def turn(rows):
    width, count = rows[0].shape[1], len(rows)
    rows = list(rows) + [jnp.zeros_like(rows[0])] * (-count % 8)
    turned = jnp.concatenate(rows, axis=0).T
    return [jnp.broadcast_to(turned[:, k : k + 1], (width, width)) for k in range(count)]


def separation(right, place):
    norm = place[0] * place[0] + place[1] * place[1] + place[2] * place[2]
    zero = jnp.zeros_like(norm)
    left = jnp.concatenate(place + [norm, jnp.ones_like(norm), zero, zero, zero], axis=0)
    square = jnp.maximum(product(left_terms(left), right, ((0,), (0,))), TINY)
    inverse = lax.rsqrt(square)
    return square * inverse, inverse


def density_tile(right, own_inverse, place, mass):
    (mass,) = turn([mass])
    dist, _ = separation(right, place)
    ratio = dist * own_inverse
    left = 1.0 - ratio
    inner = 1.0 - 6.0 * (ratio * ratio * left)
    remain = jnp.maximum(left, 0.0)
    outer = 2.0 * (remain * remain * remain)
    value = jnp.where(ratio < 0.5, inner, outer)
    return jnp.sum(value * mass, axis=0, keepdims=True)


def slope(dist, smooth_inverse, scale):
    ratio = dist * smooth_inverse
    remain = jnp.maximum(1.0 - ratio, 0.0)
    return jnp.where(ratio < 0.5, ratio * (2.0 - 3.0 * ratio), remain * remain) * scale


def weight_tile(right, own_inverse, own_scale, place, inverse, scale):
    inverse, scale = turn([inverse, scale])
    dist, over = separation(right, place)
    return over * (slope(dist, own_inverse, own_scale) + slope(dist, inverse, scale))


def moments(mass, place):
    half = [mass] + [mass * item for item in place]
    return jnp.concatenate(half + half, axis=0)


def force(weights, rows, far_term, own_term, own_place):
    item = lax.broadcasted_iota(jnp.int32, rows.shape, 0)
    rows = jnp.where(item < 4, rows, rows * far_term)
    rows = jnp.concatenate(split(rows), axis=0).astype(jnp.bfloat16)
    sums = product(jnp.concatenate([rows, rows, rows], axis=1), weights, ((1,), (0,)))
    sums = sums[:8] + sums[8:16] + sums[16:]
    sums = own_term * sums[:4] + sums[4:]
    return own_place[:4] * sums[:1] - sums


def stack(weights):
    return jnp.concatenate([part.astype(jnp.bfloat16) for part in split(weights)], axis=0)


def flags(index, count):
    rows, width = index.shape
    lane = lax.broadcasted_iota(jnp.int32, (rows, width), 1).astype(jnp.float32)
    blocks = [(lane + float(at) == index).astype(jnp.float32) for at in range(0, count, width)]
    return jnp.concatenate(blocks, axis=1)[:, :count]


def select(onehot, data):
    onehot = jnp.concatenate([onehot] * 3, axis=1).astype(jnp.bfloat16)
    return product(onehot, jnp.concatenate(split(data), axis=0).astype(jnp.bfloat16), ((1,), (0,)))


def by_leaf(onehot, rows):
    onehot = jnp.concatenate([onehot] * 3, axis=0).astype(jnp.bfloat16)
    return product(onehot, jnp.concatenate(split(rows), axis=0).astype(jnp.bfloat16), ((0,), (0,)))


def slope_scale(h):
    square = h * h
    return (3.0 * NORM) / (square * square)


def grouped(count, body, group=GROUP):
    step = max(d for d in range(1, min(group, count) + 1) if count % d == 0)

    def run(group, carry):
        for k in range(step):
            body(group * step + k)
        return carry

    lax.fori_loop(0, count // step, run, 0)


def fetch(sems, *pairs):
    copies = [pltpu.make_async_copy(a, b, sems.at[i]) for i, (a, b) in enumerate(pairs)]
    for copy in copies:
        copy.start()
    for copy in copies:
        copy.wait()


def solution(mesh):
    groups, domains = mesh.shape["grp"], mesh.shape["dom"]
    chips = domains // 2
    fine = Mesh(mesh.devices.reshape(groups, chips, 2), ("grp", "chip", "core"))
    everyone = ("grp", "chip", "core")
    members = groups * domains
    vmem = pl.BlockSpec(memory_space=pltpu.VMEM)
    hbm = pl.BlockSpec(memory_space=pltpu.HBM)

    def call(kernel, name, outs, ins, scratch, flops, mib):
        return pl.pallas_call(
            kernel,
            out_shape=outs,
            in_specs=ins,
            out_specs=jax.tree.map(lambda _: vmem, outs),
            scratch_shapes=scratch,
            cost_estimate=pl.CostEstimate(flops=flops, bytes_accessed=1 << 16, transcendentals=0),
            compiler_params=pltpu.CompilerParams(vmem_limit_bytes=mib * MIB),
            name=name,
        )

    def body(
        positions, smoothing, energy, mass, old_density, active, pair_list, export_leaves, export_route
    ):
        leaves, _, width = positions.shape
        pairs, exports = pair_list.shape[0], export_leaves.shape[0]
        f32, s32 = jnp.float32, jnp.int32
        tile_flops = width * width

        def shape(*sizes):
            return jax.ShapeDtypeStruct(sizes, f32)

        def kept(item):
            return pltpu.with_memory_space_constraint(item, pltpu.HBM)

        place = kept(positions.transpose(1, 0, 2))
        smoothing, energy, mass = kept(smoothing), kept(energy), kept(mass)
        old_density, active = kept(old_density), kept(active)
        pair_list, export_leaves = kept(pair_list.T), kept(export_leaves.T)
        export_route = kept(export_route.T)
        pair_table, leaf_table = pltpu.SMEM((2, pairs), s32), pltpu.SMEM((2, exports), s32)
        route_table = pltpu.SMEM((1, exports), s32)
        sheet = pltpu.VMEM((leaves, width), f32)

        def copy_out(place_ref, h_ref, mass_ref, out_ref, mine_ref, sems):
            fetch(
                sems,
                (place_ref, mine_ref.at[pl.ds(0, 3)]),
                (h_ref, mine_ref.at[3]),
                (mass_ref, mine_ref.at[4]),
            )
            fetch(sems, *[(mine_ref, out_ref.at[k]) for k in range(chips)])

        outgoing = pl.pallas_call(
            copy_out,
            out_shape=pltpu.HBM((chips, 5, leaves, width), f32),
            in_specs=[hbm] * 3,
            out_specs=hbm,
            scratch_shapes=[
                pltpu.VMEM((5, leaves, width), f32),
                pltpu.SemaphoreType.DMA((max(3, chips),)),
            ],
            compiler_params=pltpu.CompilerParams(vmem_limit_bytes=2 * MIB),
            name="copy_out",
        )(place, smoothing, mass).reshape(chips, 5 * leaves, width)
        near = lax.all_to_all(outgoing, "chip", split_axis=0, concat_axis=0, tiled=True)

        def row(own_ref, item, leaf):
            return own_ref[item, pl.ds(leaf, 1), :]

        def local_place(own_ref, mine, other):
            return [row(own_ref, X + c, other) - row(own_ref, ORIGIN + c, mine) for c in range(3)]

        def local_density(
            pair_hbm, place_hbm, h_hbm, mass_hbm, energy_hbm, old_hbm, active_hbm, leaf_hbm, route_hbm,
            own_ref, right_ref, centred_ref, right_by_ref, own_by_ref, pair_ref, active_ref, leaf_ref, route_ref, sems
        ):
            fetch(
                sems,
                (pair_hbm, pair_ref),
                (place_hbm, own_ref.at[pl.ds(X, 3)]),
                (h_hbm, own_ref.at[H]),
                (mass_hbm, own_ref.at[MASS]),
                (energy_hbm, own_ref.at[ENERGY]),
                (old_hbm, own_ref.at[OLD]),
                (active_hbm, active_ref),
                (leaf_hbm, leaf_ref),
                (route_hbm, route_ref),
            )
            h = own_ref[H]
            own_ref[ACTIVE] = active_ref[...].astype(f32)
            own_ref[INVERSE] = 1.0 / h
            own_ref[SCALE] = slope_scale(h)
            own_ref[SUM] = jnp.zeros_like(h)
            norm = jnp.zeros_like(h)
            centred = []
            for c in range(3):
                mean = jnp.sum(own_ref[X + c], axis=1, keepdims=True) * (1.0 / width)
                mean = jnp.broadcast_to(mean, h.shape)
                own_ref[ORIGIN + c] = mean
                item = own_ref[X + c] - mean
                norm = norm + item * item
                centred.append(item)
            zero, one = jnp.zeros_like(h), jnp.ones_like(h)
            rights = [-2.0 * item for item in centred] + [one, norm, zero, zero, zero]
            places = [zero] + centred + [zero] * 4
            for leaf in range(leaves):
                at = slice(leaf, leaf + 1)
                right_ref[leaf] = right_terms(jnp.concatenate([item[at] for item in rights], axis=0))
                centred_ref[leaf] = jnp.concatenate([item[at] for item in places], axis=0)

            core = lax.axis_index("core")
            me = lax.axis_index("chip") * 2 + core

            def note(e):
                mine, other = leaf_ref[0, e], leaf_ref[1, e]
                target = me + 1 + route_ref[0, e]
                target = jnp.where(target >= domains, target - domains, target)
                chip = target // 2
                spot = jnp.where(target - chip * 2 == core, chip, chip + chips) * leaves + other
                at = pl.ds(e, 1)
                sheet_of, within = e // leaves, pl.ds(e % leaves, 1)
                for k, number in enumerate((spot, target * leaves + other, mine)):
                    own_ref[TABLE + k * sheets + sheet_of, within, :] = jnp.full(
                        (1, width), number.astype(f32)
                    )
                right_by_ref[e] = right_ref[mine]
                own_by_ref[0, at, :] = row(own_ref, INVERSE, mine)
                for c in range(3):
                    own_by_ref[1 + c, at, :] = row(own_ref, ORIGIN + c, mine)

            grouped(exports, note)

            def tile(e):
                mine, other = pair_ref[0, e], pair_ref[1, e]
                own_ref[SUM, pl.ds(mine, 1), :] = row(own_ref, SUM, mine) + density_tile(
                    right_ref[mine],
                    row(own_ref, INVERSE, mine),
                    local_place(own_ref, mine, other),
                    row(own_ref, MASS, other),
                )

            grouped(pairs, tile)

        spots, sheets = domains * leaves, -(-exports // leaves)

        def indices(own_ref, kind):
            at = TABLE + kind * sheets
            return own_ref[at : at + sheets].reshape(sheets * leaves, width)[:exports]

        own, right, centred, right_by, own_by = call(
            local_density,
            "local_density",
            (
                shape(TABLE + 3 * sheets, leaves, width),
                jax.ShapeDtypeStruct((leaves, 48, width), jnp.bfloat16),
                pltpu.HBM((leaves, 8, width), f32),
                jax.ShapeDtypeStruct((exports, 48, width), jnp.bfloat16),
                shape(4, exports, width),
            ),
            [hbm] * 9,
            [
                pair_table,
                pltpu.VMEM((leaves, width), s32),
                leaf_table,
                route_table,
                pltpu.SemaphoreType.DMA((9,)),
            ],
            pairs * tile_flops * 30,
            6 + exports * spots * 16 // MIB,
        )(
            pair_list, place, smoothing, mass, energy, old_density, active, export_leaves,
            export_route,
        )
        near, own = lax.optimization_barrier((near, own))
        peer = lax.ppermute(near, "core", [(0, 1), (1, 0)])

        def export(leaf_ref, route_ref, near_ref, peer_ref, own_ref, e, items):
            core = lax.axis_index("core")
            me = lax.axis_index("chip") * 2 + core
            mine, other = leaf_ref[0, e], leaf_ref[1, e]
            target = me + 1 + route_ref[0, e]
            target = jnp.where(target >= domains, target - domains, target)
            chip = target // 2
            same = (target - chip * 2) == core

            def get(c):
                at = pl.ds(c * leaves + other, 1)
                return jnp.where(same, near_ref[chip, at, :], peer_ref[chip, at, :])

            spot = [get(c) - row(own_ref, ORIGIN + c, mine) for c in range(3)]
            return mine, spot, [get(c) for c in items]

        def remote_density(
            right_by_ref, own_by_ref, own_ref, near_ref, peer_ref, spread_ref, far_ref, rows_ref
        ):
            pick = flags(indices(own_ref, 0), spots)
            owner = flags(indices(own_ref, 2), leaves)
            for k, c in enumerate((0, 1, 2, 4)):
                at = slice(c * leaves, (c + 1) * leaves)
                data = [ref[:, at, :].reshape(spots // 2, width) for ref in (near_ref, peer_ref)]
                far_ref[k] = select(pick, jnp.concatenate(data, axis=0))
            for c in range(3):
                far_ref[c] = far_ref[c] - own_by_ref[1 + c]

            def tile(e):
                rows_ref[pl.ds(e, 1), :] = density_tile(
                    right_by_ref[e],
                    row(own_by_ref, 0, e),
                    [row(far_ref, c, e) for c in range(3)],
                    row(far_ref, 3, e),
                )

            grouped(exports, tile)
            total = own_ref[SUM] + by_leaf(owner, rows_ref[...])
            inverse = own_ref[INVERSE]
            summed = (total + own_ref[MASS]) * (NORM * (inverse * inverse * inverse))
            density = jnp.where(own_ref[ACTIVE] == 1.0, summed, own_ref[OLD])
            term = (ADIABATIC - 1.0) * own_ref[ENERGY] / density
            for d in range(domains):
                spread_ref[d] = term

        wire_mib = 2 * domains * leaves * width * 20 // MIB
        outgoing = call(
            remote_density,
            "remote_density",
            pltpu.HBM((domains, leaves, width), f32),
            [vmem] * 5,
            [pltpu.VMEM((4, exports, width), f32), pltpu.VMEM((exports, width), f32)],
            exports * tile_flops * 30,
            6 + 2 * wire_mib + exports * spots * 16 // MIB,
        )(right_by, own_by, own, near, peer)
        terms = lax.all_to_all(outgoing, ("chip", "core"), split_axis=0, concat_axis=0, tiled=True)

        def prepare(
            pair_hbm, leaf_hbm, route_hbm, spread_hbm, centred_hbm, own_ref, right_ref, near_ref,
            peer_ref, density_ref, partial_ref, weight_ref, moment_ref, pair_ref, leaf_ref, route_ref,
            term_ref, centred_ref, sum_ref, sems
        ):
            fetch(
                sems,
                (pair_hbm, pair_ref),
                (leaf_hbm, leaf_ref),
                (route_hbm, route_ref),
                (spread_hbm.at[0], term_ref),
                (centred_hbm, centred_ref),
            )
            fresh = (ADIABATIC - 1.0) * own_ref[ENERGY] / term_ref[...]
            density_ref[...] = jnp.where(own_ref[ACTIVE] == 1.0, fresh, own_ref[OLD])
            sum_ref[...] = jnp.zeros_like(sum_ref)

            def weigh(mine, spot, inverse, scale):
                return weight_tile(
                    right_ref[mine],
                    row(own_ref, INVERSE, mine),
                    row(own_ref, SCALE, mine),
                    spot,
                    inverse,
                    scale,
                )

            def local_tile(e):
                mine, other = pair_ref[0, e], pair_ref[1, e]
                spot = local_place(own_ref, mine, other)
                weights = stack(
                    weigh(mine, spot, row(own_ref, INVERSE, other), row(own_ref, SCALE, other))
                )
                rows = moments(row(own_ref, MASS, other), spot)
                far_term, own_term = term_ref[pl.ds(other, 1), :], term_ref[pl.ds(mine, 1), :]
                sum_ref[mine] = sum_ref[mine] + force(
                    weights, rows, far_term, own_term, centred_ref[mine]
                )

            def remote_tile(e):
                mine, spot, (h, far_mass) = export(
                    leaf_ref, route_ref, near_ref, peer_ref, own_ref, e, (3, 4)
                )
                weight_ref[e] = stack(weigh(mine, spot, 1.0 / h, slope_scale(h)))
                moment_ref[e, 0:8, :] = moments(far_mass, spot)
                moment_ref[e, 8:16, :] = centred_ref[mine]

            grouped(pairs, local_tile)
            grouped(exports, remote_tile)
            for c in range(3):
                for leaf in range(leaves):
                    partial_ref[c, leaf : leaf + 1, :] = sum_ref[leaf, c + 1 : c + 2, :]

        stash_mib = 2 * exports * width * (6 * width + 32) // MIB
        density, partial, weights, rows = call(
            prepare,
            "prepare_force",
            (
                shape(leaves, width),
                pltpu.HBM((3, leaves, width), f32),
                jax.ShapeDtypeStruct((exports, 3 * width, width), jnp.bfloat16),
                pltpu.HBM((exports, 16, width), f32),
            ),
            [hbm] * 5 + [vmem] * 4,
            [
                pair_table,
                leaf_table,
                route_table,
                sheet,
                pltpu.VMEM((leaves, 8, width), f32),
                pltpu.VMEM((leaves, 4, width), f32),
                pltpu.SemaphoreType.DMA((5,)),
            ],
            (pairs + exports) * tile_flops * 60,
            6 + stash_mib + wire_mib,
        )(pair_list, export_leaves, export_route, kept(outgoing), kept(centred), own, right, near, peer)

        def finish(
            moment_hbm, partial_hbm, own_ref, terms_ref, weight_ref, accel_ref, least_ref, moment_ref,
            partial_ref, far_ref, mine_ref, rows_ref, sems
        ):
            copy = pltpu.make_async_copy(moment_hbm, moment_ref, sems.at[0])
            later = pltpu.make_async_copy(partial_hbm, partial_ref, sems.at[1])
            copy.start()
            later.start()
            owner = flags(indices(own_ref, 2), leaves)
            me = lax.axis_index("chip") * 2 + lax.axis_index("core")
            far_ref[...] = select(flags(indices(own_ref, 1), spots), terms_ref[...].reshape(spots, width))
            mine_ref[...] = select(owner, terms_ref[me])
            copy.wait()

            def tile(e):
                at = pl.ds(e, 1)
                part = force(
                    weight_ref[e],
                    moment_ref[e, 0:8, :],
                    far_ref[at, :],
                    mine_ref[at, :],
                    moment_ref[e, 8:16, :],
                )
                for c in range(3):
                    rows_ref[c, at, :] = part[c + 1 : c + 2]

            grouped(exports, tile)
            later.wait()
            for c in range(3):
                accel_ref[c] = partial_ref[c] + by_leaf(owner, rows_ref[c])
            awake = own_ref[ACTIVE] == 1.0
            square = jnp.zeros((leaves, width), f32)
            for c in range(3):
                part = jnp.where(awake, accel_ref[c], 0.0)
                accel_ref[c] = part
                square = square + part * part
            h = own_ref[H]
            speed = jnp.sqrt(ADIABATIC * (ADIABATIC - 1.0) * own_ref[ENERGY])
            step = COURANT * h / (speed + jnp.sqrt(h * jnp.sqrt(square)))
            least_ref[...] = jnp.full(
                (members, width), jnp.min(jnp.where(awake, step, jnp.inf)), f32
            )

        accel, least = call(
            finish,
            "finish_force",
            (shape(3, leaves, width), shape(members, width)),
            [hbm] * 2 + [vmem] * 3,
            [
                pltpu.VMEM((exports, 16, width), f32),
                pltpu.VMEM((3, leaves, width), f32),
                pltpu.VMEM((exports, width), f32),
                pltpu.VMEM((exports, width), f32),
                pltpu.VMEM((3, exports, width), f32),
                pltpu.SemaphoreType.DMA((2,)),
            ],
            exports * tile_flops * 16,
            8 + stash_mib + wire_mib + exports * spots * 16 // MIB,
        )(kept(rows), kept(partial), own, terms, weights)

        everywhere = lax.all_to_all(least, everyone, split_axis=0, concat_axis=0, tiled=True)
        return density, accel.transpose(1, 0, 2), jnp.min(everywhere)

    flat = P(everyone, None)
    deep = P(everyone, None, None)
    return jax.shard_map(
        body,
        mesh=fine,
        in_specs=(deep,) + (flat,) * 8,
        out_specs=(flat, deep, P()),
        check_vma=False,
    )
```

```python
import math

import jax
import jax.numpy as jnp
from jax import lax
from jax.experimental import pallas as pl
from jax.experimental.pallas import tpu as pltpu
from jax.sharding import Mesh, PartitionSpec as P

ADIABATIC = 5.0 / 3.0
COURANT = 0.3
GROUP = 24
MOST = 2
TINY = 1e-30
NORM = 8.0 / math.pi
MIB = 1 << 20
X, MASS, H, INVERSE, SCALE, ORIGIN, ENERGY, OLD, ACTIVE, SUM, TABLE = 0, 3, 4, 5, 6, 7, 10, 11, 12, 13, 14


def split(item):
    first = item.astype(jnp.bfloat16).astype(jnp.float32)
    rest = item - first
    second = rest.astype(jnp.bfloat16).astype(jnp.float32)
    return first, second, rest - second


def product(a, b, dims):
    return lax.dot_general(a, b, (dims, ((), ())), preferred_element_type=jnp.float32)


def left_terms(item):
    first, second, third = split(item)
    return jnp.concatenate([first, first, second, first, third, second], axis=0).astype(jnp.bfloat16)


def right_terms(item):
    first, second, third = split(item)
    return jnp.concatenate([first, second, first, third, first, second], axis=0).astype(jnp.bfloat16)


def turn(rows):
    width, count = rows[0].shape[1], len(rows)
    rows = list(rows) + [jnp.zeros_like(rows[0])] * (-count % 8)
    turned = jnp.concatenate(rows, axis=0).T
    return [jnp.broadcast_to(turned[:, k : k + 1], (width, width)) for k in range(count)]


def separation(right, place):
    norm = place[0] * place[0] + place[1] * place[1] + place[2] * place[2]
    zero = jnp.zeros_like(norm)
    left = jnp.concatenate(place + [norm, jnp.ones_like(norm), zero, zero, zero], axis=0)
    square = jnp.maximum(product(left_terms(left), right, ((0,), (0,))), TINY)
    inverse = lax.rsqrt(square)
    return square * inverse, inverse


def density_tile(right, own_inverse, place, mass):
    (mass,) = turn([mass])
    dist, _ = separation(right, place)
    ratio = dist * own_inverse
    left = 1.0 - ratio
    inner = 1.0 - 6.0 * (ratio * ratio * left)
    remain = jnp.maximum(left, 0.0)
    outer = 2.0 * (remain * remain * remain)
    value = jnp.where(ratio < 0.5, inner, outer)
    return jnp.sum(value * mass, axis=0, keepdims=True)


def slope(dist, smooth_inverse, scale):
    ratio = dist * smooth_inverse
    remain = jnp.maximum(1.0 - ratio, 0.0)
    return jnp.where(ratio < 0.5, ratio * (2.0 - 3.0 * ratio), remain * remain) * scale


def weight_tile(right, own_inverse, own_scale, place, inverse, scale):
    inverse, scale = turn([inverse, scale])
    dist, over = separation(right, place)
    return over * (slope(dist, own_inverse, own_scale) + slope(dist, inverse, scale))


def moments(mass, place):
    half = [mass] + [mass * item for item in place]
    return jnp.concatenate(half + half, axis=0)


def force(weights, rows, far_term, own_term, own_place):
    item = lax.broadcasted_iota(jnp.int32, rows.shape, 0)
    rows = jnp.where(item < 4, rows, rows * far_term)
    rows = jnp.concatenate(split(rows), axis=0).astype(jnp.bfloat16)
    sums = product(jnp.concatenate([rows, rows, rows], axis=1), weights, ((1,), (0,)))
    sums = sums[:8] + sums[8:16] + sums[16:]
    sums = own_term * sums[:4] + sums[4:]
    return own_place[:4] * sums[:1] - sums


def stack(weights):
    return jnp.concatenate([part.astype(jnp.bfloat16) for part in split(weights)], axis=0)


def flags(index, count):
    rows, width = index.shape
    lane = lax.broadcasted_iota(jnp.int32, (rows, width), 1).astype(jnp.float32)
    blocks = [(lane + float(at) == index).astype(jnp.float32) for at in range(0, count, width)]
    return jnp.concatenate(blocks, axis=1)[:, :count]


def select(onehot, data):
    onehot = jnp.concatenate([onehot] * 3, axis=1).astype(jnp.bfloat16)
    return product(onehot, jnp.concatenate(split(data), axis=0).astype(jnp.bfloat16), ((1,), (0,)))


def by_leaf(onehot, rows):
    onehot = jnp.concatenate([onehot] * 3, axis=0).astype(jnp.bfloat16)
    return product(onehot, jnp.concatenate(split(rows), axis=0).astype(jnp.bfloat16), ((0,), (0,)))


def slope_scale(h):
    square = h * h
    return (3.0 * NORM) / (square * square)


def grouped(count, body, group=GROUP):
    step = max(d for d in range(1, min(group, count) + 1) if count % d == 0)

    def run(group, carry):
        for k in range(step):
            body(group * step + k)
        return carry

    lax.fori_loop(0, count // step, run, 0)


def fetch(sems, *pairs):
    copies = [pltpu.make_async_copy(a, b, sems.at[i]) for i, (a, b) in enumerate(pairs)]
    for copy in copies:
        copy.start()
    for copy in copies:
        copy.wait()


def solution(mesh):
    groups, domains = mesh.shape["grp"], mesh.shape["dom"]
    chips = domains // 2
    fine = Mesh(mesh.devices.reshape(groups, chips, 2), ("grp", "chip", "core"))
    everyone = ("grp", "chip", "core")
    members = groups * domains
    vmem = pl.BlockSpec(memory_space=pltpu.VMEM)
    hbm = pl.BlockSpec(memory_space=pltpu.HBM)

    def call(kernel, name, outs, ins, scratch, flops, mib):
        return pl.pallas_call(
            kernel,
            out_shape=outs,
            in_specs=ins,
            out_specs=jax.tree.map(lambda _: vmem, outs),
            scratch_shapes=scratch,
            cost_estimate=pl.CostEstimate(flops=flops, bytes_accessed=1 << 16, transcendentals=0),
            compiler_params=pltpu.CompilerParams(vmem_limit_bytes=mib * MIB),
            name=name,
        )

    def body(
        positions, smoothing, energy, mass, old_density, active, pair_list, export_leaves, export_route
    ):
        leaves, _, width = positions.shape
        pairs, exports = pair_list.shape[0], export_leaves.shape[0]
        f32, s32 = jnp.float32, jnp.int32
        tile_flops = width * width

        def shape(*sizes):
            return jax.ShapeDtypeStruct(sizes, f32)

        def kept(item):
            return pltpu.with_memory_space_constraint(item, pltpu.HBM)

        place = kept(positions.transpose(1, 0, 2))
        smoothing, energy, mass = kept(smoothing), kept(energy), kept(mass)
        old_density, active = kept(old_density), kept(active)
        pair_list, export_leaves = kept(pair_list.T), kept(export_leaves.T)
        export_route = kept(export_route.T)
        pair_table, leaf_table = pltpu.SMEM((2, pairs), s32), pltpu.SMEM((2, exports), s32)
        route_table = pltpu.SMEM((1, exports), s32)
        sheet = pltpu.VMEM((leaves, width), f32)

        def copy_out(place_ref, h_ref, mass_ref, out_ref, mine_ref, sems):
            fetch(
                sems,
                (place_ref, mine_ref.at[pl.ds(0, 3)]),
                (h_ref, mine_ref.at[3]),
                (mass_ref, mine_ref.at[4]),
            )
            fetch(sems, *[(mine_ref, out_ref.at[k]) for k in range(chips)])

        outgoing = pl.pallas_call(
            copy_out,
            out_shape=pltpu.HBM((chips, 5, leaves, width), f32),
            in_specs=[hbm] * 3,
            out_specs=hbm,
            scratch_shapes=[
                pltpu.VMEM((5, leaves, width), f32),
                pltpu.SemaphoreType.DMA((max(3, chips),)),
            ],
            compiler_params=pltpu.CompilerParams(vmem_limit_bytes=2 * MIB),
            name="copy_out",
        )(place, smoothing, mass).reshape(chips, 5 * leaves, width)
        near = lax.all_to_all(outgoing, "chip", split_axis=0, concat_axis=0, tiled=True)

        def row(own_ref, item, leaf):
            return own_ref[item, pl.ds(leaf, 1), :]

        def local_place(own_ref, mine, other):
            return [row(own_ref, X + c, other) - row(own_ref, ORIGIN + c, mine) for c in range(3)]

        def local_density(
            pair_hbm, place_hbm, h_hbm, mass_hbm, energy_hbm, old_hbm, active_hbm, leaf_hbm, route_hbm,
            own_ref, right_ref, centred_ref, right_by_ref, own_by_ref, pair_ref, active_ref, leaf_ref, route_ref, sems
        ):
            fetch(
                sems,
                (pair_hbm, pair_ref),
                (place_hbm, own_ref.at[pl.ds(X, 3)]),
                (h_hbm, own_ref.at[H]),
                (mass_hbm, own_ref.at[MASS]),
                (energy_hbm, own_ref.at[ENERGY]),
                (old_hbm, own_ref.at[OLD]),
                (active_hbm, active_ref),
                (leaf_hbm, leaf_ref),
                (route_hbm, route_ref),
            )
            h = own_ref[H]
            own_ref[ACTIVE] = active_ref[...].astype(f32)
            own_ref[INVERSE] = 1.0 / h
            own_ref[SCALE] = slope_scale(h)
            own_ref[SUM] = jnp.zeros_like(h)
            norm = jnp.zeros_like(h)
            centred = []
            for c in range(3):
                mean = jnp.sum(own_ref[X + c], axis=1, keepdims=True) * (1.0 / width)
                mean = jnp.broadcast_to(mean, h.shape)
                own_ref[ORIGIN + c] = mean
                item = own_ref[X + c] - mean
                norm = norm + item * item
                centred.append(item)
            zero, one = jnp.zeros_like(h), jnp.ones_like(h)
            rights = [-2.0 * item for item in centred] + [one, norm, zero, zero, zero]
            places = [zero] + centred + [zero] * 4
            for leaf in range(leaves):
                at = slice(leaf, leaf + 1)
                right_ref[leaf] = right_terms(jnp.concatenate([item[at] for item in rights], axis=0))
                centred_ref[leaf] = jnp.concatenate([item[at] for item in places], axis=0)

            core = lax.axis_index("core")
            me = lax.axis_index("chip") * 2 + core

            own_ref[pl.ds(TABLE, 4 * sheets)] = jnp.full((4 * sheets, leaves, width), -1.0, f32)
            right_by_ref[...] = jnp.zeros_like(right_by_ref)
            own_by_ref[...] = jnp.zeros_like(own_by_ref)

            def write(kind, at, number):
                own_ref[TABLE + kind * sheets + at // leaves, pl.ds(at % leaves, 1), :] = jnp.full(
                    (1, width), number.astype(f32)
                )

            def note(e, used):
                mine, other = leaf_ref[0, e], leaf_ref[1, e]
                target = me + 1 + route_ref[0, e]
                target = jnp.where(target >= domains, target - domains, target)
                chip = target // 2
                same = (target - chip * 2 == core).astype(s32)
                slot = jnp.where(same == 1, used[0], near_slots + used[1])
                write(0, slot, chip * leaves + other)
                write(1, e, target * leaves + other)
                write(2, e, mine)
                write(3, slot, mine)
                at = pl.ds(slot, 1)
                right_by_ref[slot] = right_ref[mine]
                own_by_ref[0, at, :] = row(own_ref, INVERSE, mine)
                for c in range(3):
                    own_by_ref[1 + c, at, :] = row(own_ref, ORIGIN + c, mine)
                return used[0] + same, used[1] + 1 - same

            lax.fori_loop(0, exports, note, (jnp.int32(0), jnp.int32(0)))

            def tile(e):
                mine, other = pair_ref[0, e], pair_ref[1, e]
                own_ref[SUM, pl.ds(mine, 1), :] = row(own_ref, SUM, mine) + density_tile(
                    right_ref[mine],
                    row(own_ref, INVERSE, mine),
                    local_place(own_ref, mine, other),
                    row(own_ref, MASS, other),
                )

            grouped(pairs, tile)

        near_slots = -(-min(exports, MOST * (chips - 1)) // 8) * 8
        peer_slots = -(-min(exports, MOST * chips) // 8) * 8
        slots = near_slots + peer_slots
        spots, sheets = domains * leaves, -(-max(exports, slots) // leaves)

        def indices(own_ref, kind, first, count):
            at = TABLE + kind * sheets
            return own_ref[at : at + sheets].reshape(sheets * leaves, width)[first : first + count]

        own, right, centred, right_by, own_by = call(
            local_density,
            "local_density",
            (
                shape(TABLE + 4 * sheets, leaves, width),
                jax.ShapeDtypeStruct((leaves, 48, width), jnp.bfloat16),
                pltpu.HBM((leaves, 8, width), f32),
                jax.ShapeDtypeStruct((slots, 48, width), jnp.bfloat16),
                shape(4, slots, width),
            ),
            [hbm] * 9,
            [
                pair_table,
                pltpu.VMEM((leaves, width), s32),
                leaf_table,
                route_table,
                pltpu.SemaphoreType.DMA((9,)),
            ],
            pairs * tile_flops * 30,
            6 + exports * spots * 16 // MIB,
        )(
            pair_list, place, smoothing, mass, energy, old_density, active, export_leaves,
            export_route,
        )
        near, own = lax.optimization_barrier((near, own))
        peer = lax.ppermute(near, "core", [(0, 1), (1, 0)])

        def export(leaf_ref, route_ref, near_ref, peer_ref, own_ref, e, items):
            core = lax.axis_index("core")
            me = lax.axis_index("chip") * 2 + core
            mine, other = leaf_ref[0, e], leaf_ref[1, e]
            target = me + 1 + route_ref[0, e]
            target = jnp.where(target >= domains, target - domains, target)
            chip = target // 2
            same = (target - chip * 2) == core

            def get(c):
                at = pl.ds(c * leaves + other, 1)
                return jnp.where(same, near_ref[chip, at, :], peer_ref[chip, at, :])

            spot = [get(c) - row(own_ref, ORIGIN + c, mine) for c in range(3)]
            return mine, spot, [get(c) for c in items]

        def slot_density(first, count, right_by_ref, own_by_ref, own_ref, data_ref, far_ref, rows_ref):
            pick = flags(indices(own_ref, 0, first, count), spots // 2)
            owner = flags(indices(own_ref, 3, first, count), leaves)
            for k, c in enumerate((0, 1, 2, 4)):
                data = data_ref[:, c * leaves : (c + 1) * leaves, :].reshape(spots // 2, width)
                far_ref[k] = select(pick, data)
            for c in range(3):
                far_ref[c] = far_ref[c] - own_by_ref[1 + c, first : first + count]

            def tile(e):
                rows_ref[pl.ds(e, 1), :] = density_tile(
                    right_by_ref[first + e],
                    row(own_by_ref, 0, first + e),
                    [row(far_ref, c, e) for c in range(3)],
                    row(far_ref, 3, e),
                )

            grouped(count, tile)
            return by_leaf(owner, rows_ref[...])

        def near_density(right_by_ref, own_by_ref, own_ref, near_ref, sum_ref, far_ref, rows_ref):
            sum_ref[...] = own_ref[SUM] + slot_density(
                0, near_slots, right_by_ref, own_by_ref, own_ref, near_ref, far_ref, rows_ref
            )

        wire_mib = 2 * domains * leaves * width * 20 // MIB
        near_sum = call(
            near_density,
            "near_density",
            shape(leaves, width),
            [vmem] * 4,
            [pltpu.VMEM((4, near_slots, width), f32), pltpu.VMEM((near_slots, width), f32)],
            near_slots * tile_flops * 30,
            6 + wire_mib + exports * spots * 16 // MIB,
        )(right_by, own_by, own, near)

        def peer_density(
            right_by_ref, own_by_ref, own_ref, sum_ref, peer_ref, spread_ref, far_ref, rows_ref
        ):
            total = sum_ref[...] + slot_density(
                near_slots, peer_slots, right_by_ref, own_by_ref, own_ref, peer_ref, far_ref, rows_ref
            )
            inverse = own_ref[INVERSE]
            summed = (total + own_ref[MASS]) * (NORM * (inverse * inverse * inverse))
            density = jnp.where(own_ref[ACTIVE] == 1.0, summed, own_ref[OLD])
            term = (ADIABATIC - 1.0) * own_ref[ENERGY] / density
            for d in range(domains):
                spread_ref[d] = term

        outgoing = call(
            peer_density,
            "peer_density",
            pltpu.HBM((domains, leaves, width), f32),
            [vmem] * 5,
            [pltpu.VMEM((4, peer_slots, width), f32), pltpu.VMEM((peer_slots, width), f32)],
            peer_slots * tile_flops * 30,
            6 + 2 * wire_mib + exports * spots * 16 // MIB,
        )(right_by, own_by, own, near_sum, peer)
        terms = lax.all_to_all(outgoing, ("chip", "core"), split_axis=0, concat_axis=0, tiled=True)

        def prepare(
            pair_hbm, leaf_hbm, route_hbm, spread_hbm, centred_hbm, own_ref, right_ref, near_ref,
            peer_ref, density_ref, partial_ref, weight_ref, moment_ref, pair_ref, leaf_ref, route_ref,
            term_ref, centred_ref, sum_ref, sems
        ):
            fetch(
                sems,
                (pair_hbm, pair_ref),
                (leaf_hbm, leaf_ref),
                (route_hbm, route_ref),
                (spread_hbm.at[0], term_ref),
                (centred_hbm, centred_ref),
            )
            fresh = (ADIABATIC - 1.0) * own_ref[ENERGY] / term_ref[...]
            density_ref[...] = jnp.where(own_ref[ACTIVE] == 1.0, fresh, own_ref[OLD])
            sum_ref[...] = jnp.zeros_like(sum_ref)

            def weigh(mine, spot, inverse, scale):
                return weight_tile(
                    right_ref[mine],
                    row(own_ref, INVERSE, mine),
                    row(own_ref, SCALE, mine),
                    spot,
                    inverse,
                    scale,
                )

            def local_tile(e):
                mine, other = pair_ref[0, e], pair_ref[1, e]
                spot = local_place(own_ref, mine, other)
                weights = stack(
                    weigh(mine, spot, row(own_ref, INVERSE, other), row(own_ref, SCALE, other))
                )
                rows = moments(row(own_ref, MASS, other), spot)
                far_term, own_term = term_ref[pl.ds(other, 1), :], term_ref[pl.ds(mine, 1), :]
                sum_ref[mine] = sum_ref[mine] + force(
                    weights, rows, far_term, own_term, centred_ref[mine]
                )

            def remote_tile(e):
                mine, spot, (h, far_mass) = export(
                    leaf_ref, route_ref, near_ref, peer_ref, own_ref, e, (3, 4)
                )
                weight_ref[e] = stack(weigh(mine, spot, 1.0 / h, slope_scale(h)))
                moment_ref[e, 0:8, :] = moments(far_mass, spot)
                moment_ref[e, 8:16, :] = centred_ref[mine]

            grouped(pairs, local_tile)
            grouped(exports, remote_tile)
            for c in range(3):
                for leaf in range(leaves):
                    partial_ref[c, leaf : leaf + 1, :] = sum_ref[leaf, c + 1 : c + 2, :]

        stash_mib = 2 * exports * width * (6 * width + 32) // MIB
        density, partial, weights, rows = call(
            prepare,
            "prepare_force",
            (
                shape(leaves, width),
                pltpu.HBM((3, leaves, width), f32),
                jax.ShapeDtypeStruct((exports, 3 * width, width), jnp.bfloat16),
                pltpu.HBM((exports, 16, width), f32),
            ),
            [hbm] * 5 + [vmem] * 4,
            [
                pair_table,
                leaf_table,
                route_table,
                sheet,
                pltpu.VMEM((leaves, 8, width), f32),
                pltpu.VMEM((leaves, 4, width), f32),
                pltpu.SemaphoreType.DMA((5,)),
            ],
            (pairs + exports) * tile_flops * 60,
            6 + stash_mib + wire_mib,
        )(pair_list, export_leaves, export_route, kept(outgoing), kept(centred), own, right, near, peer)

        def finish(
            moment_hbm, partial_hbm, own_ref, terms_ref, weight_ref, accel_hbm, least_ref, accel_ref,
            moment_ref, partial_ref, far_ref, mine_ref, rows_ref, sems
        ):
            copy = pltpu.make_async_copy(moment_hbm, moment_ref, sems.at[0])
            later = pltpu.make_async_copy(partial_hbm, partial_ref, sems.at[1])
            copy.start()
            later.start()
            owner = flags(indices(own_ref, 2, 0, exports), leaves)
            me = lax.axis_index("chip") * 2 + lax.axis_index("core")
            far_ref[...] = select(flags(indices(own_ref, 1, 0, exports), spots), terms_ref[...].reshape(spots, width))
            mine_ref[...] = select(owner, terms_ref[me])
            copy.wait()

            def tile(e):
                at = pl.ds(e, 1)
                part = force(
                    weight_ref[e],
                    moment_ref[e, 0:8, :],
                    far_ref[at, :],
                    mine_ref[at, :],
                    moment_ref[e, 8:16, :],
                )
                for c in range(3):
                    rows_ref[c, at, :] = part[c + 1 : c + 2]

            grouped(exports, tile)
            later.wait()
            for c in range(3):
                accel_ref[c] = partial_ref[c] + by_leaf(owner, rows_ref[c])
            awake = own_ref[ACTIVE] == 1.0
            square = jnp.zeros((leaves, width), f32)
            for c in range(3):
                part = jnp.where(awake, accel_ref[c], 0.0)
                accel_ref[c] = part
                square = square + part * part
            done = pltpu.make_async_copy(accel_ref, accel_hbm, sems.at[2])
            done.start()
            h = own_ref[H]
            speed = jnp.sqrt(ADIABATIC * (ADIABATIC - 1.0) * own_ref[ENERGY])
            step = COURANT * h / (speed + jnp.sqrt(h * jnp.sqrt(square)))
            least_ref[...] = jnp.full(
                (members, width), jnp.min(jnp.where(awake, step, jnp.inf)), f32
            )
            done.wait()

        accel, least = pl.pallas_call(
            finish,
            out_shape=(pltpu.HBM((3, leaves, width), f32), shape(members, width)),
            in_specs=[hbm] * 2 + [vmem] * 3,
            out_specs=(hbm, vmem),
            scratch_shapes=[
                pltpu.VMEM((3, leaves, width), f32),
                pltpu.VMEM((exports, 16, width), f32),
                pltpu.VMEM((3, leaves, width), f32),
                pltpu.VMEM((exports, width), f32),
                pltpu.VMEM((exports, width), f32),
                pltpu.VMEM((3, exports, width), f32),
                pltpu.SemaphoreType.DMA((3,)),
            ],
            compiler_params=pltpu.CompilerParams(
                vmem_limit_bytes=(8 + stash_mib + wire_mib + exports * spots * 16 // MIB) * MIB
            ),
            name="finish_force",
        )(kept(rows), kept(partial), own, terms, weights)

        everywhere = lax.all_to_all(least, everyone, split_axis=0, concat_axis=0, tiled=True)
        return density, accel.transpose(1, 0, 2), jnp.min(everywhere)

    flat = P(everyone, None)
    deep = P(everyone, None, None)
    return jax.shard_map(
        body,
        mesh=fine,
        in_specs=(deep,) + (flat,) * 8,
        out_specs=(flat, deep, P()),
        check_vma=False,
    )
```

```python
import math

import jax
import jax.numpy as jnp
from jax import lax
from jax.experimental import pallas as pl
from jax.experimental.pallas import tpu as pltpu
from jax.sharding import Mesh, PartitionSpec as P

ADIABATIC = 5.0 / 3.0
COURANT = 0.3
GROUP = 24
MOST = 2
TINY = 1e-30
NORM = 8.0 / math.pi
MIB = 1 << 20
X, MASS, H, INVERSE, SCALE, ORIGIN, ENERGY, OLD, ACTIVE, SUM, TABLE = 0, 3, 4, 5, 6, 7, 10, 11, 12, 13, 14


def split(item):
    first = item.astype(jnp.bfloat16).astype(jnp.float32)
    rest = item - first
    second = rest.astype(jnp.bfloat16).astype(jnp.float32)
    return first, second, rest - second


def product(a, b, dims):
    return lax.dot_general(a, b, (dims, ((), ())), preferred_element_type=jnp.float32)


def left_terms(item):
    first, second, third = split(item)
    return jnp.concatenate([first, first, second, first, third, second], axis=0).astype(jnp.bfloat16)


def right_terms(item):
    first, second, third = split(item)
    return jnp.concatenate([first, second, first, third, first, second], axis=0).astype(jnp.bfloat16)


def turn(rows):
    width, count = rows[0].shape[1], len(rows)
    rows = list(rows) + [jnp.zeros_like(rows[0])] * (-count % 8)
    turned = jnp.concatenate(rows, axis=0).T
    return [jnp.broadcast_to(turned[:, k : k + 1], (width, width)) for k in range(count)]


def separation(right, place):
    norm = place[0] * place[0] + place[1] * place[1] + place[2] * place[2]
    zero = jnp.zeros_like(norm)
    left = jnp.concatenate(place + [norm, jnp.ones_like(norm), zero, zero, zero], axis=0)
    square = jnp.maximum(product(left_terms(left), right, ((0,), (0,))), TINY)
    inverse = lax.rsqrt(square)
    return square * inverse, inverse


def density_tile(right, own_inverse, place, mass):
    (mass,) = turn([mass])
    dist, _ = separation(right, place)
    ratio = dist * own_inverse
    left = 1.0 - ratio
    inner = 1.0 - 6.0 * (ratio * ratio * left)
    remain = jnp.maximum(left, 0.0)
    outer = 2.0 * (remain * remain * remain)
    value = jnp.where(ratio < 0.5, inner, outer)
    return jnp.sum(value * mass, axis=0, keepdims=True)


def slope(dist, smooth_inverse, scale):
    ratio = dist * smooth_inverse
    remain = jnp.maximum(1.0 - ratio, 0.0)
    return jnp.where(ratio < 0.5, ratio * (2.0 - 3.0 * ratio), remain * remain) * scale


def weight_tile(right, own_inverse, own_scale, place, inverse, scale):
    inverse, scale = turn([inverse, scale])
    dist, over = separation(right, place)
    return over * (slope(dist, own_inverse, own_scale) + slope(dist, inverse, scale))


def moments(mass, place):
    half = [mass] + [mass * item for item in place]
    return jnp.concatenate(half + half, axis=0)


def force(weights, rows, far_term, own_term, own_place):
    item = lax.broadcasted_iota(jnp.int32, rows.shape, 0)
    rows = jnp.where(item < 4, rows, rows * far_term)
    rows = jnp.concatenate(split(rows), axis=0).astype(jnp.bfloat16)
    sums = product(jnp.concatenate([rows, rows, rows], axis=1), weights, ((1,), (0,)))
    sums = sums[:8] + sums[8:16] + sums[16:]
    sums = own_term * sums[:4] + sums[4:]
    return own_place[:4] * sums[:1] - sums


def stack(weights):
    return jnp.concatenate([part.astype(jnp.bfloat16) for part in split(weights)], axis=0)


def flags(index, count):
    rows, width = index.shape
    lane = lax.broadcasted_iota(jnp.int32, (rows, width), 1).astype(jnp.float32)
    blocks = [(lane + float(at) == index).astype(jnp.float32) for at in range(0, count, width)]
    return jnp.concatenate(blocks, axis=1)[:, :count]


def select(onehot, data):
    onehot = jnp.concatenate([onehot] * 3, axis=1).astype(jnp.bfloat16)
    return product(onehot, jnp.concatenate(split(data), axis=0).astype(jnp.bfloat16), ((1,), (0,)))


def by_leaf(onehot, rows):
    onehot = jnp.concatenate([onehot] * 3, axis=0).astype(jnp.bfloat16)
    return product(onehot, jnp.concatenate(split(rows), axis=0).astype(jnp.bfloat16), ((0,), (0,)))


def slope_scale(h):
    square = h * h
    return (3.0 * NORM) / (square * square)


def grouped(count, body, group=GROUP):
    step = max(d for d in range(1, min(group, count) + 1) if count % d == 0)

    def run(group, carry):
        for k in range(step):
            body(group * step + k)
        return carry

    lax.fori_loop(0, count // step, run, 0)


def fetch(sems, *pairs):
    copies = [pltpu.make_async_copy(a, b, sems.at[i]) for i, (a, b) in enumerate(pairs)]
    for copy in copies:
        copy.start()
    for copy in copies:
        copy.wait()


def solution(mesh):
    groups, domains = mesh.shape["grp"], mesh.shape["dom"]
    chips = domains // 2
    fine = Mesh(mesh.devices.reshape(groups, chips, 2), ("grp", "chip", "core"))
    everyone = ("grp", "chip", "core")
    members = groups * domains
    vmem = pl.BlockSpec(memory_space=pltpu.VMEM)
    hbm = pl.BlockSpec(memory_space=pltpu.HBM)

    def call(kernel, name, outs, ins, scratch, flops, mib):
        return pl.pallas_call(
            kernel,
            out_shape=outs,
            in_specs=ins,
            out_specs=jax.tree.map(lambda _: vmem, outs),
            scratch_shapes=scratch,
            cost_estimate=pl.CostEstimate(flops=flops, bytes_accessed=1 << 16, transcendentals=0),
            compiler_params=pltpu.CompilerParams(vmem_limit_bytes=mib * MIB),
            name=name,
        )

    def body(
        positions, smoothing, energy, mass, old_density, active, pair_list, export_leaves, export_route
    ):
        leaves, _, width = positions.shape
        pairs, exports = pair_list.shape[0], export_leaves.shape[0]
        f32, s32 = jnp.float32, jnp.int32
        tile_flops = width * width

        def shape(*sizes):
            return jax.ShapeDtypeStruct(sizes, f32)

        def kept(item):
            return pltpu.with_memory_space_constraint(item, pltpu.HBM)

        place = kept(positions.transpose(1, 0, 2))
        smoothing, energy, mass = kept(smoothing), kept(energy), kept(mass)
        old_density, active = kept(old_density), kept(active)
        pair_list, export_leaves = kept(pair_list.T), kept(export_leaves.T)
        export_route = kept(export_route.T)
        pair_table, leaf_table = pltpu.SMEM((2, pairs), s32), pltpu.SMEM((2, exports), s32)
        route_table = pltpu.SMEM((1, exports), s32)
        sheet = pltpu.VMEM((leaves, width), f32)

        def copy_out(place_ref, h_ref, mass_ref, out_ref, mine_ref, sems):
            fetch(
                sems,
                (place_ref, mine_ref.at[pl.ds(0, 3)]),
                (h_ref, mine_ref.at[3]),
                (mass_ref, mine_ref.at[4]),
            )
            fetch(sems, *[(mine_ref, out_ref.at[k]) for k in range(chips)])

        outgoing = pl.pallas_call(
            copy_out,
            out_shape=pltpu.HBM((chips, 5, leaves, width), f32),
            in_specs=[hbm] * 3,
            out_specs=hbm,
            scratch_shapes=[
                pltpu.VMEM((5, leaves, width), f32),
                pltpu.SemaphoreType.DMA((max(3, chips),)),
            ],
            compiler_params=pltpu.CompilerParams(vmem_limit_bytes=2 * MIB),
            name="copy_out",
        )(place, smoothing, mass).reshape(chips, 5 * leaves, width)
        near = lax.all_to_all(outgoing, "chip", split_axis=0, concat_axis=0, tiled=True)

        def row(own_ref, item, leaf):
            return own_ref[item, pl.ds(leaf, 1), :]

        def local_place(own_ref, mine, other):
            return [row(own_ref, X + c, other) - row(own_ref, ORIGIN + c, mine) for c in range(3)]

        def local_density(
            pair_hbm, place_hbm, h_hbm, mass_hbm, energy_hbm, old_hbm, active_hbm, leaf_hbm, route_hbm,
            own_ref, right_ref, centred_ref, right_by_ref, own_by_ref, pair_ref, active_ref, leaf_ref, route_ref, sems
        ):
            fetch(
                sems,
                (pair_hbm, pair_ref),
                (place_hbm, own_ref.at[pl.ds(X, 3)]),
                (h_hbm, own_ref.at[H]),
                (mass_hbm, own_ref.at[MASS]),
                (energy_hbm, own_ref.at[ENERGY]),
                (old_hbm, own_ref.at[OLD]),
                (active_hbm, active_ref),
                (leaf_hbm, leaf_ref),
                (route_hbm, route_ref),
            )
            h = own_ref[H]
            own_ref[ACTIVE] = active_ref[...].astype(f32)
            own_ref[INVERSE] = 1.0 / h
            own_ref[SCALE] = slope_scale(h)
            own_ref[SUM] = jnp.zeros_like(h)
            norm = jnp.zeros_like(h)
            centred = []
            for c in range(3):
                mean = jnp.sum(own_ref[X + c], axis=1, keepdims=True) * (1.0 / width)
                mean = jnp.broadcast_to(mean, h.shape)
                own_ref[ORIGIN + c] = mean
                item = own_ref[X + c] - mean
                norm = norm + item * item
                centred.append(item)
            zero, one = jnp.zeros_like(h), jnp.ones_like(h)
            rights = [-2.0 * item for item in centred] + [one, norm, zero, zero, zero]
            places = [zero] + centred + [zero] * 4
            for leaf in range(leaves):
                at = slice(leaf, leaf + 1)
                right_ref[leaf] = right_terms(jnp.concatenate([item[at] for item in rights], axis=0))
                centred_ref[leaf] = jnp.concatenate([item[at] for item in places], axis=0)

            core = lax.axis_index("core")
            me = lax.axis_index("chip") * 2 + core

            own_ref[pl.ds(TABLE, 4 * sheets)] = jnp.full((4 * sheets, leaves, width), -1.0, f32)
            right_by_ref[...] = jnp.zeros_like(right_by_ref)
            own_by_ref[...] = jnp.zeros_like(own_by_ref)

            def write(kind, at, number):
                own_ref[TABLE + kind * sheets + at // leaves, pl.ds(at % leaves, 1), :] = jnp.full(
                    (1, width), number.astype(f32)
                )

            def note(e, used):
                mine, other = leaf_ref[0, e], leaf_ref[1, e]
                target = me + 1 + route_ref[0, e]
                target = jnp.where(target >= domains, target - domains, target)
                chip = target // 2
                same = (target - chip * 2 == core).astype(s32)
                slot = jnp.where(same == 1, used[0], near_slots + used[1])
                write(0, slot, chip * leaves + other)
                write(1, e, target * leaves + other)
                write(2, e, mine)
                write(3, slot, mine)
                at = pl.ds(slot, 1)
                right_by_ref[slot] = right_ref[mine]
                own_by_ref[0, at, :] = row(own_ref, INVERSE, mine)
                for c in range(3):
                    own_by_ref[1 + c, at, :] = row(own_ref, ORIGIN + c, mine)
                return used[0] + same, used[1] + 1 - same

            lax.fori_loop(0, exports, note, (jnp.int32(0), jnp.int32(0)))

            def tile(e):
                mine, other = pair_ref[0, e], pair_ref[1, e]
                own_ref[SUM, pl.ds(mine, 1), :] = row(own_ref, SUM, mine) + density_tile(
                    right_ref[mine],
                    row(own_ref, INVERSE, mine),
                    local_place(own_ref, mine, other),
                    row(own_ref, MASS, other),
                )

            grouped(pairs, tile)

        near_slots = -(-min(exports, MOST * (chips - 1)) // 8) * 8
        peer_slots = -(-min(exports, MOST * chips) // 8) * 8
        slots = near_slots + peer_slots
        spots, sheets = domains * leaves, -(-max(exports, slots) // leaves)

        def indices(own_ref, kind, first, count):
            at = TABLE + kind * sheets
            return own_ref[at : at + sheets].reshape(sheets * leaves, width)[first : first + count]

        own, right, centred, right_by, own_by = call(
            local_density,
            "local_density",
            (
                shape(TABLE + 4 * sheets, leaves, width),
                pltpu.HBM((leaves, 48, width), jnp.bfloat16),
                pltpu.HBM((leaves, 8, width), f32),
                jax.ShapeDtypeStruct((slots, 48, width), jnp.bfloat16),
                shape(4, slots, width),
            ),
            [hbm] * 9,
            [
                pair_table,
                pltpu.VMEM((leaves, width), s32),
                leaf_table,
                route_table,
                pltpu.SemaphoreType.DMA((9,)),
            ],
            pairs * tile_flops * 30,
            6 + exports * spots * 16 // MIB,
        )(
            pair_list, place, smoothing, mass, energy, old_density, active, export_leaves,
            export_route,
        )
        near, own = lax.optimization_barrier((near, own))
        peer = lax.ppermute(near, "core", [(0, 1), (1, 0)])

        def export(leaf_ref, route_ref, near_ref, peer_ref, own_ref, e, items):
            core = lax.axis_index("core")
            me = lax.axis_index("chip") * 2 + core
            mine, other = leaf_ref[0, e], leaf_ref[1, e]
            target = me + 1 + route_ref[0, e]
            target = jnp.where(target >= domains, target - domains, target)
            chip = target // 2
            same = (target - chip * 2) == core

            def get(c):
                at = pl.ds(c * leaves + other, 1)
                return jnp.where(same, near_ref[chip, at, :], peer_ref[chip, at, :])

            spot = [get(c) - row(own_ref, ORIGIN + c, mine) for c in range(3)]
            return mine, spot, [get(c) for c in items]

        def slot_density(first, count, right_by_ref, own_by_ref, own_ref, data_ref, far_ref, rows_ref):
            pick = flags(indices(own_ref, 0, first, count), spots // 2)
            owner = flags(indices(own_ref, 3, first, count), leaves)
            for k, c in enumerate((0, 1, 2, 4)):
                data = data_ref[:, c * leaves : (c + 1) * leaves, :].reshape(spots // 2, width)
                far_ref[k] = select(pick, data)
            for c in range(3):
                far_ref[c] = far_ref[c] - own_by_ref[1 + c, first : first + count]

            def tile(e):
                rows_ref[pl.ds(e, 1), :] = density_tile(
                    right_by_ref[first + e],
                    row(own_by_ref, 0, first + e),
                    [row(far_ref, c, e) for c in range(3)],
                    row(far_ref, 3, e),
                )

            grouped(count, tile)
            return by_leaf(owner, rows_ref[...])

        def near_density(right_by_ref, own_by_ref, own_ref, near_ref, sum_ref, far_ref, rows_ref):
            sum_ref[...] = own_ref[SUM] + slot_density(
                0, near_slots, right_by_ref, own_by_ref, own_ref, near_ref, far_ref, rows_ref
            )

        wire_mib = 2 * domains * leaves * width * 20 // MIB
        near_sum = call(
            near_density,
            "near_density",
            shape(leaves, width),
            [vmem] * 4,
            [pltpu.VMEM((4, near_slots, width), f32), pltpu.VMEM((near_slots, width), f32)],
            near_slots * tile_flops * 30,
            6 + wire_mib + exports * spots * 16 // MIB,
        )(right_by, own_by, own, near)

        def peer_density(
            right_by_ref, own_by_ref, own_ref, sum_ref, peer_ref, spread_ref, far_ref, rows_ref
        ):
            total = sum_ref[...] + slot_density(
                near_slots, peer_slots, right_by_ref, own_by_ref, own_ref, peer_ref, far_ref, rows_ref
            )
            inverse = own_ref[INVERSE]
            summed = (total + own_ref[MASS]) * (NORM * (inverse * inverse * inverse))
            density = jnp.where(own_ref[ACTIVE] == 1.0, summed, own_ref[OLD])
            term = (ADIABATIC - 1.0) * own_ref[ENERGY] / density
            for d in range(domains):
                spread_ref[d] = term

        outgoing = call(
            peer_density,
            "peer_density",
            pltpu.HBM((domains, leaves, width), f32),
            [vmem] * 5,
            [pltpu.VMEM((4, peer_slots, width), f32), pltpu.VMEM((peer_slots, width), f32)],
            peer_slots * tile_flops * 30,
            6 + 2 * wire_mib + exports * spots * 16 // MIB,
        )(right_by, own_by, own, near_sum, peer)
        terms = lax.all_to_all(outgoing, ("chip", "core"), split_axis=0, concat_axis=0, tiled=True)

        def prepare(
            pair_hbm, leaf_hbm, route_hbm, spread_hbm, centred_hbm, right_hbm, own_ref, near_ref,
            peer_ref, density_ref, partial_ref, weight_ref, pair_ref, leaf_ref, route_ref,
            term_ref, centred_ref, right_ref, sum_ref, sems
        ):
            fetch(
                sems,
                (pair_hbm, pair_ref),
                (leaf_hbm, leaf_ref),
                (route_hbm, route_ref),
                (spread_hbm.at[0], term_ref),
                (centred_hbm, centred_ref),
                (right_hbm, right_ref),
            )
            fresh = (ADIABATIC - 1.0) * own_ref[ENERGY] / term_ref[...]
            density_ref[...] = jnp.where(own_ref[ACTIVE] == 1.0, fresh, own_ref[OLD])
            sum_ref[...] = jnp.zeros_like(sum_ref)

            def weigh(mine, spot, inverse, scale):
                return weight_tile(
                    right_ref[mine],
                    row(own_ref, INVERSE, mine),
                    row(own_ref, SCALE, mine),
                    spot,
                    inverse,
                    scale,
                )

            def local_tile(e):
                mine, other = pair_ref[0, e], pair_ref[1, e]
                spot = local_place(own_ref, mine, other)
                weights = stack(
                    weigh(mine, spot, row(own_ref, INVERSE, other), row(own_ref, SCALE, other))
                )
                rows = moments(row(own_ref, MASS, other), spot)
                far_term, own_term = term_ref[pl.ds(other, 1), :], term_ref[pl.ds(mine, 1), :]
                sum_ref[mine] = sum_ref[mine] + force(
                    weights, rows, far_term, own_term, centred_ref[mine]
                )

            def remote_tile(e):
                mine, spot, (h, far_mass) = export(
                    leaf_ref, route_ref, near_ref, peer_ref, own_ref, e, (3, 4)
                )
                weight_ref[e, : 3 * width, :] = stack(weigh(mine, spot, 1.0 / h, slope_scale(h)))
                extra = [far_mass] + [far_mass * item for item in spot] + [centred_ref[mine][:4]]
                weight_ref[e, 3 * width :, :] = stack(jnp.concatenate(extra, axis=0))

            grouped(pairs, local_tile)
            grouped(exports, remote_tile)
            for c in range(3):
                for leaf in range(leaves):
                    partial_ref[c, leaf : leaf + 1, :] = sum_ref[leaf, c + 1 : c + 2, :]

        stash_mib = 2 * exports * width * (6 * width + 32) // MIB
        density, partial, weights = call(
            prepare,
            "prepare_force",
            (
                shape(leaves, width),
                pltpu.HBM((3, leaves, width), f32),
                jax.ShapeDtypeStruct((exports, 3 * width + 24, width), jnp.bfloat16),
            ),
            [hbm] * 6 + [vmem] * 3,
            [
                pair_table,
                leaf_table,
                route_table,
                sheet,
                pltpu.VMEM((leaves, 8, width), f32),
                pltpu.VMEM((leaves, 48, width), jnp.bfloat16),
                pltpu.VMEM((leaves, 4, width), f32),
                pltpu.SemaphoreType.DMA((6,)),
            ],
            (pairs + exports) * tile_flops * 60,
            6 + stash_mib + wire_mib,
        )(pair_list, export_leaves, export_route, kept(outgoing), kept(centred), kept(right), own, near, peer)

        def finish(
            partial_hbm, own_ref, terms_ref, weight_ref, accel_hbm, least_ref, accel_ref, partial_ref,
            far_ref, mine_ref, rows_ref, sems
        ):
            later = pltpu.make_async_copy(partial_hbm, partial_ref, sems.at[0])
            later.start()
            owner = flags(indices(own_ref, 2, 0, exports), leaves)
            me = lax.axis_index("chip") * 2 + lax.axis_index("core")
            far_ref[...] = select(flags(indices(own_ref, 1, 0, exports), spots), terms_ref[...].reshape(spots, width))
            mine_ref[...] = select(owner, terms_ref[me])

            def tile(e):
                at = pl.ds(e, 1)
                parts = weight_ref[e, 3 * width :, :].astype(f32)
                extra = parts[:8] + parts[8:16] + parts[16:]
                part = force(
                    weight_ref[e, : 3 * width, :],
                    jnp.concatenate([extra[:4], extra[:4]], axis=0),
                    far_ref[at, :],
                    mine_ref[at, :],
                    extra[4:],
                )
                for c in range(3):
                    rows_ref[c, at, :] = part[c + 1 : c + 2]

            grouped(exports, tile)
            later.wait()
            for c in range(3):
                accel_ref[c] = partial_ref[c] + by_leaf(owner, rows_ref[c])
            awake = own_ref[ACTIVE] == 1.0
            square = jnp.zeros((leaves, width), f32)
            for c in range(3):
                part = jnp.where(awake, accel_ref[c], 0.0)
                accel_ref[c] = part
                square = square + part * part
            done = pltpu.make_async_copy(accel_ref, accel_hbm, sems.at[1])
            done.start()
            h = own_ref[H]
            speed = jnp.sqrt(ADIABATIC * (ADIABATIC - 1.0) * own_ref[ENERGY])
            step = COURANT * h / (speed + jnp.sqrt(h * jnp.sqrt(square)))
            least_ref[...] = jnp.full(
                (members, width), jnp.min(jnp.where(awake, step, jnp.inf)), f32
            )
            done.wait()

        accel, least = pl.pallas_call(
            finish,
            out_shape=(pltpu.HBM((3, leaves, width), f32), shape(members, width)),
            in_specs=[hbm] + [vmem] * 3,
            out_specs=(hbm, vmem),
            scratch_shapes=[
                pltpu.VMEM((3, leaves, width), f32),
                pltpu.VMEM((3, leaves, width), f32),
                pltpu.VMEM((exports, width), f32),
                pltpu.VMEM((exports, width), f32),
                pltpu.VMEM((3, exports, width), f32),
                pltpu.SemaphoreType.DMA((2,)),
            ],
            compiler_params=pltpu.CompilerParams(
                vmem_limit_bytes=(8 + stash_mib + wire_mib + exports * spots * 16 // MIB) * MIB
            ),
            name="finish_force",
        )(kept(partial), own, terms, weights)

        everywhere = lax.all_to_all(least, everyone, split_axis=0, concat_axis=0, tiled=True)
        return density, accel.transpose(1, 0, 2), jnp.min(everywhere)

    flat = P(everyone, None)
    deep = P(everyone, None, None)
    return jax.shard_map(
        body,
        mesh=fine,
        in_specs=(deep,) + (flat,) * 8,
        out_specs=(flat, deep, P()),
        check_vma=False,
    )
```

```python
import math

import jax
import jax.numpy as jnp
from jax import lax
from jax.experimental import pallas as pl
from jax.experimental.pallas import tpu as pltpu
from jax.sharding import Mesh, PartitionSpec as P

ADIABATIC = 5.0 / 3.0
COURANT = 0.3
GROUP = 24
MOST = 2
TINY = 1e-30
NORM = 8.0 / math.pi
MIB = 1 << 20
X, MASS, H, INVERSE, SCALE, ORIGIN, ENERGY, OLD, ACTIVE, SUM, TABLE = 0, 3, 4, 5, 6, 7, 10, 11, 12, 13, 14


def split(item):
    first = item.astype(jnp.bfloat16).astype(jnp.float32)
    rest = item - first
    second = rest.astype(jnp.bfloat16).astype(jnp.float32)
    return first, second, rest - second


def product(a, b, dims):
    return lax.dot_general(a, b, (dims, ((), ())), preferred_element_type=jnp.float32)


def left_terms(item):
    first, second, third = split(item)
    return jnp.concatenate([first, first, second, first, third, second], axis=0).astype(jnp.bfloat16)


def right_terms(item):
    first, second, third = split(item)
    return jnp.concatenate([first, second, first, third, first, second], axis=0).astype(jnp.bfloat16)


def turn(rows):
    width, count = rows[0].shape[1], len(rows)
    rows = list(rows) + [jnp.zeros_like(rows[0])] * (-count % 8)
    turned = jnp.concatenate(rows, axis=0).T
    return [jnp.broadcast_to(turned[:, k : k + 1], (width, width)) for k in range(count)]


def separation(right, place):
    norm = place[0] * place[0] + place[1] * place[1] + place[2] * place[2]
    zero = jnp.zeros_like(norm)
    left = jnp.concatenate(place + [norm, jnp.ones_like(norm), zero, zero, zero], axis=0)
    square = jnp.maximum(product(left_terms(left), right, ((0,), (0,))), TINY)
    inverse = lax.rsqrt(square)
    return square * inverse, inverse


def density_tile(right, own_inverse, place, mass):
    (mass,) = turn([mass])
    dist, _ = separation(right, place)
    ratio = dist * own_inverse
    left = 1.0 - ratio
    inner = 1.0 - 6.0 * (ratio * ratio * left)
    remain = jnp.maximum(left, 0.0)
    outer = 2.0 * (remain * remain * remain)
    value = jnp.where(ratio < 0.5, inner, outer)
    return jnp.sum(value * mass, axis=0, keepdims=True)


def slope(dist, smooth_inverse, scale):
    ratio = dist * smooth_inverse
    remain = jnp.maximum(1.0 - ratio, 0.0)
    return jnp.where(ratio < 0.5, ratio * (2.0 - 3.0 * ratio), remain * remain) * scale


def weight_tile(right, own_inverse, own_scale, place, inverse, scale):
    inverse, scale = turn([inverse, scale])
    dist, over = separation(right, place)
    return over * (slope(dist, own_inverse, own_scale) + slope(dist, inverse, scale))


def moments(mass, place):
    half = [mass] + [mass * item for item in place]
    return jnp.concatenate(half + half, axis=0)


def force(weights, rows, far_term, own_term, own_place):
    item = lax.broadcasted_iota(jnp.int32, rows.shape, 0)
    rows = jnp.where(item < 4, rows, rows * far_term)
    rows = jnp.concatenate(split(rows), axis=0).astype(jnp.bfloat16)
    sums = product(jnp.concatenate([rows, rows, rows], axis=1), weights, ((1,), (0,)))
    sums = sums[:8] + sums[8:16] + sums[16:]
    sums = own_term * sums[:4] + sums[4:]
    return own_place[:4] * sums[:1] - sums


def stack(weights):
    return jnp.concatenate([part.astype(jnp.bfloat16) for part in split(weights)], axis=0)


def flags(index, count):
    rows, width = index.shape
    lane = lax.broadcasted_iota(jnp.int32, (rows, width), 1).astype(jnp.float32)
    blocks = [(lane + float(at) == index).astype(jnp.float32) for at in range(0, count, width)]
    return jnp.concatenate(blocks, axis=1)[:, :count]


def select(onehot, data):
    onehot = jnp.concatenate([onehot] * 3, axis=1).astype(jnp.bfloat16)
    return product(onehot, jnp.concatenate(split(data), axis=0).astype(jnp.bfloat16), ((1,), (0,)))


def by_leaf(onehot, rows):
    onehot = jnp.concatenate([onehot] * 3, axis=0).astype(jnp.bfloat16)
    return product(onehot, jnp.concatenate(split(rows), axis=0).astype(jnp.bfloat16), ((0,), (0,)))


def slope_scale(h):
    square = h * h
    return (3.0 * NORM) / (square * square)


def grouped(count, body, group=GROUP):
    step = max(d for d in range(1, min(group, count) + 1) if count % d == 0)

    def run(group, carry):
        for k in range(step):
            body(group * step + k)
        return carry

    lax.fori_loop(0, count // step, run, 0)


def fetch(sems, *pairs):
    copies = [pltpu.make_async_copy(a, b, sems.at[i]) for i, (a, b) in enumerate(pairs)]
    for copy in copies:
        copy.start()
    for copy in copies:
        copy.wait()


def solution(mesh):
    groups, domains = mesh.shape["grp"], mesh.shape["dom"]
    chips = domains // 2
    fine = Mesh(mesh.devices.reshape(groups, chips, 2), ("grp", "chip", "core"))
    everyone = ("grp", "chip", "core")
    members = groups * domains
    vmem = pl.BlockSpec(memory_space=pltpu.VMEM)
    hbm = pl.BlockSpec(memory_space=pltpu.HBM)

    def call(kernel, name, outs, ins, scratch, flops, mib):
        return pl.pallas_call(
            kernel,
            out_shape=outs,
            in_specs=ins,
            out_specs=jax.tree.map(lambda _: vmem, outs),
            scratch_shapes=scratch,
            cost_estimate=pl.CostEstimate(flops=flops, bytes_accessed=1 << 16, transcendentals=0),
            compiler_params=pltpu.CompilerParams(vmem_limit_bytes=mib * MIB),
            name=name,
        )

    def body(
        positions, smoothing, energy, mass, old_density, active, pair_list, export_leaves, export_route
    ):
        leaves, _, width = positions.shape
        pairs, exports = pair_list.shape[0], export_leaves.shape[0]
        f32, s32 = jnp.float32, jnp.int32
        tile_flops = width * width

        def shape(*sizes):
            return jax.ShapeDtypeStruct(sizes, f32)

        def kept(item):
            return pltpu.with_memory_space_constraint(item, pltpu.HBM)

        place = kept(positions.transpose(1, 0, 2))
        smoothing, energy, mass = kept(smoothing), kept(energy), kept(mass)
        old_density, active = kept(old_density), kept(active)
        pair_list, export_leaves = kept(pair_list.T), kept(export_leaves.T)
        export_route = kept(export_route.T)
        pair_table, leaf_table = pltpu.SMEM((2, pairs), s32), pltpu.SMEM((2, exports), s32)
        route_table = pltpu.SMEM((1, exports), s32)
        sheet = pltpu.VMEM((leaves, width), f32)

        def copy_out(place_ref, h_ref, mass_ref, out_ref, mine_ref, sems):
            fetch(
                sems,
                (place_ref, mine_ref.at[pl.ds(0, 3)]),
                (h_ref, mine_ref.at[3]),
                (mass_ref, mine_ref.at[4]),
            )
            fetch(sems, *[(mine_ref, out_ref.at[k]) for k in range(chips)])

        outgoing = pl.pallas_call(
            copy_out,
            out_shape=pltpu.HBM((chips, 5, leaves, width), f32),
            in_specs=[hbm] * 3,
            out_specs=hbm,
            scratch_shapes=[
                pltpu.VMEM((5, leaves, width), f32),
                pltpu.SemaphoreType.DMA((max(3, chips),)),
            ],
            compiler_params=pltpu.CompilerParams(vmem_limit_bytes=2 * MIB),
            name="copy_out",
        )(place, smoothing, mass).reshape(chips, 5 * leaves, width)
        near = lax.all_to_all(outgoing, "chip", split_axis=0, concat_axis=0, tiled=True)

        def row(own_ref, item, leaf):
            return own_ref[item, pl.ds(leaf, 1), :]

        def local_place(own_ref, mine, other):
            return [row(own_ref, X + c, other) - row(own_ref, ORIGIN + c, mine) for c in range(3)]

        def local_density(
            pair_hbm, place_hbm, h_hbm, mass_hbm, energy_hbm, old_hbm, active_hbm, leaf_hbm, route_hbm,
            own_ref, right_ref, centred_ref, right_by_ref, own_by_ref, pair_ref, active_ref, leaf_ref, route_ref, sems
        ):
            fetch(
                sems,
                (pair_hbm, pair_ref),
                (place_hbm, own_ref.at[pl.ds(X, 3)]),
                (h_hbm, own_ref.at[H]),
                (mass_hbm, own_ref.at[MASS]),
                (energy_hbm, own_ref.at[ENERGY]),
                (old_hbm, own_ref.at[OLD]),
                (active_hbm, active_ref),
                (leaf_hbm, leaf_ref),
                (route_hbm, route_ref),
            )
            h = own_ref[H]
            own_ref[ACTIVE] = active_ref[...].astype(f32)
            own_ref[INVERSE] = 1.0 / h
            own_ref[SCALE] = slope_scale(h)
            own_ref[SUM] = jnp.zeros_like(h)
            norm = jnp.zeros_like(h)
            centred = []
            for c in range(3):
                mean = jnp.sum(own_ref[X + c], axis=1, keepdims=True) * (1.0 / width)
                mean = jnp.broadcast_to(mean, h.shape)
                own_ref[ORIGIN + c] = mean
                item = own_ref[X + c] - mean
                norm = norm + item * item
                centred.append(item)
            zero, one = jnp.zeros_like(h), jnp.ones_like(h)
            rights = [-2.0 * item for item in centred] + [one, norm, zero, zero, zero]
            places = [zero] + centred + [zero] * 4
            for leaf in range(leaves):
                at = slice(leaf, leaf + 1)
                right_ref[leaf] = right_terms(jnp.concatenate([item[at] for item in rights], axis=0))
                centred_ref[leaf] = jnp.concatenate([item[at] for item in places], axis=0)

            core = lax.axis_index("core")
            me = lax.axis_index("chip") * 2 + core

            own_ref[pl.ds(TABLE, 4 * sheets)] = jnp.full((4 * sheets, leaves, width), -1.0, f32)
            right_by_ref[...] = jnp.zeros_like(right_by_ref)
            own_by_ref[...] = jnp.zeros_like(own_by_ref)

            def write(kind, at, number):
                own_ref[TABLE + kind * sheets + at // leaves, pl.ds(at % leaves, 1), :] = jnp.full(
                    (1, width), number.astype(f32)
                )

            def note(e, used):
                mine, other = leaf_ref[0, e], leaf_ref[1, e]
                target = me + 1 + route_ref[0, e]
                target = jnp.where(target >= domains, target - domains, target)
                chip = target // 2
                same = (target - chip * 2 == core).astype(s32)
                slot = jnp.where(same == 1, used[0], near_slots + used[1])
                write(0, slot, chip * leaves + other)
                write(1, e, target * leaves + other)
                write(2, e, mine)
                write(3, slot, mine)
                at = pl.ds(slot, 1)
                right_by_ref[slot] = right_ref[mine]
                own_by_ref[0, at, :] = row(own_ref, INVERSE, mine)
                for c in range(3):
                    own_by_ref[1 + c, at, :] = row(own_ref, ORIGIN + c, mine)
                return used[0] + same, used[1] + 1 - same

            lax.fori_loop(0, exports, note, (jnp.int32(0), jnp.int32(0)))

            def tile(e):
                mine, other = pair_ref[0, e], pair_ref[1, e]
                own_ref[SUM, pl.ds(mine, 1), :] = row(own_ref, SUM, mine) + density_tile(
                    right_ref[mine],
                    row(own_ref, INVERSE, mine),
                    local_place(own_ref, mine, other),
                    row(own_ref, MASS, other),
                )

            grouped(pairs, tile)

        near_slots = -(-min(exports, MOST * (chips - 1)) // 8) * 8
        peer_slots = -(-min(exports, MOST * chips) // 8) * 8
        slots = near_slots + peer_slots
        spots, sheets = domains * leaves, -(-max(exports, slots) // leaves)

        def indices(own_ref, kind, first, count):
            at = TABLE + kind * sheets
            return own_ref[at : at + sheets].reshape(sheets * leaves, width)[first : first + count]

        own, right, centred, right_by, own_by = call(
            local_density,
            "local_density",
            (
                shape(TABLE + 4 * sheets, leaves, width),
                pltpu.HBM((leaves, 48, width), jnp.bfloat16),
                pltpu.HBM((leaves, 8, width), f32),
                jax.ShapeDtypeStruct((slots, 48, width), jnp.bfloat16),
                shape(4, slots, width),
            ),
            [hbm] * 9,
            [
                pair_table,
                pltpu.VMEM((leaves, width), s32),
                leaf_table,
                route_table,
                pltpu.SemaphoreType.DMA((9,)),
            ],
            pairs * tile_flops * 30,
            6 + exports * spots * 16 // MIB,
        )(
            pair_list, place, smoothing, mass, energy, old_density, active, export_leaves,
            export_route,
        )
        near, own = lax.optimization_barrier((near, own))
        peer = lax.ppermute(near, "core", [(0, 1), (1, 0)])

        def export(leaf_ref, route_ref, near_ref, peer_ref, own_ref, e, items):
            core = lax.axis_index("core")
            me = lax.axis_index("chip") * 2 + core
            mine, other = leaf_ref[0, e], leaf_ref[1, e]
            target = me + 1 + route_ref[0, e]
            target = jnp.where(target >= domains, target - domains, target)
            chip = target // 2
            same = (target - chip * 2) == core

            def get(c):
                at = pl.ds(c * leaves + other, 1)
                return jnp.where(same, near_ref[chip, at, :], peer_ref[chip, at, :])

            spot = [get(c) - row(own_ref, ORIGIN + c, mine) for c in range(3)]
            return mine, spot, [get(c) for c in items]

        def slot_density(first, count, right_by_ref, own_by_ref, own_ref, data_ref, far_ref, rows_ref):
            pick = flags(indices(own_ref, 0, first, count), spots // 2)
            owner = flags(indices(own_ref, 3, first, count), leaves)
            for k, c in enumerate((0, 1, 2, 4)):
                data = data_ref[:, c * leaves : (c + 1) * leaves, :].reshape(spots // 2, width)
                far_ref[k] = select(pick, data)
            for c in range(3):
                far_ref[c] = far_ref[c] - own_by_ref[1 + c, first : first + count]

            def tile(e):
                rows_ref[pl.ds(e, 1), :] = density_tile(
                    right_by_ref[first + e],
                    row(own_by_ref, 0, first + e),
                    [row(far_ref, c, e) for c in range(3)],
                    row(far_ref, 3, e),
                )

            grouped(count, tile)
            return by_leaf(owner, rows_ref[...])

        def near_density(right_by_ref, own_by_ref, own_ref, near_ref, sum_ref, far_ref, rows_ref):
            sum_ref[...] = own_ref[SUM] + slot_density(
                0, near_slots, right_by_ref, own_by_ref, own_ref, near_ref, far_ref, rows_ref
            )

        wire_mib = 2 * domains * leaves * width * 20 // MIB
        near_sum = call(
            near_density,
            "near_density",
            shape(leaves, width),
            [vmem] * 4,
            [pltpu.VMEM((4, near_slots, width), f32), pltpu.VMEM((near_slots, width), f32)],
            near_slots * tile_flops * 30,
            6 + wire_mib + exports * spots * 16 // MIB,
        )(right_by, own_by, own, near)

        def peer_density(
            right_by_ref, own_by_ref, own_ref, sum_ref, peer_ref, spread_ref, far_ref, rows_ref, term_ref, sems
        ):
            total = sum_ref[...] + slot_density(
                near_slots, peer_slots, right_by_ref, own_by_ref, own_ref, peer_ref, far_ref, rows_ref
            )
            inverse = own_ref[INVERSE]
            summed = (total + own_ref[MASS]) * (NORM * (inverse * inverse * inverse))
            density = jnp.where(own_ref[ACTIVE] == 1.0, summed, own_ref[OLD])
            term = (ADIABATIC - 1.0) * own_ref[ENERGY] / density
            term_ref[...] = term
            fetch(sems, *[(term_ref, spread_ref.at[d]) for d in range(domains)])

        outgoing = pl.pallas_call(
            peer_density,
            out_shape=pltpu.HBM((domains, leaves, width), f32),
            in_specs=[vmem] * 5,
            out_specs=hbm,
            scratch_shapes=[
                pltpu.VMEM((4, peer_slots, width), f32),
                pltpu.VMEM((peer_slots, width), f32),
                sheet,
                pltpu.SemaphoreType.DMA((domains,)),
            ],
            compiler_params=pltpu.CompilerParams(
                vmem_limit_bytes=(6 + 2 * wire_mib + exports * spots * 16 // MIB) * MIB
            ),
            name="peer_density",
        )(right_by, own_by, own, near_sum, peer)
        terms = lax.all_to_all(outgoing, ("chip", "core"), split_axis=0, concat_axis=0, tiled=True)

        def prepare(
            pair_hbm, leaf_hbm, route_hbm, spread_hbm, centred_hbm, right_hbm, own_ref, near_ref,
            peer_ref, density_ref, partial_ref, weight_ref, pair_ref, leaf_ref, route_ref,
            term_ref, centred_ref, right_ref, sum_ref, sems
        ):
            fetch(
                sems,
                (pair_hbm, pair_ref),
                (leaf_hbm, leaf_ref),
                (route_hbm, route_ref),
                (spread_hbm.at[0], term_ref),
                (centred_hbm, centred_ref),
                (right_hbm, right_ref),
            )
            fresh = (ADIABATIC - 1.0) * own_ref[ENERGY] / term_ref[...]
            density_ref[...] = jnp.where(own_ref[ACTIVE] == 1.0, fresh, own_ref[OLD])
            sum_ref[...] = jnp.zeros_like(sum_ref)

            def weigh(mine, spot, inverse, scale):
                return weight_tile(
                    right_ref[mine],
                    row(own_ref, INVERSE, mine),
                    row(own_ref, SCALE, mine),
                    spot,
                    inverse,
                    scale,
                )

            def local_tile(e):
                mine, other = pair_ref[0, e], pair_ref[1, e]
                spot = local_place(own_ref, mine, other)
                weights = stack(
                    weigh(mine, spot, row(own_ref, INVERSE, other), row(own_ref, SCALE, other))
                )
                rows = moments(row(own_ref, MASS, other), spot)
                far_term, own_term = term_ref[pl.ds(other, 1), :], term_ref[pl.ds(mine, 1), :]
                sum_ref[mine] = sum_ref[mine] + force(
                    weights, rows, far_term, own_term, centred_ref[mine]
                )

            def remote_tile(e):
                mine, spot, (h, far_mass) = export(
                    leaf_ref, route_ref, near_ref, peer_ref, own_ref, e, (3, 4)
                )
                weight_ref[e, : 3 * width, :] = stack(weigh(mine, spot, 1.0 / h, slope_scale(h)))
                extra = [far_mass] + [far_mass * item for item in spot] + [centred_ref[mine][:4]]
                weight_ref[e, 3 * width :, :] = stack(jnp.concatenate(extra, axis=0))

            grouped(pairs, local_tile)
            grouped(exports, remote_tile)
            for c in range(3):
                for leaf in range(leaves):
                    partial_ref[c, leaf : leaf + 1, :] = sum_ref[leaf, c + 1 : c + 2, :]

        stash_mib = 2 * exports * width * (6 * width + 32) // MIB
        density, partial, weights = call(
            prepare,
            "prepare_force",
            (
                shape(leaves, width),
                pltpu.HBM((3, leaves, width), f32),
                jax.ShapeDtypeStruct((exports, 3 * width + 24, width), jnp.bfloat16),
            ),
            [hbm] * 6 + [vmem] * 3,
            [
                pair_table,
                leaf_table,
                route_table,
                sheet,
                pltpu.VMEM((leaves, 8, width), f32),
                pltpu.VMEM((leaves, 48, width), jnp.bfloat16),
                pltpu.VMEM((leaves, 4, width), f32),
                pltpu.SemaphoreType.DMA((6,)),
            ],
            (pairs + exports) * tile_flops * 60,
            6 + stash_mib + wire_mib,
        )(pair_list, export_leaves, export_route, kept(outgoing), kept(centred), kept(right), own, near, peer)

        def finish(
            partial_hbm, own_ref, terms_ref, weight_ref, accel_hbm, least_ref, accel_ref, partial_ref,
            far_ref, mine_ref, rows_ref, sems
        ):
            later = pltpu.make_async_copy(partial_hbm, partial_ref, sems.at[0])
            later.start()
            owner = flags(indices(own_ref, 2, 0, exports), leaves)
            me = lax.axis_index("chip") * 2 + lax.axis_index("core")
            far_ref[...] = select(flags(indices(own_ref, 1, 0, exports), spots), terms_ref[...].reshape(spots, width))
            mine_ref[...] = select(owner, terms_ref[me])

            def tile(e):
                at = pl.ds(e, 1)
                parts = weight_ref[e, 3 * width :, :].astype(f32)
                extra = parts[:8] + parts[8:16] + parts[16:]
                part = force(
                    weight_ref[e, : 3 * width, :],
                    jnp.concatenate([extra[:4], extra[:4]], axis=0),
                    far_ref[at, :],
                    mine_ref[at, :],
                    extra[4:],
                )
                for c in range(3):
                    rows_ref[c, at, :] = part[c + 1 : c + 2]

            grouped(exports, tile)
            later.wait()
            for c in range(3):
                accel_ref[c] = partial_ref[c] + by_leaf(owner, rows_ref[c])
            awake = own_ref[ACTIVE] == 1.0
            square = jnp.zeros((leaves, width), f32)
            for c in range(3):
                part = jnp.where(awake, accel_ref[c], 0.0)
                accel_ref[c] = part
                square = square + part * part
            done = pltpu.make_async_copy(accel_ref, accel_hbm, sems.at[1])
            done.start()
            h = own_ref[H]
            speed = jnp.sqrt(ADIABATIC * (ADIABATIC - 1.0) * own_ref[ENERGY])
            step = COURANT * h / (speed + jnp.sqrt(h * jnp.sqrt(square)))
            least_ref[...] = jnp.full(
                (members, width), jnp.min(jnp.where(awake, step, jnp.inf)), f32
            )
            done.wait()

        accel, least = pl.pallas_call(
            finish,
            out_shape=(pltpu.HBM((3, leaves, width), f32), shape(members, width)),
            in_specs=[hbm] + [vmem] * 3,
            out_specs=(hbm, vmem),
            scratch_shapes=[
                pltpu.VMEM((3, leaves, width), f32),
                pltpu.VMEM((3, leaves, width), f32),
                pltpu.VMEM((exports, width), f32),
                pltpu.VMEM((exports, width), f32),
                pltpu.VMEM((3, exports, width), f32),
                pltpu.SemaphoreType.DMA((2,)),
            ],
            compiler_params=pltpu.CompilerParams(
                vmem_limit_bytes=(8 + stash_mib + wire_mib + exports * spots * 16 // MIB) * MIB
            ),
            name="finish_force",
        )(kept(partial), own, terms, weights)

        everywhere = lax.all_to_all(least, everyone, split_axis=0, concat_axis=0, tiled=True)
        return density, accel.transpose(1, 0, 2), jnp.min(everywhere)

    flat = P(everyone, None)
    deep = P(everyone, None, None)
    return jax.shard_map(
        body,
        mesh=fine,
        in_specs=(deep,) + (flat,) * 8,
        out_specs=(flat, deep, P()),
        check_vma=False,
    )
```
